128 devices in a mesh: dp: 8 (over z_lo, x), blk: 16 (over y, z_hi, core).
Axes of the slice: x: 4, y: 4, z: 4 (z_hi: 2, z_lo: 2; z = z_hi * 2 + z_lo), core: 2. Of those that a mesh axis runs over, the one named last changes fastest.
Arguments:
- inputs: bfloat16 [8, 4096, 1024], P('dp', 'blk'), may hold values from -6 to 6
- upstream: bfloat16 [8, 4096, 1024], P('dp', 'blk'), may hold values from -6 to 6
- gain: float32 [1024], replicated, may hold values from 0.5 to 1.5
- w_query: bfloat16 [1024, 1024], replicated
- w_key: bfloat16 [1024, 256], replicated
- w_value: bfloat16 [1024, 256], replicated, may hold values from -0.1875 to 0.1875
- w_out: bfloat16 [1024, 1024], replicated, may hold values from -0.1875 to 0.1875
- prefix_len: int32 [8], P('dp'), may hold values from 512 to 4032
- bound: int32 [8], P('dp'), may hold values from 0 to 31
Outputs:
- d_inputs: bfloat16 [8, 4096, 1024], P('dp', 'blk')
- d_query: float32 [1024, 1024], P('blk')
- d_key: float32 [1024, 256], P('blk')
- d_value: float32 [1024, 256], P('blk')
- d_out: float32 [1024, 1024], P('blk')
- d_gain: float32 [1024], P('blk')
The draws below stay inside these ranges and needn't reach their ends.
All inputs are finite; a program needn't handle non-finite values.
Results may differ from the reference program's by a relative error of at most 0.02.
The reference program's roundings to bfloat16 on the way (of `hidden`, `query`, `d_attn`, `probs_b`, `attn`, `dscores`, `dq` and `dk`) count: a program that leaves them out, or rounds other values in their place, can miss the bound.
Values may be sent and summed in bfloat16 or wider, within the bound.
No kernel may reach another device: no remote copies, remote signals or barrier semaphores. Data moves between devices by JAX's collectives and lax.ppermute only.
A program may use at most 128 MiB of HBM per device.

```python
import jax
import jax.numpy as jnp
from jax import lax

D = 1024
HEADS = 4
HS = 256
ACT = 64
BLOCK = 128
HQ = 1024
SEQ = 4096
EPISODES = 8


def paired_weights(key):
    base_query = jax.random.normal(jax.random.fold_in(key, 11), (D, HEADS * HS), jnp.float32) * D ** (-0.5)
    base_key = jax.random.normal(jax.random.fold_in(key, 12), (D, HS), jnp.float32) * D ** (-0.5)
    return (base_query, base_key)


def draw_w_query(key, part):
    return paired_weights(key)[0].astype(jnp.bfloat16)


def draw_w_key(key, part):
    return paired_weights(key)[1].astype(jnp.bfloat16)


def touch_ends(entries, own_key, low, top_value):
    index_at = [jax.random.randint(jax.random.fold_in(own_key, axis), (), 0, length) for axis, length in enumerate(entries.shape)]
    longest = entries.shape.index(max(entries.shape))
    next_to = index_at[:longest] + [(index_at[longest] + 1) % entries.shape[longest]] + index_at[longest + 1:]
    return entries.at[tuple(index_at)].set(low).at[tuple(next_to)].set(top_value)


def shard_levels(rng, dims, shards, least, top_value):
    def one(axis_at, shards_of):
        draws = jax.random.uniform(jax.random.fold_in(jax.random.fold_in(rng, 6), axis_at), (shards_of,), jnp.float32, least / len(shards), top_value / len(shards))
        return jnp.repeat(jnp.exp(draws), dims[axis_at] // shards_of).reshape((-1,) + (1,) * (len(dims) - axis_at - 1))

    level = one(*shards[0])
    for cut in shards[1:]:
        level = level * one(*cut)
    return level


def noise(stream_key, shape, width, most, shards=(), kind=jnp.bfloat16):
    values = jax.random.normal(stream_key, shape, jnp.float32) * width
    if len(shards) > 0:
        values = shard_levels(stream_key, shape, shards, -0.22, 0.18) * values
    return jnp.clip(values, min=-most, max=most).astype(kind)


def setup_inputs(seed: int = 0) -> dict:
    splits = jax.random.split(jax.random.key(seed), 10)
    return {
        "inputs": noise(splits[0], (EPISODES, SEQ, D), 1.0, 6.0, ((0, 8), (1, 16))),
        "upstream": noise(splits[1], (EPISODES, SEQ, D), 1.0, 6.0, ((0, 8), (1, 16))),
        "gain": jnp.clip(1.0 + 0.1 * jax.random.normal(splits[2], (D,), jnp.float32), 0.5, 1.5),
        "w_query": draw_w_query(jax.random.fold_in(splits[9], 71), 0),
        "w_key": draw_w_key(jax.random.fold_in(splits[9], 71), 0),
        "w_value": noise(splits[5], (D, HS), D ** -0.5, 0.1875),
        "w_out": noise(splits[6], (HQ, D), HQ ** -0.5, 0.1875),
        "prefix_len": touch_ends(jax.random.randint(splits[7], (EPISODES,), SEQ // 8, SEQ - ACT + 1), jax.random.fold_in(splits[7], 1), SEQ // 8, SEQ - ACT).astype(jnp.int32),
        "bound": touch_ends(jax.random.randint(splits[8], (EPISODES,), 0, SEQ // BLOCK), jax.random.fold_in(splits[8], 1), 0, (SEQ // BLOCK) - 1).astype(jnp.int32),
    }


EPS = 1e-06
NEG = -1e+30

def episode_grads(inputs, upstream, plen, edge_block, gain, w_query, w_key, w_value, w_out):
    scaling = HS ** (-0.5)
    xf = inputs.astype(jnp.float32)
    inv = lax.rsqrt(lax.optimization_barrier(jnp.mean(xf * xf, axis=-1, keepdims=True)) + EPS)
    normed = xf * inv
    hidden = (normed * gain).astype(jnp.bfloat16)
    query = jnp.dot(hidden, w_query, preferred_element_type=jnp.float32).astype(jnp.bfloat16)
    keys = jnp.dot(hidden, w_key, preferred_element_type=jnp.float32).astype(jnp.bfloat16)
    values = jnp.dot(hidden, w_value, preferred_element_type=jnp.float32).astype(jnp.bfloat16)
    d_attn = jnp.dot(upstream, w_out.T, preferred_element_type=jnp.float32).astype(jnp.bfloat16)
    pos = jnp.arange(SEQ, dtype=jnp.int32)
    key_ok = (pos < plen) | (pos >= SEQ - ACT)
    visible = key_ok[None, :] & ((pos[None, :] < BLOCK * edge_block) | (pos[None, :] <= pos[:, None]))
    q_heads = query.reshape(SEQ, HEADS, HS).transpose(1, 0, 2)
    a_heads = d_attn.reshape(SEQ, HEADS, HS).transpose(1, 0, 2)

    def one_head(pair):
        q_one, da_one = pair
        scores = jnp.dot(q_one, keys.T, preferred_element_type=jnp.float32) * scaling
        scores = jnp.where(visible, scores, NEG)
        top = lax.optimization_barrier(jnp.max(scores, axis=-1, keepdims=True))
        expo = jnp.exp(scores - top)
        probs = expo / lax.optimization_barrier(jnp.sum(expo, axis=-1, keepdims=True))
        probs_b = probs.astype(jnp.bfloat16)
        attn = jnp.dot(probs_b, values, preferred_element_type=jnp.float32).astype(jnp.bfloat16)
        dprobs = jnp.dot(da_one, values.T, preferred_element_type=jnp.float32)
        delta = lax.optimization_barrier(jnp.sum(da_one.astype(jnp.float32) * attn.astype(jnp.float32), axis=-1, keepdims=True))
        dscores = (probs * (dprobs - delta)).astype(jnp.bfloat16)
        dq = jnp.dot(dscores, keys, preferred_element_type=jnp.float32) * scaling
        dk = jnp.dot(dscores.T, q_one, preferred_element_type=jnp.float32) * scaling
        dv = jnp.dot(probs_b.T, da_one, preferred_element_type=jnp.float32)
        return (attn, dq, dk, dv)
    attn_h, dq_h, dk_h, dv_h = lax.map(one_head, (q_heads, a_heads))
    attn = attn_h.transpose(1, 0, 2).reshape(SEQ, HEADS * HS)
    dq = dq_h.transpose(1, 0, 2).reshape(SEQ, HEADS * HS).astype(jnp.bfloat16)
    dk = lax.optimization_barrier(jnp.sum(dk_h, axis=0)).astype(jnp.bfloat16)
    dv = lax.optimization_barrier(jnp.sum(dv_h, axis=0)).astype(jnp.bfloat16)
    dhidden = jnp.dot(dq, w_query.T, preferred_element_type=jnp.float32)
    dhidden = dhidden + jnp.dot(dk, w_key.T, preferred_element_type=jnp.float32)
    dhidden = dhidden + jnp.dot(dv, w_value.T, preferred_element_type=jnp.float32)
    g_query = jnp.dot(hidden.T, dq, preferred_element_type=jnp.float32)
    g_key = jnp.dot(hidden.T, dk, preferred_element_type=jnp.float32)
    g_value = jnp.dot(hidden.T, dv, preferred_element_type=jnp.float32)
    g_out = jnp.dot(attn.T, upstream, preferred_element_type=jnp.float32)
    g_gain = lax.optimization_barrier(jnp.sum(dhidden * normed, axis=0))
    scaled = dhidden * gain
    d_in = upstream.astype(jnp.float32) + inv * (scaled - normed * lax.optimization_barrier(jnp.mean(scaled * normed, axis=-1, keepdims=True)))
    return (d_in.astype(jnp.bfloat16), g_query, g_key, g_value, g_out, g_gain)

def reference(inputs, upstream, gain, w_query, w_key, w_value, w_out, prefix_len, bound):

    def per_episode(item):
        x_one, g_one, plen, edge_block = item
        return episode_grads(x_one, g_one, plen, edge_block, gain, w_query, w_key, w_value, w_out)
    d_in, g_query, g_key, g_value, g_out, g_gain = lax.map(per_episode, (inputs, upstream, prefix_len, bound))
    return (d_in, lax.optimization_barrier(jnp.sum(g_query, axis=0)), lax.optimization_barrier(jnp.sum(g_key, axis=0)), lax.optimization_barrier(jnp.sum(g_value, axis=0)), lax.optimization_barrier(jnp.sum(g_out, axis=0)), lax.optimization_barrier(jnp.sum(g_gain, axis=0)))
```

```python
import functools

import jax
import jax.numpy as jnp
from jax import lax
from jax.experimental import pallas as pl
from jax.experimental.pallas import tpu as pltpu
from jax.sharding import PartitionSpec as P

HS = 256
ACT = 64
BLOCK = 128
NEG = -1e30
LOG2E = 1.4426950408889634
VMEM_BYTES = 60 * 1024 * 1024
NT = (((1,), (1,)), ((), ()))


def dot_nt(a, b):
    return lax.dot_general(a, b, NT, preferred_element_type=jnp.float32)


def dot_nn(a, b):
    return jnp.dot(a, b, preferred_element_type=jnp.float32)


def block_state(info, chip, tok, seq):
    my, plen, edge = info[0], info[1], info[2]
    low = chip * (2 * tok)
    high = low + 2 * tok
    first, last = my * tok, my * tok + tok - 1
    seen = ((low < plen) | (high > seq - ACT)) & ((low < edge) | (low <= last))
    full = (high <= plen) & ((high <= edge) | (high - 1 <= first))
    return seen, full


def mask_of(info, chip, tok, seq):
    my, plen, edge, core = info[0], info[1], info[2], info[3]
    rows = lax.broadcasted_iota(jnp.int32, (2 * tok, tok), 0)
    k_pos = chip * (2 * tok) + (rows ^ (core * tok))
    q_pos = my * tok + lax.broadcasted_iota(jnp.int32, (2 * tok, tok), 1)
    key_ok = (k_pos < plen) | (k_pos >= seq - ACT)
    return key_ok & ((k_pos < edge) | (k_pos <= q_pos))


def per_block(info, chips, tok, seq, work, rest):
    def step(chip, carry):
        seen, full = block_state(info, chip, tok, seq)

        @pl.when(full)
        def _():
            work(chip, None)

        @pl.when(seen & jnp.logical_not(full))
        def _():
            work(chip, mask_of(info, chip, tok, seq))

        if rest is not None:

            @pl.when(jnp.logical_not(seen))
            def _():
                rest(chip)

        return carry

    lax.fori_loop(0, chips, step, 0)


def take_in(sources, scratch, sems, tok):
    copies = []
    for n, (own, pair, into) in enumerate(zip(sources[::2], sources[1::2], scratch)):
        copies.append(pltpu.make_async_copy(own, into.at[:, :tok, :], sems.at[2 * n]))
        copies.append(pltpu.make_async_copy(pair, into.at[:, tok:, :], sems.at[2 * n + 1]))
    for c in copies:
        c.start()
    return copies


def head(h):
    return pl.ds(h * HS, HS)


def scaled_scores(keys, q, h, mask):
    s = dot_nt(keys, q[:, head(h)]) * (HS ** (-0.5) * LOG2E)
    return s if mask is None else jnp.where(mask, s, NEG)


def stats_kernel(heads, seq, info, q, k_own, k_pair, lse, keys, top, total, sems):
    tok, chips = q.shape[0], k_own.shape[0]
    copies = take_in((k_own, k_pair), (keys,), sems, tok)
    top[...] = jnp.full(top.shape, NEG, jnp.float32)
    total[...] = jnp.zeros(total.shape, jnp.float32)
    for c in copies:
        c.wait()

    def work(chip, mask):
        for h in range(heads):
            s = scaled_scores(keys[chip], q, h, mask)
            old = top[:, head(h)]
            new = jnp.maximum(old, jnp.max(s, axis=0, keepdims=True))
            top[:, head(h)] = new
            total[:, head(h)] = total[:, head(h)] * jnp.exp2(old - new) + jnp.sum(
                jnp.exp2(s - new), axis=0, keepdims=True
            )

    per_block(info, chips, tok, seq, work, None)
    lse[...] = top[...] + jnp.log(total[...]) * LOG2E


def attend_kernel(
    heads, seq, info, q, da, lse, k_own, k_pair, v_own, v_pair,
    attn_t, delta, dv_own, dv_pair, probs_out,
    keys, values, values_t, da_rows, probs, sems, out_sems,
):
    tok, chips = q.shape[0], k_own.shape[0]
    wide = 2 * tok
    copies = take_in((k_own, k_pair, v_own, v_pair), (keys, values), sems, tok)
    for h in range(heads):
        da_rows[head(h), :] = da[:, head(h)]
    for c in copies:
        c.wait()
    for chip in range(chips):
        values_t[:, pl.ds(chip * wide, wide)] = values[chip].T

    def out_copy(chip):
        rows = pl.ds(pl.multiple_of(chip * wide, wide), wide)
        return pltpu.make_async_copy(probs.at[rows, :], probs_out.at[rows, :], out_sems.at[chip])

    def work(chip, mask):
        rows = pl.ds(pl.multiple_of(chip * wide, wide), wide)
        for h in range(heads):
            s = scaled_scores(keys[chip], q, h, mask)
            probs[rows, head(h)] = jnp.exp2(s - lse[:, head(h)]).astype(jnp.bfloat16)
        dv = dot_nn(probs[rows, :], da_rows[...]).astype(jnp.bfloat16)
        dv_own[chip] = dv[:tok]
        dv_pair[chip] = dv[tok:]
        out_copy(chip).start()

    def rest(chip):
        rows = pl.ds(pl.multiple_of(chip * wide, wide), wide)
        probs[rows, :] = jnp.zeros((wide, heads * HS), jnp.bfloat16)
        dv_own[chip] = jnp.zeros((tok, HS), jnp.bfloat16)
        dv_pair[chip] = jnp.zeros((tok, HS), jnp.bfloat16)
        out_copy(chip).start()

    per_block(info, chips, tok, seq, work, rest)
    for h in range(heads):
        a = dot_nn(values_t[...], probs[:, head(h)]).astype(jnp.bfloat16)
        attn_t[head(h), :] = a
        delta[:, head(h)] = jnp.sum(
            a.astype(jnp.float32) * da_rows[head(h), :].T.astype(jnp.float32), axis=0, keepdims=True
        )
    lax.fori_loop(0, chips, lambda chip, c: (out_copy(chip).wait(), c)[1], 0)


def grads_kernel(
    heads, seq, info, q, da, delta, k_own, k_pair, v_own, v_pair, probs_in,
    dq, dk_own, dk_pair,
    keys, values, keys_t, q_rows, probs, dscores, sems, in_sems,
):
    tok, chips = q.shape[0], k_own.shape[0]
    wide = 2 * tok
    copies = take_in((k_own, k_pair, v_own, v_pair), (keys, values), sems, tok)

    def in_copy(chip):
        rows = pl.ds(pl.multiple_of(chip * wide, wide), wide)
        return pltpu.make_async_copy(probs_in.at[rows, :], probs.at[rows, :], in_sems.at[chip])

    lax.fori_loop(0, chips, lambda chip, c: (in_copy(chip).start(), c)[1], 0)
    for h in range(heads):
        q_rows[head(h), :] = q[:, head(h)]
    for c in copies:
        c.wait()
    for chip in range(chips):
        keys_t[:, pl.ds(chip * wide, wide)] = keys[chip].T

    def step(chip, carry):
        rows = pl.ds(pl.multiple_of(chip * wide, wide), wide)
        in_copy(chip).wait()
        seen, _ = block_state(info, chip, tok, seq)

        @pl.when(seen)
        def _():
            for h in range(heads):
                dp = dot_nt(values[chip], da[:, head(h)])
                p = probs[rows, head(h)].astype(jnp.float32)
                dscores[rows, head(h)] = (p * (dp - delta[:, head(h)])).astype(jnp.bfloat16)
            dk = (dot_nn(dscores[rows, :], q_rows[...]) * HS ** (-0.5)).astype(jnp.bfloat16)
            dk_own[chip] = dk[:tok]
            dk_pair[chip] = dk[tok:]

        @pl.when(jnp.logical_not(seen))
        def _():
            dscores[rows, :] = jnp.zeros((wide, heads * HS), jnp.bfloat16)
            dk_own[chip] = jnp.zeros((tok, HS), jnp.bfloat16)
            dk_pair[chip] = jnp.zeros((tok, HS), jnp.bfloat16)

        return carry

    lax.fori_loop(0, chips, step, 0)
    for h in range(heads):
        d = dot_nn(keys_t[...], dscores[:, head(h)]) * HS ** (-0.5)
        dq[:, head(h)] = d.T.astype(jnp.bfloat16)


SMEM = pl.BlockSpec(memory_space=pltpu.SMEM)
VMEM = pl.BlockSpec(memory_space=pltpu.VMEM)
ANY = pl.BlockSpec(memory_space=pl.ANY)


def params():
    return pltpu.CompilerParams(vmem_limit_bytes=VMEM_BYTES)


def cost(flops, elements):
    return pl.CostEstimate(flops=flops, bytes_accessed=2 * elements, transcendentals=elements)


def run_stats(info, q, k_own, k_pair):
    tok, width = q.shape
    heads, chips = width // HS, k_own.shape[0]
    seq = 2 * tok * chips
    return pl.pallas_call(
        functools.partial(stats_kernel, heads, seq),
        out_shape=jax.ShapeDtypeStruct((1, width), jnp.float32),
        in_specs=[SMEM, VMEM, ANY, ANY],
        out_specs=VMEM,
        scratch_shapes=[
            pltpu.VMEM((chips, 2 * tok, HS), jnp.bfloat16),
            pltpu.VMEM((1, width), jnp.float32),
            pltpu.VMEM((1, width), jnp.float32),
            pltpu.SemaphoreType.DMA((2,)),
        ],
        compiler_params=params(),
        cost_estimate=cost(2 * seq * width * HS, seq * width),
        name="stats",
    )(info, q, k_own, k_pair)


def run_attend(info, q, da, lse, k_own, k_pair, v_own, v_pair):
    tok, width = q.shape
    heads, chips = width // HS, k_own.shape[0]
    seq = 2 * tok * chips
    part = jax.ShapeDtypeStruct((chips, tok, HS), jnp.bfloat16)
    return pl.pallas_call(
        functools.partial(attend_kernel, heads, seq),
        out_shape=(
            jax.ShapeDtypeStruct((width, tok), jnp.bfloat16),
            jax.ShapeDtypeStruct((1, width), jnp.float32),
            part,
            part,
            jax.ShapeDtypeStruct((seq, width), jnp.bfloat16),
        ),
        in_specs=[SMEM, VMEM, VMEM, VMEM, ANY, ANY, ANY, ANY],
        out_specs=(VMEM, VMEM, VMEM, VMEM, ANY),
        scratch_shapes=[
            pltpu.VMEM((chips, 2 * tok, HS), jnp.bfloat16),
            pltpu.VMEM((chips, 2 * tok, HS), jnp.bfloat16),
            pltpu.VMEM((HS, seq), jnp.bfloat16),
            pltpu.VMEM((width, HS), jnp.bfloat16),
            pltpu.VMEM((seq, width), jnp.bfloat16),
            pltpu.SemaphoreType.DMA((4,)),
            pltpu.SemaphoreType.DMA((chips,)),
        ],
        compiler_params=params(),
        cost_estimate=cost(6 * seq * width * HS, seq * width),
        name="attend",
    )(info, q, da, lse, k_own, k_pair, v_own, v_pair)


def run_grads(info, q, da, delta, k_own, k_pair, v_own, v_pair, probs):
    tok, width = q.shape
    heads, chips = width // HS, k_own.shape[0]
    seq = 2 * tok * chips
    part = jax.ShapeDtypeStruct((chips, tok, HS), jnp.bfloat16)
    return pl.pallas_call(
        functools.partial(grads_kernel, heads, seq),
        out_shape=(jax.ShapeDtypeStruct((tok, width), jnp.bfloat16), part, part),
        in_specs=[SMEM, VMEM, VMEM, VMEM, ANY, ANY, ANY, ANY, ANY],
        out_specs=(VMEM, VMEM, VMEM),
        scratch_shapes=[
            pltpu.VMEM((chips, 2 * tok, HS), jnp.bfloat16),
            pltpu.VMEM((chips, 2 * tok, HS), jnp.bfloat16),
            pltpu.VMEM((HS, seq), jnp.bfloat16),
            pltpu.VMEM((width, HS), jnp.bfloat16),
            pltpu.VMEM((seq, width), jnp.bfloat16),
            pltpu.VMEM((seq, width), jnp.bfloat16),
            pltpu.SemaphoreType.DMA((4,)),
            pltpu.SemaphoreType.DMA((chips,)),
        ],
        compiler_params=params(),
        cost_estimate=cost(6 * seq * width * HS, seq * width),
        name="grads",
    )(info, q, da, delta, k_own, k_pair, v_own, v_pair, probs)


EPS = 1e-06


def contract_first(left, right):
    return lax.dot_general(
        left, right, (((0,), (0,)), ((), ())), preferred_element_type=jnp.float32
    )


def same_core(count):
    return [[core + 2 * chip for chip in range(count // 2)] for core in range(2)]


def swap_cores(value):
    count = lax.axis_size("blk")
    return lax.ppermute(value, "blk", [(i, i ^ 1) for i in range(count)])


def exchange_chips(value):
    groups = same_core(lax.axis_size("blk"))
    return lax.all_to_all(value, "blk", 0, 0, tiled=True, axis_index_groups=groups)


def gather_chips(value):
    copies = jnp.broadcast_to(value, (lax.axis_size("blk") // 2, *value.shape))
    return exchange_chips(copies)


def sum_first(parts):
    return jnp.sum(parts.astype(jnp.float32), axis=0)


def reduce_to_owner(own, pair):
    received = swap_cores(pair.astype(jnp.bfloat16))
    chip_sum = own.astype(jnp.float32) + received.astype(jnp.float32)
    return sum_first(exchange_chips(chip_sum.astype(jnp.bfloat16)))


def reduce_weights(grad):
    count, core = lax.axis_size("blk"), lax.axis_index("blk") % 2
    rows = grad.shape[0] // count
    parts = grad.reshape(count // 2, 2, rows, *grad.shape[1:])
    own = lax.dynamic_index_in_dim(parts, core, 1, keepdims=False)
    pair = lax.dynamic_index_in_dim(parts, 1 - core, 1, keepdims=False)
    mine = reduce_to_owner(own, pair).astype(jnp.bfloat16)
    copies = jnp.broadcast_to(mine, (lax.axis_size("dp"), *mine.shape))
    return sum_first(lax.all_to_all(copies, "dp", 0, 0, tiled=True))


def per_device(inputs, upstream, gain, w_query, w_key, w_value, w_out, prefix_len, bound):
    bf16 = jnp.bfloat16
    xf = inputs[0].astype(jnp.float32)
    grad_out = upstream[0]
    my = lax.axis_index("blk")
    count = lax.axis_size("blk")
    inv = lax.rsqrt(jnp.mean(xf * xf, axis=-1, keepdims=True) + EPS)
    normed = xf * inv
    hidden = (normed * gain).astype(bf16)
    keys = dot_nn(hidden, w_key).astype(bf16)
    k_own = gather_chips(keys)
    values = dot_nn(hidden, w_value).astype(bf16)
    v_own = gather_chips(values)
    k_pair = swap_cores(k_own)
    v_pair = swap_cores(v_own)
    query = dot_nn(hidden, w_query).astype(bf16)
    d_attn = dot_nt(grad_out, w_out).astype(bf16)
    info = jnp.stack([my, prefix_len[0], bound[0] * BLOCK, my % 2]).astype(jnp.int32)

    lse = run_stats(info, query, k_own, k_pair)
    attn_t, delta, dv_own, dv_pair, probs = run_attend(
        info, query, d_attn, lse, k_own, k_pair, v_own, v_pair
    )
    d_value_rows = reduce_to_owner(dv_own, dv_pair).astype(bf16)
    g_out = dot_nn(attn_t, grad_out)
    g_value = contract_first(hidden, d_value_rows)

    d_query_rows, dk_own, dk_pair = run_grads(
        info, query, d_attn, delta, k_own, k_pair, v_own, v_pair, probs
    )
    d_key_rows = reduce_to_owner(dk_own, dk_pair).astype(bf16)
    g_query = contract_first(hidden, d_query_rows)
    dhidden = (
        dot_nt(d_query_rows, w_query) + dot_nt(d_key_rows, w_key) + dot_nt(d_value_rows, w_value)
    )
    g_key = contract_first(hidden, d_key_rows)
    g_gain = jnp.sum(dhidden * normed, axis=0)
    scaled = dhidden * gain
    d_in = grad_out.astype(jnp.float32) + inv * (
        scaled - normed * jnp.mean(scaled * normed, axis=-1, keepdims=True)
    )

    rows = g_gain.shape[0] // count
    gain_rows = jnp.pad(g_gain.reshape(count, 1, rows), ((0, 0), (0, 7), (0, HS - rows)))
    late = jnp.concatenate([g_key.reshape(count, rows, HS), gain_rows], axis=1)
    late = reduce_weights(late.reshape(count * (rows + 8), HS))
    early = reduce_weights(jnp.concatenate([g_out, g_value], axis=1))
    d_q = reduce_weights(g_query)
    width = g_out.shape[1]
    return (
        d_in.astype(bf16)[None],
        d_q,
        late[:rows],
        early[:, width:],
        early[:, :width],
        late[rows, :rows],
    )


def solution(mesh):
    placed = (P("dp", "blk", None), P("dp", "blk", None), P(), P(), P(), P(), P(), P("dp"), P("dp"))
    return jax.shard_map(
        per_device,
        mesh=mesh,
        in_specs=placed,
        out_specs=(
            P("dp", "blk", None),
            P("blk", None),
            P("blk", None),
            P("blk", None),
            P("blk", None),
            P("blk"),
        ),
        check_vma=False,
    )
```

```python
import functools

import jax
import jax.numpy as jnp
from jax import lax
from jax.experimental import pallas as pl
from jax.experimental.pallas import tpu as pltpu
from jax.sharding import PartitionSpec as P

HS = 256
ACT = 64
BLOCK = 128
NEG = -1e30
EPS = 1e-06
LOG2E = 1.4426950408889634
VMEM_BYTES = 60 * 1024 * 1024
NT = (((1,), (1,)), ((), ()))


def dot_nt(a, b):
    return lax.dot_general(a, b, NT, preferred_element_type=jnp.float32)


def dot_nn(a, b):
    return jnp.dot(a, b, preferred_element_type=jnp.float32)


def block_state(info, chip, tok, seq):
    my, plen, edge = info[0], info[1], info[2]
    low = chip * (2 * tok)
    high = low + 2 * tok
    first, last = my * tok, my * tok + tok - 1
    seen = ((low < plen) | (high > seq - ACT)) & ((low < edge) | (low <= last))
    full = (high <= plen) & ((high <= edge) | (high - 1 <= first))
    return seen, full


def mask_of(info, chip, tok, seq):
    my, plen, edge, core = info[0], info[1], info[2], info[3]
    rows = lax.broadcasted_iota(jnp.int32, (2 * tok, tok), 0)
    k_pos = chip * (2 * tok) + (rows ^ (core * tok))
    q_pos = my * tok + lax.broadcasted_iota(jnp.int32, (2 * tok, tok), 1)
    key_ok = (k_pos < plen) | (k_pos >= seq - ACT)
    return key_ok & ((k_pos < edge) | (k_pos <= q_pos))


def per_block(info, chips, tok, seq, work, rest):
    def step(chip, carry):
        seen, full = block_state(info, chip, tok, seq)

        @pl.when(full)
        def _():
            work(chip, None)

        @pl.when(seen & jnp.logical_not(full))
        def _():
            work(chip, mask_of(info, chip, tok, seq))

        if rest is not None:

            @pl.when(jnp.logical_not(seen))
            def _():
                rest(chip)

        return carry

    lax.fori_loop(0, chips, step, 0)


def take_in(sources, scratch, sems, tok):
    copies = []
    for n, (own, pair, into) in enumerate(zip(sources[::2], sources[1::2], scratch)):
        copies.append(pltpu.make_async_copy(own, into.at[:, :tok, :], sems.at[2 * n]))
        copies.append(pltpu.make_async_copy(pair, into.at[:, tok:, :], sems.at[2 * n + 1]))
    for c in copies:
        c.start()
    return copies


def head(h):
    return pl.ds(h * HS, HS)


def scaled_scores(keys, q, h, mask):
    s = dot_nt(keys, q[:, head(h)]) * (HS ** (-0.5) * LOG2E)
    return s if mask is None else jnp.where(mask, s, NEG)


def stats_kernel(heads, seq, info, q, k_own, k_pair, lse, keys, top, total, sems):
    tok, chips = q.shape[0], k_own.shape[0]
    copies = take_in((k_own, k_pair), (keys,), sems, tok)
    top[...] = jnp.full(top.shape, NEG, jnp.float32)
    total[...] = jnp.zeros(total.shape, jnp.float32)
    for c in copies:
        c.wait()

    def work(chip, mask):
        for h in range(heads):
            s = scaled_scores(keys[chip], q, h, mask)
            old = top[:, head(h)]
            new = jnp.maximum(old, jnp.max(s, axis=0, keepdims=True))
            top[:, head(h)] = new
            total[:, head(h)] = total[:, head(h)] * jnp.exp2(old - new) + jnp.sum(
                jnp.exp2(s - new), axis=0, keepdims=True
            )

    per_block(info, chips, tok, seq, work, None)
    lse[...] = top[...] + jnp.log(total[...]) * LOG2E


def attend_kernel(
    heads, seq, info, q, da, lse, k_own, k_pair, v_own, v_pair,
    at_own, at_pair, delta, dv_own, dv_pair, probs_out,
    keys, values, values_t, da_rows, probs, sems, out_sems,
):
    tok, chips = q.shape[0], k_own.shape[0]
    wide = 2 * tok
    copies = take_in((k_own, k_pair, v_own, v_pair), (keys, values), sems, tok)
    for h in range(heads):
        da_rows[head(h), :] = da[:, head(h)]
    for c in copies:
        c.wait()
    for chip in range(chips):
        values_t[:, pl.ds(chip * wide, wide)] = values[chip].T

    def out_copy(chip):
        rows = pl.ds(pl.multiple_of(chip * wide, wide), wide)
        return pltpu.make_async_copy(probs.at[rows, :], probs_out.at[rows, :], out_sems.at[chip])

    def work(chip, mask):
        rows = pl.ds(pl.multiple_of(chip * wide, wide), wide)
        for h in range(heads):
            s = scaled_scores(keys[chip], q, h, mask)
            probs[rows, head(h)] = jnp.exp2(s - lse[:, head(h)]).astype(jnp.bfloat16)
        dv = dot_nn(probs[rows, :], da_rows[...]).astype(jnp.bfloat16)
        dv_own[chip] = dv[:tok]
        dv_pair[chip] = dv[tok:]
        out_copy(chip).start()

    def rest(chip):
        rows = pl.ds(pl.multiple_of(chip * wide, wide), wide)
        probs[rows, :] = jnp.zeros((wide, heads * HS), jnp.bfloat16)
        dv_own[chip] = jnp.zeros((tok, HS), jnp.bfloat16)
        dv_pair[chip] = jnp.zeros((tok, HS), jnp.bfloat16)
        out_copy(chip).start()

    per_block(info, chips, tok, seq, work, rest)
    for h in range(heads):
        a = dot_nn(values_t[...], probs[:, head(h)]).astype(jnp.bfloat16)
        per_head = at_own.shape[2] // heads
        block = HS // per_head
        for n in range(per_head):
            put_rows(
                info, a[n * block : (n + 1) * block].astype(jnp.float32), h * per_head + n, at_own, at_pair
            )
        delta[:, head(h)] = jnp.sum(
            a.astype(jnp.float32) * da_rows[head(h), :].T.astype(jnp.float32), axis=0, keepdims=True
        )
    lax.fori_loop(0, chips, lambda chip, c: (out_copy(chip).wait(), c)[1], 0)


def grads_kernel(
    heads, seq, info, q, da, delta, k_own, k_pair, v_own, v_pair, probs_in,
    dq, dk_own, dk_pair,
    keys, values, keys_t, q_rows, probs, dscores, sems, in_sems,
):
    tok, chips = q.shape[0], k_own.shape[0]
    wide = 2 * tok
    copies = take_in((k_own, k_pair, v_own, v_pair), (keys, values), sems, tok)

    def in_copy(chip):
        rows = pl.ds(pl.multiple_of(chip * wide, wide), wide)
        return pltpu.make_async_copy(probs_in.at[rows, :], probs.at[rows, :], in_sems.at[chip])

    lax.fori_loop(0, chips, lambda chip, c: (in_copy(chip).start(), c)[1], 0)
    for h in range(heads):
        q_rows[head(h), :] = q[:, head(h)]
    for c in copies:
        c.wait()
    for chip in range(chips):
        keys_t[:, pl.ds(chip * wide, wide)] = keys[chip].T

    def step(chip, carry):
        rows = pl.ds(pl.multiple_of(chip * wide, wide), wide)
        in_copy(chip).wait()
        seen, _ = block_state(info, chip, tok, seq)

        @pl.when(seen)
        def _():
            for h in range(heads):
                dp = dot_nt(values[chip], da[:, head(h)])
                p = probs[rows, head(h)].astype(jnp.float32)
                dscores[rows, head(h)] = (p * (dp - delta[:, head(h)])).astype(jnp.bfloat16)
            dk = (dot_nn(dscores[rows, :], q_rows[...]) * HS ** (-0.5)).astype(jnp.bfloat16)
            dk_own[chip] = dk[:tok]
            dk_pair[chip] = dk[tok:]

        @pl.when(jnp.logical_not(seen))
        def _():
            dscores[rows, :] = jnp.zeros((wide, heads * HS), jnp.bfloat16)
            dk_own[chip] = jnp.zeros((tok, HS), jnp.bfloat16)
            dk_pair[chip] = jnp.zeros((tok, HS), jnp.bfloat16)

        return carry

    lax.fori_loop(0, chips, step, 0)
    for h in range(heads):
        d = dot_nn(keys_t[...], dscores[:, head(h)]) * HS ** (-0.5)
        dq[:, head(h)] = d.T.astype(jnp.bfloat16)


SMEM = pl.BlockSpec(memory_space=pltpu.SMEM)
VMEM = pl.BlockSpec(memory_space=pltpu.VMEM)
ANY = pl.BlockSpec(memory_space=pl.ANY)


def params():
    return pltpu.CompilerParams(vmem_limit_bytes=VMEM_BYTES)


def cost(flops, elements):
    return pl.CostEstimate(flops=flops, bytes_accessed=2 * elements, transcendentals=elements)


def run_stats(info, q, k_own, k_pair):
    tok, width = q.shape
    heads, chips = width // HS, k_own.shape[0]
    seq = 2 * tok * chips
    return pl.pallas_call(
        functools.partial(stats_kernel, heads, seq),
        out_shape=jax.ShapeDtypeStruct((1, width), jnp.float32),
        in_specs=[SMEM, VMEM, ANY, ANY],
        out_specs=VMEM,
        scratch_shapes=[
            pltpu.VMEM((chips, 2 * tok, HS), jnp.bfloat16),
            pltpu.VMEM((1, width), jnp.float32),
            pltpu.VMEM((1, width), jnp.float32),
            pltpu.SemaphoreType.DMA((2,)),
        ],
        compiler_params=params(),
        cost_estimate=cost(2 * seq * width * HS, seq * width),
        name="stats",
    )(info, q, k_own, k_pair)


def run_attend(info, q, da, lse, k_own, k_pair, v_own, v_pair, filed):
    tok, width = q.shape
    heads, chips = width // HS, k_own.shape[0]
    seq = 2 * tok * chips
    part = jax.ShapeDtypeStruct((chips, tok, HS), jnp.bfloat16)
    return pl.pallas_call(
        functools.partial(attend_kernel, heads, seq),
        out_shape=(
            filed,
            filed,
            jax.ShapeDtypeStruct((1, width), jnp.float32),
            part,
            part,
            jax.ShapeDtypeStruct((seq, width), jnp.bfloat16),
        ),
        in_specs=[SMEM, VMEM, VMEM, VMEM, ANY, ANY, ANY, ANY],
        out_specs=(VMEM, VMEM, VMEM, VMEM, VMEM, ANY),
        scratch_shapes=[
            pltpu.VMEM((chips, 2 * tok, HS), jnp.bfloat16),
            pltpu.VMEM((chips, 2 * tok, HS), jnp.bfloat16),
            pltpu.VMEM((HS, seq), jnp.bfloat16),
            pltpu.VMEM((width, HS), jnp.bfloat16),
            pltpu.VMEM((seq, width), jnp.bfloat16),
            pltpu.SemaphoreType.DMA((4,)),
            pltpu.SemaphoreType.DMA((chips,)),
        ],
        compiler_params=params(),
        cost_estimate=cost(6 * seq * width * HS, seq * width),
        name="attend",
    )(info, q, da, lse, k_own, k_pair, v_own, v_pair)


def run_grads(info, q, da, delta, k_own, k_pair, v_own, v_pair, probs):
    tok, width = q.shape
    heads, chips = width // HS, k_own.shape[0]
    seq = 2 * tok * chips
    part = jax.ShapeDtypeStruct((chips, tok, HS), jnp.bfloat16)
    return pl.pallas_call(
        functools.partial(grads_kernel, heads, seq),
        out_shape=(jax.ShapeDtypeStruct((tok, width), jnp.bfloat16), part, part),
        in_specs=[SMEM, VMEM, VMEM, VMEM, ANY, ANY, ANY, ANY, ANY],
        out_specs=(VMEM, VMEM, VMEM),
        scratch_shapes=[
            pltpu.VMEM((chips, 2 * tok, HS), jnp.bfloat16),
            pltpu.VMEM((chips, 2 * tok, HS), jnp.bfloat16),
            pltpu.VMEM((HS, seq), jnp.bfloat16),
            pltpu.VMEM((width, HS), jnp.bfloat16),
            pltpu.VMEM((seq, width), jnp.bfloat16),
            pltpu.VMEM((seq, width), jnp.bfloat16),
            pltpu.SemaphoreType.DMA((4,)),
            pltpu.SemaphoreType.DMA((chips,)),
        ],
        compiler_params=params(),
        cost_estimate=cost(6 * seq * width * HS, seq * width),
        name="grads",
    )(info, q, da, delta, k_own, k_pair, v_own, v_pair, probs)


def normed_rows(x):
    xf = x[...].astype(jnp.float32)
    return xf * lax.rsqrt(jnp.mean(xf * xf, axis=-1, keepdims=True) + EPS)


def prepare_kernel(chips, x, gain, w_key, w_value, hidden, k_copies, v_copies):
    h = (normed_rows(x) * gain[...]).astype(jnp.bfloat16)
    hidden[...] = h
    for weight, out in ((w_key, k_copies), (w_value, v_copies)):
        rows = dot_nn(h, weight[...]).astype(jnp.bfloat16)
        for chip in range(chips):
            out[chip] = rows


def put_rows(info, rows, chip, own, pair):
    core, x = info[3], info[4]
    steps, outer, _, size, _ = own.shape

    def put(same):
        for n in range(rows.shape[0] // size):
            place = n % (outer * steps)
            to = own if (n // (outer * steps)) == same else pair
            step = (place % steps - x + steps) & (steps - 1)
            to[step, place // steps, chip] = rows[n * size : (n + 1) * size].astype(to.dtype)

    for same in range(2):
        pl.when(core == same)(functools.partial(put, same))


def project_kernel(info, hidden, grad_out, w_query, w_out, query, d_attn, ht_own, ht_pair):
    h = hidden[...]
    query[...] = dot_nn(h, w_query[...]).astype(jnp.bfloat16)
    d_attn[...] = dot_nt(grad_out[...], w_out[...]).astype(jnp.bfloat16)
    chips = ht_own.shape[2]
    block = h.shape[1] // chips
    for chip in range(chips):
        part = h[:, chip * block : (chip + 1) * block].astype(jnp.float32).T
        put_rows(info, part, chip, ht_own, ht_pair)


def own_terms_kernel(left, right, received, base, *parts):
    rows = base.shape[0]
    for step in range(len(parts) + 1):
        at = pl.ds(step * rows, rows)
        total = dot_nn(left[step].reshape(rows, -1), right[...]) + received[at, :].astype(jnp.float32)
        if step == 0:
            base[...] = total
        else:
            parts[step - 1][...] = total.astype(jnp.bfloat16)


def collect_kernel(counts, *refs):
    out, at = refs[-1], 0
    for base, *parts in counts:
        total = refs[base][...]
        for p in parts:
            total = total + refs[p][...].astype(jnp.float32)
        wide = total.shape[1]
        out[:, pl.ds(at, wide)] = total.astype(jnp.bfloat16)
        at += wide


def add_kernel(a, b, out):
    out[...] = (a[...].astype(jnp.float32) + b[...].astype(jnp.float32)).astype(out.dtype)


def finish_kernel(x, grad_out, gain, dq, dk, dv, w_query, w_key, w_value, d_in):
    dhidden = (
        dot_nt(dq[...], w_query[...]) + dot_nt(dk[...], w_key[...]) + dot_nt(dv[...], w_value[...])
    )
    xf = x[...].astype(jnp.float32)
    inv = lax.rsqrt(jnp.mean(xf * xf, axis=-1, keepdims=True) + EPS)
    normed = xf * inv
    scaled = dhidden * gain[...]
    mean = jnp.mean(scaled * normed, axis=-1, keepdims=True)
    d_in[...] = (grad_out[...].astype(jnp.float32) + inv * (scaled - normed * mean)).astype(d_in.dtype)


def call(body, outs, args, flops, smem=0):
    return pl.pallas_call(
        body,
        out_shape=outs,
        in_specs=[SMEM] * smem + [VMEM] * (len(args) - smem),
        out_specs=jax.tree.map(lambda _: VMEM, outs),
        compiler_params=params(),
        cost_estimate=cost(flops, 1 << 20),
    )(*args)


def shape(*dims, dtype=jnp.bfloat16):
    return jax.ShapeDtypeStruct(dims, dtype)


def run_add(a, b):
    spec = pl.BlockSpec((2, *a.shape[1:]), lambda i: (i, 0, 0))
    return pl.pallas_call(
        add_kernel,
        grid=(a.shape[0] // 2,),
        out_shape=jax.ShapeDtypeStruct(a.shape, a.dtype),
        in_specs=[spec, spec],
        out_specs=spec,
        cost_estimate=cost(1 << 30, 1 << 20),
        name="add",
    )(a, b)


CORES = 2
X = 4


def as_bf16(value):
    return value.astype(jnp.bfloat16)


def swap_cores(value):
    count = lax.axis_size("blk")
    return lax.ppermute(value, "blk", [(i, i ^ 1) for i in range(count)])


def send_along_x(value, step):
    count = lax.axis_size("dp")
    return lax.ppermute(
        value, "dp", [(i, i // X * X + (i + step) % X) for i in range(count)]
    )


def exchange_chips(value):
    chips = lax.axis_size("blk") // CORES
    groups = [[core + CORES * chip for chip in range(chips)] for core in range(CORES)]
    return lax.all_to_all(value, "blk", 0, 0, tiled=True, axis_index_groups=groups)


def exchange_plane(value):
    blk, dp = lax.axis_size("blk"), lax.axis_size("dp")
    groups = [
        [(outer * X + x) * blk + chip * CORES + core for outer in range(dp // X) for chip in range(blk // CORES)]
        for x in range(X)
        for core in range(CORES)
    ]
    return lax.all_to_all(value, ("dp", "blk"), 0, 0, tiled=True, axis_index_groups=groups)


def sum_first(parts):
    return jnp.sum(parts.astype(jnp.float32), axis=0)


def plane_terms(left_own, left_pair, right):
    steps, outer, chips, size, tok = left_pair.shape
    rows, wide = outer * chips * size, right.shape[1]
    received = swap_cores(as_bf16(dot_nn(left_pair.reshape(steps * rows, tok), right)))
    base, *parts = call(
        own_terms_kernel,
        (shape(rows, wide, dtype=jnp.float32), *[shape(rows, wide)] * (steps - 1)),
        (left_own, right, received),
        2 * steps * rows * wide * tok,
    )
    arrived = []
    for step, part in enumerate(parts, 1):
        arrived.append(send_along_x(part, step))
    return (base, *arrived)


def to_owner(own, pair):
    received = swap_cores(pair)
    chip_sum = run_add(own, received)
    parts = exchange_chips(chip_sum)
    return as_bf16(sum_first(parts))


def per_device(inputs, upstream, gain, w_query, w_key, w_value, w_out, prefix_len, bound):
    return whole(inputs[0], upstream[0], gain, w_query, w_key, w_value, w_out, prefix_len, bound)


def whole(inputs, grad_out, gain, w_query, w_key, w_value, w_out, prefix_len, bound):
    tok, wide = inputs.shape
    my, dp = lax.axis_index("blk"), lax.axis_index("dp")
    count = lax.axis_size("blk")
    chips, outer = count // CORES, lax.axis_size("dp") // X
    core, x = my % CORES, dp % X
    info = jnp.stack([my, prefix_len[0], bound[0] * BLOCK, core, x]).astype(jnp.int32)
    gain_row = gain.reshape(1, wide)
    filed = shape(X, outer, chips, wide // (count * outer * X), tok)
    copies = shape(chips, tok, HS)
    hidden, k_copies, v_copies = call(
        functools.partial(prepare_kernel, chips),
        (shape(tok, wide), copies, copies),
        (inputs, gain_row, w_key, w_value),
        4 * tok * wide * HS,
    )
    k_own = exchange_chips(k_copies)
    k_pair = swap_cores(k_own)
    v_own = exchange_chips(v_copies)
    v_pair = swap_cores(v_own)
    query, d_attn, ht_own, ht_pair = call(
        project_kernel,
        (shape(tok, w_query.shape[1]), shape(tok, w_out.shape[0]), filed, filed),
        (info, hidden, grad_out, w_query, w_out),
        4 * tok * wide * wide,
        smem=1,
    )
    lse = run_stats(info, query, k_own, k_pair)
    at_own, at_pair, delta, dv_own, dv_pair, probs = run_attend(
        info, query, d_attn, lse, k_own, k_pair, v_own, v_pair, filed
    )
    d_value_rows = to_owner(dv_own, dv_pair)
    out_terms = plane_terms(at_own, at_pair, grad_out)
    d_query_rows, dk_own, dk_pair = run_grads(
        info, query, d_attn, delta, k_own, k_pair, v_own, v_pair, probs
    )
    d_key_rows = to_owner(dk_own, dk_pair)
    query_terms = plane_terms(ht_own, ht_pair, d_query_rows)
    d_kv_rows = jnp.concatenate([d_key_rows, d_value_rows], axis=1)
    kv_terms = plane_terms(ht_own, ht_pair, d_kv_rows)
    sets, at = [], 0
    for terms in (out_terms, query_terms, kv_terms):
        sets.append(list(range(at, at + len(terms))))
        at += len(terms)
    rows = out_terms[0].shape[0]
    total_wide = sum(t[0].shape[1] for t in (out_terms, query_terms, kv_terms))
    mine = call(
        functools.partial(collect_kernel, sets),
        shape(rows, total_wide),
        (*out_terms, *query_terms, *kv_terms),
        1 << 30,
    )
    parts = exchange_plane(mine.reshape(outer * chips, -1, total_wide))
    summed = as_bf16(sum_first(parts))
    copies = jnp.broadcast_to(summed, (lax.axis_size("dp"), *summed.shape))
    shared = lax.all_to_all(copies, "dp", 0, 0, tiled=True)
    ends = [wide, wide + query.shape[1], wide + query.shape[1] + HS]
    shared = shared.reshape(-1, total_wide).astype(jnp.float32)
    d_out, d_query, d_key, d_value = jnp.split(shared, ends, axis=1)
    d_in = call(
        finish_kernel,
        shape(tok, wide),
        (inputs, grad_out, gain_row, d_query_rows, d_key_rows, d_value_rows, w_query, w_key, w_value),
        2 * tok * wide * (wide + 2 * HS),
    )

    rows = d_query.shape[0]

    def my_rows(value):
        return lax.dynamic_slice_in_dim(value, my * rows, rows, 0).astype(jnp.float32)

    d_gain = (
        jnp.sum(my_rows(w_query) * d_query, axis=1)
        + jnp.sum(my_rows(w_key) * d_key, axis=1)
        + jnp.sum(my_rows(w_value) * d_value, axis=1)
    ) / my_rows(gain)
    return (d_in[None], d_query, d_key, d_value, d_out, d_gain)


def solution(mesh):
    placed = (P("dp", "blk", None), P("dp", "blk", None), P(), P(), P(), P(), P(), P("dp"), P("dp"))
    return jax.shard_map(
        per_device,
        mesh=mesh,
        in_specs=placed,
        out_specs=(
            P("dp", "blk", None),
            P("blk", None),
            P("blk", None),
            P("blk", None),
            P("blk", None),
            P("blk"),
        ),
        check_vma=False,
    )
```

```python
import functools

import jax
import jax.numpy as jnp
from jax import lax
from jax.experimental import pallas as pl
from jax.experimental.pallas import tpu as pltpu
from jax.sharding import PartitionSpec as P

HS = 256
ACT = 64
BLOCK = 128
NEG = -1e30
EPS = 1e-06
LOG2E = 1.4426950408889634
VMEM_BYTES = 67043328
NT = (((1,), (1,)), ((), ()))


def dot_nt(a, b):
    return lax.dot_general(a, b, NT, preferred_element_type=jnp.float32)


def dot_nn(a, b):
    return jnp.dot(a, b, preferred_element_type=jnp.float32)


def head(h):
    return pl.ds(h * HS, HS)


def part(half, h, heads):
    return pl.ds((half * heads + h) * HS, HS)


def block_state(info, chip, half, tok, seq):
    rows, plen, edge, core = info[0] ^ half, info[1], info[2], info[3]
    low = (chip * 2 + core) * tok
    high = low + tok
    first, last = rows * tok, rows * tok + tok - 1
    seen = ((low < plen) | (high > seq - ACT)) & ((low < edge) | (low <= last))
    full = (high <= plen) & ((high <= edge) | (high - 1 <= first))
    return seen, full


def mask_of(info, chip, half, tok, seq):
    rows, plen, edge, core = info[0] ^ half, info[1], info[2], info[3]
    k_pos = (chip * 2 + core) * tok + lax.broadcasted_iota(jnp.int32, (tok, tok), 0)
    q_pos = rows * tok + lax.broadcasted_iota(jnp.int32, (tok, tok), 1)
    key_ok = (k_pos < plen) | (k_pos >= seq - ACT)
    return key_ok & ((k_pos < edge) | (k_pos <= q_pos))


def when_seen(info, chip, half, tok, seq, work, rest):
    seen, full = block_state(info, chip, half, tok, seq)

    @pl.when(full)
    def _():
        work(None)

    @pl.when(seen & jnp.logical_not(full))
    def _():
        work(mask_of(info, chip, half, tok, seq))

    if rest is not None:
        pl.when(jnp.logical_not(seen))(rest)


def each_chip(chips, step):
    def body(chip, carry):
        step(chip)
        return carry

    lax.fori_loop(0, chips, body, 0)


def scaled_scores(keys, q, h, mask):
    s = dot_nt(keys, q[0, :, head(h)]) * (HS ** (-0.5) * LOG2E)
    return s if mask is None else jnp.where(mask, s, NEG)


def stats_kernel(heads, seq, info, own, pair, keys, out, top, total):
    chips, tok, _ = keys.shape
    top[...] = jnp.full(top.shape, NEG, jnp.float32)
    total[...] = jnp.zeros(total.shape, jnp.float32)

    def step(chip):
        for half, q in enumerate((own, pair)):

            def work(mask, half=half, q=q):
                for h in range(heads):
                    at = part(half, h, heads)
                    s = scaled_scores(keys[chip], q, h, mask)
                    old = top[:, at]
                    new = jnp.maximum(old, jnp.max(s, axis=0, keepdims=True))
                    top[:, at] = new
                    total[:, at] = total[:, at] * jnp.exp2(old - new) + jnp.sum(
                        jnp.exp2(s - new), axis=0, keepdims=True
                    )

            when_seen(info, chip, half, tok, seq, work, None)

    each_chip(chips, step)
    wide = heads * HS
    for half in range(2):
        out[half, 0:1, :] = top[:, pl.ds(half * wide, wide)]
        out[half, 1:2, :] = total[:, pl.ds(half * wide, wide)]


def attend_kernel(
    heads, seq, info, own, pair, mine, other, keys, values,
    attn, dv, probs_out,
    values_t, da_rows, probs, lse, out_sems,
):
    chips, tok, _ = keys.shape
    wide = heads * HS
    for half, qd in enumerate((own, pair)):
        for h in range(heads):
            da_rows[part(half, h, heads), :] = qd[1, :, head(h)]
        top_a, top_b = mine[half, 0:1, :], other[1 - half, 0:1, :]
        top = jnp.maximum(top_a, top_b)
        total = mine[half, 1:2, :] * jnp.exp2(top_a - top)
        total = total + other[1 - half, 1:2, :] * jnp.exp2(top_b - top)
        lse[:, pl.ds(half * wide, wide)] = top + jnp.log(total) * LOG2E
    for chip in range(chips):
        values_t[:, pl.ds(chip * tok, tok)] = values[chip].T

    def rows_of(chip):
        return pl.ds(pl.multiple_of(chip * tok, tok), tok)

    def out_copy(chip):
        rows = rows_of(chip)
        return pltpu.make_async_copy(probs.at[rows, :], probs_out.at[rows, :], out_sems.at[chip])

    def step(chip):
        rows = rows_of(chip)
        for half, q in enumerate((own, pair)):

            def work(mask, half=half, q=q):
                for h in range(heads):
                    at = part(half, h, heads)
                    s = scaled_scores(keys[chip], q, h, mask)
                    probs[rows, at] = jnp.exp2(s - lse[:, at]).astype(jnp.bfloat16)

            def rest(half=half):
                probs[rows, pl.ds(half * wide, wide)] = jnp.zeros((tok, wide), jnp.bfloat16)

            when_seen(info, chip, half, tok, seq, work, rest)
        dv[chip] = dot_nn(probs[rows, :], da_rows[...]).astype(jnp.bfloat16)
        out_copy(chip).start()

    each_chip(chips, step)
    for half in range(2):
        for h in range(heads):
            attn[half, head(h), :] = dot_nn(values_t[...], probs[:, part(half, h, heads)]).astype(
                jnp.bfloat16
            )
    each_chip(chips, lambda chip: out_copy(chip).wait())


def put_rows(info, rows, chip, own, pair):
    core, x = info[3], info[4]
    steps, outer, _, size, _ = own.shape

    def put(same):
        for n in range(rows.shape[0] // size):
            place = n % (outer * steps)
            to = own if (n // (outer * steps)) == same else pair
            step = (place % steps - x + steps) & (steps - 1)
            to[step, place // steps, chip] = rows[n * size : (n + 1) * size].astype(to.dtype)

    for same in range(2):
        pl.when(core == same)(functools.partial(put, same))


def grads_kernel(
    heads, seq, info, own, pair, mine, other, keys, values, probs_in,
    at_own, at_pair, dk, dq_own, dq_pair,
    keys_t, q_rows, probs, dscores, delta, in_sems,
):
    chips, tok, _ = keys.shape

    def rows_of(chip):
        return pl.ds(pl.multiple_of(chip * tok, tok), tok)

    def in_copy(chip):
        rows = rows_of(chip)
        return pltpu.make_async_copy(probs_in.at[rows, :], probs.at[rows, :], in_sems.at[chip])

    each_chip(chips, lambda chip: in_copy(chip).start())
    per_head = chips // heads
    block = HS // per_head
    for half, qd in enumerate((own, pair)):
        for h in range(heads):
            at = part(half, h, heads)
            q_rows[at, :] = qd[0, :, head(h)]
            both = mine[half, head(h), :].astype(jnp.float32) + other[1 - half, head(h), :].astype(
                jnp.float32
            )
            a = both.astype(jnp.bfloat16).astype(jnp.float32)
            delta[:, at] = jnp.sum(
                a * qd[1, :, head(h)].T.astype(jnp.float32), axis=0, keepdims=True
            )
            if half == 0:
                for n in range(per_head):
                    put_rows(info, a[n * block : (n + 1) * block], h * per_head + n, at_own, at_pair)
    for chip in range(chips):
        keys_t[:, pl.ds(chip * tok, tok)] = keys[chip].T

    def step(chip):
        rows = rows_of(chip)
        in_copy(chip).wait()
        for half, qd in enumerate((own, pair)):
            seen, _ = block_state(info, chip, half, tok, seq)

            @pl.when(seen)
            def _(half=half, qd=qd):
                for h in range(heads):
                    at = part(half, h, heads)
                    dp = dot_nt(values[chip], qd[1, :, head(h)])
                    p = probs[rows, at].astype(jnp.float32)
                    dscores[rows, at] = (p * (dp - delta[:, at])).astype(jnp.bfloat16)

            @pl.when(jnp.logical_not(seen))
            def _(half=half):
                wide = heads * HS
                dscores[rows, pl.ds(half * wide, wide)] = jnp.zeros((tok, wide), jnp.bfloat16)

        dk[chip] = (dot_nn(dscores[rows, :], q_rows[...]) * HS ** (-0.5)).astype(jnp.bfloat16)

    each_chip(chips, step)
    for half, dq in enumerate((dq_own, dq_pair)):
        for h in range(heads):
            d = dot_nn(keys_t[...], dscores[:, part(half, h, heads)]) * HS ** (-0.5)
            dq[:, head(h)] = d.T.astype(jnp.bfloat16)


def prepare_kernel(chips, x, gain, w_key, w_value, hidden, k_copies, v_copies):
    xf = x[...].astype(jnp.float32)
    inv = lax.rsqrt(jnp.mean(xf * xf, axis=-1, keepdims=True) + EPS)
    h = (xf * inv * gain[...]).astype(jnp.bfloat16)
    hidden[...] = h
    for weight, out in ((w_key, k_copies), (w_value, v_copies)):
        rows = dot_nn(h, weight[...]).astype(jnp.bfloat16)
        for chip in range(chips):
            out[chip] = rows


def project_kernel(info, hidden, grad_out, w_query, w_out, both, ht_own, ht_pair):
    h = hidden[...]
    both[0] = dot_nn(h, w_query[...]).astype(jnp.bfloat16)
    both[1] = dot_nt(grad_out[...], w_out[...]).astype(jnp.bfloat16)
    chips = ht_own.shape[2]
    block = h.shape[1] // chips
    for chip in range(chips):
        rows = h[:, chip * block : (chip + 1) * block].astype(jnp.float32).T
        put_rows(info, rows, chip, ht_own, ht_pair)


def step_terms(left, step, right, received):
    rows = left.shape[1] * left.shape[2] * left.shape[3]
    own = dot_nn(left[step].reshape(rows, -1), right)
    return own + received[pl.ds(step * rows, rows), :].astype(jnp.float32)


def own_terms_kernel(left, right, received, base, *parts):
    for step, out in enumerate((base, *parts)):
        out[...] = step_terms(left, step, right[...], received).astype(out.dtype)


def direct_terms(info, left, right, received, out, at):
    wide, steps = right.shape[1], left.shape[0]
    for step in range(steps):
        place = (info[4] + step) & (steps - 1)
        to = pl.ds(pl.multiple_of(at + place * wide, 128), wide)
        out[:, to] = step_terms(left, step, right[...], received).astype(out.dtype)


def direct_kernel(info, left, right, received, out):
    direct_terms(info, left, right, received, out, 0)


def collect_kernel(info, base, one, two, three, query_terms, left, right, received, out):
    total = base[...]
    for arrived in (one, two, three):
        total = total + arrived[...].astype(jnp.float32)
    wide = total.shape[1]
    out[:, pl.ds(0, wide)] = total.astype(out.dtype)
    out[:, pl.ds(wide, query_terms.shape[1])] = query_terms[...]
    direct_terms(info, left, right, received, out, wide + query_terms.shape[1])


def spread_kernel(parts, out):
    total = parts[0].astype(jnp.float32)
    for n in range(1, parts.shape[0]):
        total = total + parts[n].astype(jnp.float32)
    total = total.astype(out.dtype)
    for n in range(out.shape[0]):
        out[n] = total


def weights_kernel(steps, shared, w_query, w_key, w_value, gain, d_query, d_key, d_value, d_out, d_gain):
    size = shared.shape[1]
    wide, heads_wide = d_out.shape[1], d_query.shape[1]
    gains = []
    for place in range(shared.shape[0]):
        outer, x = place // steps, place % steps
        rows = slice(place * size, (place + 1) * size)
        d_out[rows, :] = shared[place, :, pl.ds(0, wide)].astype(jnp.float32)

        def added(at, width):
            total = 0.0
            for source in range(steps):
                total = total + shared[outer * steps + source, :, pl.ds(at, width)].astype(jnp.float32)
            return total

        query = added(wide + x * heads_wide, heads_wide)
        kv = added(wide + steps * heads_wide + x * 2 * HS, 2 * HS)
        d_query[rows, :] = query
        d_key[rows, :] = kv[:, :HS]
        d_value[rows, :] = kv[:, HS:]
        row_sum = (
            jnp.sum(w_query[rows, :].astype(jnp.float32) * query, axis=1, keepdims=True)
            + jnp.sum(w_key[rows, :].astype(jnp.float32) * kv[:, :HS], axis=1, keepdims=True)
            + jnp.sum(w_value[rows, :].astype(jnp.float32) * kv[:, HS:], axis=1, keepdims=True)
        )
        gains.append(jnp.broadcast_to(row_sum, (size, 128)))
    d_gain[...] = jnp.concatenate(gains, axis=0).T[0:1, :] / gain[...]


def finish_kernel(x, grad_out, gain, dq, dkv, w_query, w_key, w_value, d_in):
    dhidden = (
        dot_nt(dq[...], w_query[...])
        + dot_nt(dkv[:, :HS], w_key[...])
        + dot_nt(dkv[:, HS:], w_value[...])
    )
    xf = x[...].astype(jnp.float32)
    inv = lax.rsqrt(jnp.mean(xf * xf, axis=-1, keepdims=True) + EPS)
    normed = xf * inv
    scaled = dhidden * gain[...]
    mean = jnp.mean(scaled * normed, axis=-1, keepdims=True)
    d_in[...] = (grad_out[...].astype(jnp.float32) + inv * (scaled - normed * mean)).astype(d_in.dtype)


SMEM = pl.BlockSpec(memory_space=pltpu.SMEM)
VMEM = pl.BlockSpec(memory_space=pltpu.VMEM)
ANY = pl.BlockSpec(memory_space=pl.ANY)


def shape(*dims, dtype=jnp.bfloat16):
    return jax.ShapeDtypeStruct(dims, dtype)


def call(body, outs, args, flops, smem=0, scratch=(), in_any=(), out_any=()):
    specs = [SMEM if n < smem else ANY if n in in_any else VMEM for n in range(len(args))]
    if isinstance(outs, tuple):
        out_specs = tuple(ANY if n in out_any else VMEM for n in range(len(outs)))
    else:
        out_specs = VMEM
    return pl.pallas_call(
        body,
        out_shape=outs,
        in_specs=specs,
        out_specs=out_specs,
        scratch_shapes=list(scratch),
        compiler_params=pltpu.CompilerParams(vmem_limit_bytes=VMEM_BYTES),
        cost_estimate=pl.CostEstimate(flops=flops, bytes_accessed=1 << 20, transcendentals=0),
    )(*args)


def scratch(*dims, dtype=jnp.bfloat16):
    return pltpu.VMEM(dims, dtype)


def run_stats(info, own, pair, keys):
    _, tok, wide = own.shape
    chips, heads = keys.shape[0], wide // HS
    seq = 2 * tok * chips
    rows = scratch(1, 2 * wide, dtype=jnp.float32)
    return call(
        functools.partial(stats_kernel, heads, seq),
        shape(2, 2, wide, dtype=jnp.float32),
        (info, own, pair, keys),
        2 * seq * wide * HS,
        smem=1,
        scratch=(rows, rows),
    )


def run_attend(info, own, pair, mine, other, keys, values):
    _, tok, wide = own.shape
    chips, heads = keys.shape[0], wide // HS
    seq = 2 * tok * chips
    return call(
        functools.partial(attend_kernel, heads, seq),
        (shape(2, wide, tok), shape(chips, tok, HS), shape(chips * tok, 2 * wide)),
        (info, own, pair, mine, other, keys, values),
        6 * seq * wide * HS,
        smem=1,
        out_any=(2,),
        scratch=(
            scratch(HS, chips * tok),
            scratch(2 * wide, HS),
            scratch(chips * tok, 2 * wide),
            scratch(1, 2 * wide, dtype=jnp.float32),
            pltpu.SemaphoreType.DMA((chips,)),
        ),
    )


def run_grads(info, own, pair, mine, other, keys, values, probs, filed):
    _, tok, wide = own.shape
    chips, heads = keys.shape[0], wide // HS
    seq = 2 * tok * chips
    return call(
        functools.partial(grads_kernel, heads, seq),
        (filed, filed, shape(chips, tok, HS), shape(tok, wide), shape(tok, wide)),
        (info, own, pair, mine, other, keys, values, probs),
        6 * seq * wide * HS,
        smem=1,
        in_any=(7,),
        scratch=(
            scratch(HS, chips * tok),
            scratch(2 * wide, HS),
            scratch(chips * tok, 2 * wide),
            scratch(chips * tok, 2 * wide),
            scratch(1, 2 * wide, dtype=jnp.float32),
            pltpu.SemaphoreType.DMA((chips,)),
        ),
    )


CORES = 2
X = 4


def as_bf16(value):
    return value.astype(jnp.bfloat16)


def swap_cores(value):
    count = lax.axis_size("blk")
    return lax.ppermute(value, "blk", [(i, i ^ 1) for i in range(count)])


def send_along_x(value, step):
    count = lax.axis_size("dp")
    return lax.ppermute(
        value, "dp", [(i, i // X * X + (i + step) % X) for i in range(count)]
    )


def exchange_chips(value):
    chips = lax.axis_size("blk") // CORES
    groups = [[core + CORES * chip for chip in range(chips)] for core in range(CORES)]
    return lax.all_to_all(value, "blk", 0, 0, tiled=True, axis_index_groups=groups)


def exchange_plane(value):
    blk, dp = lax.axis_size("blk"), lax.axis_size("dp")
    groups = [
        [(outer * X + x) * blk + chip * CORES + core for outer in range(dp // X) for chip in range(blk // CORES)]
        for x in range(X)
        for core in range(CORES)
    ]
    return lax.all_to_all(value, ("dp", "blk"), 0, 0, tiled=True, axis_index_groups=groups)


def sum_first(parts):
    return as_bf16(jnp.sum(parts.astype(jnp.float32), axis=0))


def pair_terms(left_pair, right):
    terms = as_bf16(dot_nn(left_pair.reshape(-1, left_pair.shape[-1]), right))
    return swap_cores(terms)


def per_device(inputs, upstream, gain, w_query, w_key, w_value, w_out, prefix_len, bound):
    return whole(inputs[0], upstream[0], gain, w_query, w_key, w_value, w_out, prefix_len, bound)


def whole(inputs, grad_out, gain, w_query, w_key, w_value, w_out, prefix_len, bound):
    tok, wide = inputs.shape
    heads_wide = w_query.shape[1]
    my, dp = lax.axis_index("blk"), lax.axis_index("dp")
    count, share = lax.axis_size("blk"), lax.axis_size("dp")
    chips, outer = count // CORES, share // X
    size = wide // (count * share)
    core, x = my % CORES, dp % X
    info = jnp.stack([my, prefix_len[0], bound[0] * BLOCK, core, x]).astype(jnp.int32)
    gain_row = gain.reshape(1, wide)
    filed = shape(X, outer, chips, size, tok)
    copies = shape(chips, tok, HS)
    hidden, k_copies, v_copies = call(
        functools.partial(prepare_kernel, chips),
        (shape(tok, wide), copies, copies),
        (inputs, gain_row, w_key, w_value),
        4 * tok * wide * HS,
    )
    keys = exchange_chips(k_copies)
    values = exchange_chips(v_copies)
    own, ht_own, ht_pair = call(
        project_kernel,
        (shape(2, tok, heads_wide), filed, filed),
        (info, hidden, grad_out, w_query, w_out),
        4 * tok * wide * wide,
        smem=1,
    )
    pair = swap_cores(own)
    mine = run_stats(info, own, pair, keys)
    other = swap_cores(mine)
    attn, dv, probs = run_attend(info, own, pair, mine, other, keys, values)
    attn_other = swap_cores(attn)
    d_value_rows = sum_first(exchange_chips(dv))
    at_own, at_pair, dk, dq_own, dq_pair = run_grads(
        info, own, pair, attn, attn_other, keys, values, probs, filed
    )
    dq_other = swap_cores(dq_pair)
    d_key_rows = sum_first(exchange_chips(dk))
    d_query_rows = as_bf16(dq_own.astype(jnp.float32) + dq_other.astype(jnp.float32))

    out_received = pair_terms(at_pair, grad_out)
    rows = outer * chips * size
    base, *parts = call(
        own_terms_kernel,
        (shape(rows, wide, dtype=jnp.float32), *[shape(rows, wide)] * (X - 1)),
        (at_own, grad_out, out_received),
        2 * X * rows * wide * tok,
    )
    arrived = []
    for step, terms in enumerate(parts, 1):
        arrived.append(send_along_x(terms, step))
    query_received = pair_terms(ht_pair, d_query_rows)
    query_terms = call(
        direct_kernel,
        shape(rows, X * heads_wide),
        (info, ht_own, d_query_rows, query_received),
        2 * X * rows * heads_wide * tok,
        smem=1,
    )
    d_kv_rows = jnp.concatenate([d_key_rows, d_value_rows], axis=1)
    kv_received = pair_terms(ht_pair, d_kv_rows)
    total = wide + X * (heads_wide + 2 * HS)
    terms = call(
        collect_kernel,
        shape(rows, total),
        (info, base, *arrived, query_terms, ht_own, d_kv_rows, kv_received),
        1 << 30,
        smem=1,
    )
    parts = exchange_plane(terms.reshape(outer * chips, size, total))
    copies = call(spread_kernel, shape(share, size, total), (parts,), 1 << 30)
    shared = lax.all_to_all(copies, "dp", 0, 0, tiled=True)
    d_in = call(
        finish_kernel,
        shape(tok, wide),
        (inputs, grad_out, gain_row, d_query_rows, d_kv_rows, w_query, w_key, w_value),
        2 * tok * wide * (wide + 2 * HS),
    )
    held = wide // count

    def my_rows(value):
        return lax.dynamic_slice_in_dim(value, my * held, held, 0)

    slices = [my_rows(w) for w in (w_query, w_key, w_value)]
    slices.append(my_rows(gain).reshape(1, held))
    f32 = functools.partial(shape, dtype=jnp.float32)
    d_query, d_key, d_value, d_out, d_gain = call(
        functools.partial(weights_kernel, X),
        (f32(held, heads_wide), f32(held, HS), f32(held, HS), f32(held, wide), f32(1, held)),
        (shared, *slices),
        1 << 30,
    )
    return (d_in[None], d_query, d_key, d_value, d_out, d_gain.reshape(held))


def solution(mesh):
    placed = (P("dp", "blk", None), P("dp", "blk", None), P(), P(), P(), P(), P(), P("dp"), P("dp"))
    return jax.shard_map(
        per_device,
        mesh=mesh,
        in_specs=placed,
        out_specs=(
            P("dp", "blk", None),
            P("blk", None),
            P("blk", None),
            P("blk", None),
            P("blk", None),
            P("blk"),
        ),
        check_vma=False,
    )
```

```python
import functools

import jax
import jax.numpy as jnp
from jax import lax
from jax.experimental import pallas as pl
from jax.experimental.pallas import tpu as pltpu
from jax.sharding import PartitionSpec as P

HS = 256
ACT = 64
BLOCK = 128
NEG = -1e30
EPS = 1e-06
LOG2E = 1.4426950408889634
VMEM_BYTES = 67043328
NT = (((1,), (1,)), ((), ()))


def dot_nt(a, b):
    return lax.dot_general(a, b, NT, preferred_element_type=jnp.float32)


def dot_nn(a, b):
    return jnp.dot(a, b, preferred_element_type=jnp.float32)


def head(h):
    return pl.ds(h * HS, HS)


def part(half, h, heads):
    return pl.ds((half * heads + h) * HS, HS)


def block_state(info, chip, half, tok, seq):
    rows, plen, edge, core = info[0] ^ half, info[1], info[2], info[3]
    low = (chip * 2 + core) * tok
    high = low + tok
    first, last = rows * tok, rows * tok + tok - 1
    seen = ((low < plen) | (high > seq - ACT)) & ((low < edge) | (low <= last))
    full = (high <= plen) & ((high <= edge) | (high - 1 <= first))
    return seen, full


def mask_of(info, chip, half, tok, seq):
    rows, plen, edge, core = info[0] ^ half, info[1], info[2], info[3]
    k_pos = (chip * 2 + core) * tok + lax.broadcasted_iota(jnp.int32, (tok, tok), 0)
    q_pos = rows * tok + lax.broadcasted_iota(jnp.int32, (tok, tok), 1)
    key_ok = (k_pos < plen) | (k_pos >= seq - ACT)
    return key_ok & ((k_pos < edge) | (k_pos <= q_pos))


def when_seen(info, chip, half, tok, seq, work, rest):
    seen, full = block_state(info, chip, half, tok, seq)

    @pl.when(full)
    def _():
        work(None)

    @pl.when(seen & jnp.logical_not(full))
    def _():
        work(mask_of(info, chip, half, tok, seq))

    if rest is not None:
        pl.when(jnp.logical_not(seen))(rest)


def each_chip(chips, step):
    def body(chip, carry):
        step(chip)
        return carry

    lax.fori_loop(0, chips, body, 0)


def scaled_scores(keys, q, h, mask):
    s = dot_nt(keys, q[0, :, head(h)]) * (HS ** (-0.5) * LOG2E)
    return s if mask is None else jnp.where(mask, s, NEG)


def stats_kernel(heads, seq, info, own, pair, keys, out, top, total):
    chips, tok, _ = keys.shape
    top[...] = jnp.full(top.shape, NEG, jnp.float32)
    total[...] = jnp.zeros(total.shape, jnp.float32)

    def step(chip):
        for half, q in enumerate((own, pair)):

            def work(mask, half=half, q=q):
                for h in range(heads):
                    at = part(half, h, heads)
                    s = scaled_scores(keys[chip], q, h, mask)
                    old = top[:, at]
                    new = jnp.maximum(old, jnp.max(s, axis=0, keepdims=True))
                    top[:, at] = new
                    total[:, at] = total[:, at] * jnp.exp2(old - new) + jnp.sum(
                        jnp.exp2(s - new), axis=0, keepdims=True
                    )

            when_seen(info, chip, half, tok, seq, work, None)

    each_chip(chips, step)
    wide = heads * HS
    for half in range(2):
        out[half, 0:1, :] = top[:, pl.ds(half * wide, wide)]
        out[half, 1:2, :] = total[:, pl.ds(half * wide, wide)]


def take_values(blocks, values, sems):
    copies = [pltpu.make_async_copy(b, values.at[n], sems.at[n]) for n, b in enumerate(blocks)]
    for c in copies:
        c.start()
    return copies


def attend_kernel(heads, seq, info, own, pair, mine, other, keys, *refs):
    chips, tok, _ = keys.shape
    blocks = refs[:chips]
    attn, dv, probs_out, values, values_t, da_rows, probs, lse, out_sems, in_sems = refs[chips:]
    copies = take_values(blocks, values, in_sems)
    wide = heads * HS
    for half, qd in enumerate((own, pair)):
        for h in range(heads):
            da_rows[part(half, h, heads), :] = qd[1, :, head(h)]
        top_a, top_b = mine[half, 0:1, :], other[1 - half, 0:1, :]
        top = jnp.maximum(top_a, top_b)
        total = mine[half, 1:2, :] * jnp.exp2(top_a - top)
        total = total + other[1 - half, 1:2, :] * jnp.exp2(top_b - top)
        lse[:, pl.ds(half * wide, wide)] = top + jnp.log(total) * LOG2E
    for c in copies:
        c.wait()
    for chip in range(chips):
        values_t[:, pl.ds(chip * tok, tok)] = values[chip ^ (info[0] // 2)].T

    def rows_of(chip):
        return pl.ds(pl.multiple_of(chip * tok, tok), tok)

    def out_copy(chip):
        rows = rows_of(chip)
        return pltpu.make_async_copy(probs.at[rows, :], probs_out.at[rows, :], out_sems.at[chip])

    def step(chip):
        rows = rows_of(chip)
        for half, q in enumerate((own, pair)):

            def work(mask, half=half, q=q):
                for h in range(heads):
                    at = part(half, h, heads)
                    s = scaled_scores(keys[chip], q, h, mask)
                    probs[rows, at] = jnp.exp2(s - lse[:, at]).astype(jnp.bfloat16)

            def rest(half=half):
                probs[rows, pl.ds(half * wide, wide)] = jnp.zeros((tok, wide), jnp.bfloat16)

            when_seen(info, chip, half, tok, seq, work, rest)
        dv[chip] = dot_nn(probs[rows, :], da_rows[...]).astype(jnp.bfloat16)
        out_copy(chip).start()

    each_chip(chips, step)
    for half in range(2):
        for h in range(heads):
            attn[half, head(h), :] = dot_nn(values_t[...], probs[:, part(half, h, heads)]).astype(
                jnp.bfloat16
            )
    each_chip(chips, lambda chip: out_copy(chip).wait())


def put_rows(info, rows, chip, own, pair):
    core, x = info[3], info[4]
    steps, outer, _, size, _ = own.shape

    def put(same):
        for n in range(rows.shape[0] // size):
            place = n % (outer * steps)
            to = own if (n // (outer * steps)) == same else pair
            step = (place % steps - x + steps) & (steps - 1)
            to[step, place // steps, chip] = rows[n * size : (n + 1) * size].astype(to.dtype)

    for same in range(2):
        pl.when(core == same)(functools.partial(put, same))


def grads_kernel(heads, seq, info, own, pair, mine, other, keys, *refs):
    chips, tok, _ = keys.shape
    blocks, probs_in = refs[:chips], refs[chips]
    at_own, at_pair, dk, dq_own, dq_pair = refs[chips + 1 : chips + 6]
    values, keys_t, q_rows, probs, dscores, delta, in_sems, v_sems = refs[chips + 6 :]
    copies = take_values(blocks, values, v_sems)

    def rows_of(chip):
        return pl.ds(pl.multiple_of(chip * tok, tok), tok)

    def in_copy(chip):
        rows = rows_of(chip)
        return pltpu.make_async_copy(probs_in.at[rows, :], probs.at[rows, :], in_sems.at[chip])

    each_chip(chips, lambda chip: in_copy(chip).start())
    per_head = chips // heads
    block = HS // per_head
    for half, qd in enumerate((own, pair)):
        for h in range(heads):
            at = part(half, h, heads)
            q_rows[at, :] = qd[0, :, head(h)]
            both = mine[half, head(h), :].astype(jnp.float32) + other[1 - half, head(h), :].astype(
                jnp.float32
            )
            a = both.astype(jnp.bfloat16).astype(jnp.float32)
            delta[:, at] = jnp.sum(
                a * qd[1, :, head(h)].T.astype(jnp.float32), axis=0, keepdims=True
            )
            if half == 0:
                for n in range(per_head):
                    put_rows(info, a[n * block : (n + 1) * block], h * per_head + n, at_own, at_pair)
    for chip in range(chips):
        keys_t[:, pl.ds(chip * tok, tok)] = keys[chip].T
    for c in copies:
        c.wait()

    def step(chip):
        rows = rows_of(chip)
        in_copy(chip).wait()
        for half, qd in enumerate((own, pair)):
            seen, _ = block_state(info, chip, half, tok, seq)

            @pl.when(seen)
            def _(half=half, qd=qd):
                for h in range(heads):
                    at = part(half, h, heads)
                    dp = dot_nt(values[chip ^ (info[0] // 2)], qd[1, :, head(h)])
                    p = probs[rows, at].astype(jnp.float32)
                    dscores[rows, at] = (p * (dp - delta[:, at])).astype(jnp.bfloat16)

            @pl.when(jnp.logical_not(seen))
            def _(half=half):
                wide = heads * HS
                dscores[rows, pl.ds(half * wide, wide)] = jnp.zeros((tok, wide), jnp.bfloat16)

        dk[chip] = (dot_nn(dscores[rows, :], q_rows[...]) * HS ** (-0.5)).astype(jnp.bfloat16)

    each_chip(chips, step)
    for half, dq in enumerate((dq_own, dq_pair)):
        for h in range(heads):
            d = dot_nn(keys_t[...], dscores[:, part(half, h, heads)]) * HS ** (-0.5)
            dq[:, head(h)] = d.T.astype(jnp.bfloat16)


def prepare_kernel(chips, x, gain, w_key, w_value, hidden, k_copies, values):
    xf = x[...].astype(jnp.float32)
    inv = lax.rsqrt(jnp.mean(xf * xf, axis=-1, keepdims=True) + EPS)
    h = (xf * inv * gain[...]).astype(jnp.bfloat16)
    hidden[...] = h
    rows = dot_nn(h, w_key[...]).astype(jnp.bfloat16)
    for chip in range(chips):
        k_copies[chip] = rows
    values[...] = dot_nn(h, w_value[...]).astype(jnp.bfloat16)


def project_kernel(info, hidden, grad_out, w_query, w_out, both, ht_own, ht_pair):
    h = hidden[...]
    both[0] = dot_nn(h, w_query[...]).astype(jnp.bfloat16)
    both[1] = dot_nt(grad_out[...], w_out[...]).astype(jnp.bfloat16)
    chips = ht_own.shape[2]
    block = h.shape[1] // chips
    for chip in range(chips):
        rows = h[:, chip * block : (chip + 1) * block].astype(jnp.float32).T
        put_rows(info, rows, chip, ht_own, ht_pair)


def step_terms(left, step, right, received):
    rows = left.shape[1] * left.shape[2] * left.shape[3]
    own = dot_nn(left[step].reshape(rows, -1), right)
    return own + received[pl.ds(step * rows, rows), :].astype(jnp.float32)


def own_terms_kernel(left, right, received, base, *parts):
    for step, out in enumerate((base, *parts)):
        out[...] = step_terms(left, step, right[...], received).astype(out.dtype)


def direct_terms(info, left, right, received, out, at):
    wide, steps = right.shape[1], left.shape[0]
    for step in range(steps):
        place = (info[4] + step) & (steps - 1)
        to = pl.ds(pl.multiple_of(at + place * wide, 128), wide)
        out[:, to] = step_terms(left, step, right[...], received).astype(out.dtype)


def direct_kernel(info, left, right, received, out):
    direct_terms(info, left, right, received, out, 0)


def collect_kernel(info, base, one, two, three, left, right, received, out):
    total = base[...]
    for arrived in (one, two, three):
        total = total + arrived[...].astype(jnp.float32)
    wide = total.shape[1]
    out[:, pl.ds(0, wide)] = total.astype(out.dtype)
    direct_terms(info, left, right, received, out, wide)


def added_parts(parts):
    total = parts[0].astype(jnp.float32)
    for n in range(1, parts.shape[0]):
        total = total + parts[n].astype(jnp.float32)
    return total.astype(jnp.bfloat16)


def total_kernel(parts, out):
    out[...] = added_parts(parts)


def spread_kernel(first, parts, query, out):
    total = added_parts(parts)
    last = first + query.shape[1]
    for n in range(out.shape[0]):
        out[n, :, pl.ds(0, first)] = total[:, :first]
        out[n, :, pl.ds(first, query.shape[1])] = query[...]
        out[n, :, pl.ds(last, total.shape[1] - first)] = total[:, first:]


def weights_kernel(steps, shared, w_query, w_key, w_value, gain, d_query, d_key, d_value, d_out, d_gain):
    size = shared.shape[1]
    wide, heads_wide = d_out.shape[1], d_query.shape[1]
    gains = []
    for place in range(shared.shape[0]):
        outer, x = place // steps, place % steps
        rows = slice(place * size, (place + 1) * size)
        d_out[rows, :] = shared[place, :, pl.ds(0, wide)].astype(jnp.float32)

        def added(at, width):
            total = 0.0
            for source in range(steps):
                total = total + shared[outer * steps + source, :, pl.ds(at, width)].astype(jnp.float32)
            return total

        query = added(wide + x * heads_wide, heads_wide)
        kv = added(wide + steps * heads_wide + x * 2 * HS, 2 * HS)
        d_query[rows, :] = query
        d_key[rows, :] = kv[:, :HS]
        d_value[rows, :] = kv[:, HS:]
        row_sum = (
            jnp.sum(w_query[rows, :].astype(jnp.float32) * query, axis=1, keepdims=True)
            + jnp.sum(w_key[rows, :].astype(jnp.float32) * kv[:, :HS], axis=1, keepdims=True)
            + jnp.sum(w_value[rows, :].astype(jnp.float32) * kv[:, HS:], axis=1, keepdims=True)
        )
        gains.append(jnp.broadcast_to(row_sum, (size, 128)))
    d_gain[...] = jnp.concatenate(gains, axis=0).T[0:1, :] / gain[...]


def finish_kernel(x, grad_out, gain, dq, dkv, w_query, w_key, w_value, d_in):
    dhidden = (
        dot_nt(dq[...], w_query[...])
        + dot_nt(dkv[:, :HS], w_key[...])
        + dot_nt(dkv[:, HS:], w_value[...])
    )
    xf = x[...].astype(jnp.float32)
    inv = lax.rsqrt(jnp.mean(xf * xf, axis=-1, keepdims=True) + EPS)
    normed = xf * inv
    scaled = dhidden * gain[...]
    mean = jnp.mean(scaled * normed, axis=-1, keepdims=True)
    d_in[...] = (grad_out[...].astype(jnp.float32) + inv * (scaled - normed * mean)).astype(d_in.dtype)


SMEM = pl.BlockSpec(memory_space=pltpu.SMEM)
VMEM = pl.BlockSpec(memory_space=pltpu.VMEM)
ANY = pl.BlockSpec(memory_space=pl.ANY)


def shape(*dims, dtype=jnp.bfloat16):
    return jax.ShapeDtypeStruct(dims, dtype)


def call(body, outs, args, flops, smem=0, scratch=(), in_any=(), out_any=()):
    specs = [SMEM if n < smem else ANY if n in in_any else VMEM for n in range(len(args))]
    if isinstance(outs, tuple):
        out_specs = tuple(ANY if n in out_any else VMEM for n in range(len(outs)))
    else:
        out_specs = VMEM
    return pl.pallas_call(
        body,
        out_shape=outs,
        in_specs=specs,
        out_specs=out_specs,
        scratch_shapes=list(scratch),
        compiler_params=pltpu.CompilerParams(vmem_limit_bytes=VMEM_BYTES),
        cost_estimate=pl.CostEstimate(flops=flops, bytes_accessed=1 << 20, transcendentals=0),
    )(*args)


def scratch(*dims, dtype=jnp.bfloat16):
    return pltpu.VMEM(dims, dtype)


def run_stats(info, own, pair, keys):
    _, tok, wide = own.shape
    chips, heads = keys.shape[0], wide // HS
    seq = 2 * tok * chips
    rows = scratch(1, 2 * wide, dtype=jnp.float32)
    return call(
        functools.partial(stats_kernel, heads, seq),
        shape(2, 2, wide, dtype=jnp.float32),
        (info, own, pair, keys),
        2 * seq * wide * HS,
        smem=1,
        scratch=(rows, rows),
    )


def run_attend(info, own, pair, mine, other, keys, values):
    _, tok, wide = own.shape
    chips, heads = keys.shape[0], wide // HS
    seq = 2 * tok * chips
    return call(
        functools.partial(attend_kernel, heads, seq),
        (shape(2, wide, tok), shape(chips, tok, HS), shape(chips * tok, 2 * wide)),
        (info, own, pair, mine, other, keys, *values),
        6 * seq * wide * HS,
        smem=1,
        in_any=range(6, 6 + chips),
        out_any=(2,),
        scratch=(
            scratch(chips, tok, HS),
            scratch(HS, chips * tok),
            scratch(2 * wide, HS),
            scratch(chips * tok, 2 * wide),
            scratch(1, 2 * wide, dtype=jnp.float32),
            pltpu.SemaphoreType.DMA((chips,)),
            pltpu.SemaphoreType.DMA((chips,)),
        ),
    )


def run_grads(info, own, pair, mine, other, keys, values, probs, filed):
    _, tok, wide = own.shape
    chips, heads = keys.shape[0], wide // HS
    seq = 2 * tok * chips
    return call(
        functools.partial(grads_kernel, heads, seq),
        (filed, filed, shape(chips, tok, HS), shape(tok, wide), shape(tok, wide)),
        (info, own, pair, mine, other, keys, *values, probs),
        6 * seq * wide * HS,
        smem=1,
        in_any=range(6, 7 + chips),
        scratch=(
            scratch(chips, tok, HS),
            scratch(HS, chips * tok),
            scratch(2 * wide, HS),
            scratch(chips * tok, 2 * wide),
            scratch(chips * tok, 2 * wide),
            scratch(1, 2 * wide, dtype=jnp.float32),
            pltpu.SemaphoreType.DMA((chips,)),
            pltpu.SemaphoreType.DMA((chips,)),
        ),
    )


CORES = 2
X = 4


def as_bf16(value):
    return value.astype(jnp.bfloat16)


def swap_cores(value):
    count = lax.axis_size("blk")
    return lax.ppermute(value, "blk", [(i, i ^ 1) for i in range(count)])


def send_along_x(value, step):
    count = lax.axis_size("dp")
    return lax.ppermute(
        value, "dp", [(i, i // X * X + (i + step) % X) for i in range(count)]
    )


def exchange_chips(value):
    chips = lax.axis_size("blk") // CORES
    groups = [[core + CORES * chip for chip in range(chips)] for core in range(CORES)]
    return lax.all_to_all(value, "blk", 0, 0, tiled=True, axis_index_groups=groups)


def exchange_plane(value):
    blk, dp = lax.axis_size("blk"), lax.axis_size("dp")
    groups = [
        [(outer * X + x) * blk + chip * CORES + core for outer in range(dp // X) for chip in range(blk // CORES)]
        for x in range(X)
        for core in range(CORES)
    ]
    value = value.reshape(dp // X * (blk // CORES), -1, value.shape[1])
    return lax.all_to_all(value, ("dp", "blk"), 0, 0, tiled=True, axis_index_groups=groups)


def sum_first(parts):
    return as_bf16(jnp.sum(parts.astype(jnp.float32), axis=0))


def pair_terms(left_pair, right):
    terms = as_bf16(dot_nn(left_pair.reshape(-1, left_pair.shape[-1]), right))
    return swap_cores(terms)


def per_device(inputs, upstream, gain, w_query, w_key, w_value, w_out, prefix_len, bound):
    return whole(inputs[0], upstream[0], gain, w_query, w_key, w_value, w_out, prefix_len, bound)


def whole(inputs, grad_out, gain, w_query, w_key, w_value, w_out, prefix_len, bound):
    tok, wide = inputs.shape
    heads_wide = w_query.shape[1]
    my, dp = lax.axis_index("blk"), lax.axis_index("dp")
    count, share = lax.axis_size("blk"), lax.axis_size("dp")
    chips, outer = count // CORES, share // X
    size = wide // (count * share)
    core, x = my % CORES, dp % X
    info = jnp.stack([my, prefix_len[0], bound[0] * BLOCK, core, x]).astype(jnp.int32)
    gain_row = gain.reshape(1, wide)
    filed = shape(X, outer, chips, size, tok)
    copies = shape(chips, tok, HS)
    hidden, k_copies, my_values = call(
        functools.partial(prepare_kernel, chips),
        (shape(tok, wide), copies, shape(tok, HS)),
        (inputs, gain_row, w_key, w_value),
        4 * tok * wide * HS,
    )
    keys = exchange_chips(k_copies)
    values = [my_values]
    for other in range(1, chips):
        steps = [(i, i ^ (other * CORES)) for i in range(count)]
        values.append(lax.ppermute(my_values, "blk", steps))
    own, ht_own, ht_pair = call(
        project_kernel,
        (shape(2, tok, heads_wide), filed, filed),
        (info, hidden, grad_out, w_query, w_out),
        4 * tok * wide * wide,
        smem=1,
    )
    pair = swap_cores(own)
    mine = run_stats(info, own, pair, keys)
    other = swap_cores(mine)
    attn, dv, probs = run_attend(info, own, pair, mine, other, keys, values)
    attn_other = swap_cores(attn)
    d_value_rows = sum_first(exchange_chips(dv))
    at_own, at_pair, dk, dq_own, dq_pair = run_grads(
        info, own, pair, attn, attn_other, keys, values, probs, filed
    )
    dq_other = swap_cores(dq_pair)
    d_key_rows = sum_first(exchange_chips(dk))
    d_query_rows = as_bf16(dq_own.astype(jnp.float32) + dq_other.astype(jnp.float32))

    out_received = pair_terms(at_pair, grad_out)
    rows = outer * chips * size
    base, *parts = call(
        own_terms_kernel,
        (shape(rows, wide, dtype=jnp.float32), *[shape(rows, wide)] * (X - 1)),
        (at_own, grad_out, out_received),
        2 * X * rows * wide * tok,
    )
    arrived = []
    for step, terms in enumerate(parts, 1):
        arrived.append(send_along_x(terms, step))
    query_received = pair_terms(ht_pair, d_query_rows)
    query_terms = call(
        direct_kernel,
        shape(rows, X * heads_wide),
        (info, ht_own, d_query_rows, query_received),
        2 * X * rows * heads_wide * tok,
        smem=1,
    )
    d_kv_rows = jnp.concatenate([d_key_rows, d_value_rows], axis=1)
    kv_received = pair_terms(ht_pair, d_kv_rows)
    total = wide + X * (heads_wide + 2 * HS)
    terms = call(
        collect_kernel,
        shape(rows, wide + 2 * HS * X),
        (info, base, *arrived, ht_own, d_kv_rows, kv_received),
        1 << 30,
        smem=1,
    )
    query_parts = exchange_plane(query_terms)
    query_total = call(total_kernel, shape(size, X * heads_wide), (query_parts,), 1 << 30)
    parts = exchange_plane(terms)
    copies = call(
        functools.partial(spread_kernel, wide),
        shape(share, size, total),
        (parts, query_total),
        1 << 30,
    )
    shared = lax.all_to_all(copies, "dp", 0, 0, tiled=True)
    d_in = call(
        finish_kernel,
        shape(tok, wide),
        (inputs, grad_out, gain_row, d_query_rows, d_kv_rows, w_query, w_key, w_value),
        2 * tok * wide * (wide + 2 * HS),
    )
    held = wide // count

    def my_rows(value):
        return lax.dynamic_slice_in_dim(value, my * held, held, 0)

    slices = [my_rows(w) for w in (w_query, w_key, w_value)]
    slices.append(my_rows(gain).reshape(1, held))
    f32 = functools.partial(shape, dtype=jnp.float32)
    d_query, d_key, d_value, d_out, d_gain = call(
        functools.partial(weights_kernel, X),
        (f32(held, heads_wide), f32(held, HS), f32(held, HS), f32(held, wide), f32(1, held)),
        (shared, *slices),
        1 << 30,
    )
    return (d_in[None], d_query, d_key, d_value, d_out, d_gain.reshape(held))


def solution(mesh):
    placed = (P("dp", "blk", None), P("dp", "blk", None), P(), P(), P(), P(), P(), P("dp"), P("dp"))
    return jax.shard_map(
        per_device,
        mesh=mesh,
        in_specs=placed,
        out_specs=(
            P("dp", "blk", None),
            P("blk", None),
            P("blk", None),
            P("blk", None),
            P("blk", None),
            P("blk"),
        ),
        check_vma=False,
    )
```

```python
import functools

import jax
import jax.numpy as jnp
from jax import lax
from jax.experimental import pallas as pl
from jax.experimental.pallas import tpu as pltpu
from jax.sharding import PartitionSpec as P

HS = 256
ACT = 64
BLOCK = 128
NEG = -1e30
EPS = 1e-06
LOG2E = 1.4426950408889634
VMEM_BYTES = 67043328
NT = (((1,), (1,)), ((), ()))


def dot_nt(a, b):
    return lax.dot_general(a, b, NT, preferred_element_type=jnp.float32)


def dot_nn(a, b):
    return jnp.dot(a, b, preferred_element_type=jnp.float32)


def head(h):
    return pl.ds(h * HS, HS)


def part(half, h, heads):
    return pl.ds((half * heads + h) * HS, HS)


def block_state(info, chip, half, tok, seq):
    rows, plen, edge, core = info[0] ^ half, info[1], info[2], info[3]
    low = (chip * 2 + core) * tok
    high = low + tok
    first, last = rows * tok, rows * tok + tok - 1
    seen = ((low < plen) | (high > seq - ACT)) & ((low < edge) | (low <= last))
    full = (high <= plen) & ((high <= edge) | (high - 1 <= first))
    return seen, full


def mask_of(info, chip, half, tok, seq):
    rows, plen, edge, core = info[0] ^ half, info[1], info[2], info[3]
    k_pos = (chip * 2 + core) * tok + lax.broadcasted_iota(jnp.int32, (tok, tok), 0)
    q_pos = rows * tok + lax.broadcasted_iota(jnp.int32, (tok, tok), 1)
    key_ok = (k_pos < plen) | (k_pos >= seq - ACT)
    return key_ok & ((k_pos < edge) | (k_pos <= q_pos))


def when_seen(info, chip, half, tok, seq, work, rest):
    seen, full = block_state(info, chip, half, tok, seq)

    @pl.when(full)
    def _():
        work(None)

    @pl.when(seen & jnp.logical_not(full))
    def _():
        work(mask_of(info, chip, half, tok, seq))

    if rest is not None:
        pl.when(jnp.logical_not(seen))(rest)


def each_chip(chips, step):
    def body(chip, carry):
        step(chip)
        return carry

    lax.fori_loop(0, chips, body, 0)


def scaled_scores(keys, q, h, mask):
    s = dot_nt(keys, q[0, :, head(h)]) * (HS ** (-0.5) * LOG2E)
    return s if mask is None else jnp.where(mask, s, NEG)


def stats_kernel(heads, seq, info, own, pair, keys, out, top, total):
    chips, tok, _ = keys.shape
    top[...] = jnp.full(top.shape, NEG, jnp.float32)
    total[...] = jnp.zeros(total.shape, jnp.float32)

    def step(chip):
        for half, q in enumerate((own, pair)):

            def work(mask, half=half, q=q):
                for h in range(heads):
                    at = part(half, h, heads)
                    s = scaled_scores(keys[chip], q, h, mask)
                    old = top[:, at]
                    new = jnp.maximum(old, jnp.max(s, axis=0, keepdims=True))
                    top[:, at] = new
                    total[:, at] = total[:, at] * jnp.exp2(old - new) + jnp.sum(
                        jnp.exp2(s - new), axis=0, keepdims=True
                    )

            when_seen(info, chip, half, tok, seq, work, None)

    each_chip(chips, step)
    wide = heads * HS
    for half in range(2):
        out[half, 0:1, :] = top[:, pl.ds(half * wide, wide)]
        out[half, 1:2, :] = total[:, pl.ds(half * wide, wide)]


def attend_kernel(
    heads, seq, info, own, pair, mine, other, keys, values,
    attn, dv, probs_out,
    values_t, da_rows, probs, lse, out_sems,
):
    chips, tok, _ = keys.shape
    wide = heads * HS
    for half, qd in enumerate((own, pair)):
        for h in range(heads):
            da_rows[part(half, h, heads), :] = qd[1, :, head(h)]
        top_a, top_b = mine[half, 0:1, :], other[1 - half, 0:1, :]
        top = jnp.maximum(top_a, top_b)
        total = mine[half, 1:2, :] * jnp.exp2(top_a - top)
        total = total + other[1 - half, 1:2, :] * jnp.exp2(top_b - top)
        lse[:, pl.ds(half * wide, wide)] = top + jnp.log(total) * LOG2E
    for chip in range(chips):
        values_t[:, pl.ds(chip * tok, tok)] = values[chip].T

    def rows_of(chip):
        return pl.ds(pl.multiple_of(chip * tok, tok), tok)

    def out_copy(chip):
        rows = rows_of(chip)
        return pltpu.make_async_copy(probs.at[rows, :], probs_out.at[rows, :], out_sems.at[chip])

    def step(chip):
        rows = rows_of(chip)
        for half, q in enumerate((own, pair)):

            def work(mask, half=half, q=q):
                for h in range(heads):
                    at = part(half, h, heads)
                    s = scaled_scores(keys[chip], q, h, mask)
                    probs[rows, at] = jnp.exp2(s - lse[:, at]).astype(jnp.bfloat16)

            def rest(half=half):
                probs[rows, pl.ds(half * wide, wide)] = jnp.zeros((tok, wide), jnp.bfloat16)

            when_seen(info, chip, half, tok, seq, work, rest)
        dv[chip] = dot_nn(probs[rows, :], da_rows[...]).astype(jnp.bfloat16)
        out_copy(chip).start()

    each_chip(chips, step)
    for half in range(2):
        for h in range(heads):
            attn[half, head(h), :] = dot_nn(values_t[...], probs[:, part(half, h, heads)]).astype(
                jnp.bfloat16
            )
    each_chip(chips, lambda chip: out_copy(chip).wait())


def put_rows(info, rows, chip, own, pair):
    core, x = info[3], info[4]
    steps, outer, _, size, _ = own.shape

    def put(same):
        for n in range(rows.shape[0] // size):
            place = n % (outer * steps)
            to = own if (n // (outer * steps)) == same else pair
            if to is None:
                continue
            step = (place % steps - x + steps) & (steps - 1)
            to[step, place // steps, chip] = rows[n * size : (n + 1) * size].astype(to.dtype)

    for same in range(2):
        pl.when(core == same)(functools.partial(put, same))


def grads_kernel(
    heads, seq, info, own, pair, mine, other, keys, values, probs_in,
    at_own, at_pair, dk, dq,
    keys_t, q_rows, probs, dscores, delta, in_sems,
):
    chips, tok, _ = keys.shape

    def rows_of(chip):
        return pl.ds(pl.multiple_of(chip * tok, tok), tok)

    def in_copy(chip):
        rows = rows_of(chip)
        return pltpu.make_async_copy(probs_in.at[rows, :], probs.at[rows, :], in_sems.at[chip])

    each_chip(chips, lambda chip: in_copy(chip).start())
    per_head = chips // heads
    block = HS // per_head
    for half, qd in enumerate((own, pair)):
        for h in range(heads):
            at = part(half, h, heads)
            q_rows[at, :] = qd[0, :, head(h)]
            both = mine[half, head(h), :].astype(jnp.float32) + other[1 - half, head(h), :].astype(
                jnp.float32
            )
            a = both.astype(jnp.bfloat16).astype(jnp.float32)
            delta[:, at] = jnp.sum(
                a * qd[1, :, head(h)].T.astype(jnp.float32), axis=0, keepdims=True
            )
            for n in range(per_head):
                put_rows(info, a[n * block : (n + 1) * block], h * per_head + n, (at_own, at_pair)[half], None)
    for chip in range(chips):
        keys_t[:, pl.ds(chip * tok, tok)] = keys[chip].T

    def step(chip):
        rows = rows_of(chip)
        in_copy(chip).wait()
        for half, qd in enumerate((own, pair)):
            seen, _ = block_state(info, chip, half, tok, seq)

            @pl.when(seen)
            def _(half=half, qd=qd):
                for h in range(heads):
                    at = part(half, h, heads)
                    dp = dot_nt(values[chip], qd[1, :, head(h)])
                    p = probs[rows, at].astype(jnp.float32)
                    dscores[rows, at] = (p * (dp - delta[:, at])).astype(jnp.bfloat16)

            @pl.when(jnp.logical_not(seen))
            def _(half=half):
                wide = heads * HS
                dscores[rows, pl.ds(half * wide, wide)] = jnp.zeros((tok, wide), jnp.bfloat16)

        dk[chip] = (dot_nn(dscores[rows, :], q_rows[...]) * HS ** (-0.5)).astype(jnp.bfloat16)

    each_chip(chips, step)
    for half in range(2):
        for h in range(heads):
            d = dot_nn(keys_t[...], dscores[:, part(half, h, heads)]) * HS ** (-0.5)
            dq[half, :, head(h)] = d.T.astype(jnp.bfloat16)


def prepare_kernel(chips, x, gain, w_key, w_value, hidden, k_copies, v_copies):
    xf = x[...].astype(jnp.float32)
    inv = lax.rsqrt(jnp.mean(xf * xf, axis=-1, keepdims=True) + EPS)
    h = (xf * inv * gain[...]).astype(jnp.bfloat16)
    hidden[...] = h
    for weight, out in ((w_key, k_copies), (w_value, v_copies)):
        rows = dot_nn(h, weight[...]).astype(jnp.bfloat16)
        for chip in range(chips):
            out[chip] = rows


def project_kernel(info, hidden, grad_out, w_query, w_out, both, ht_own, ht_pair):
    h = hidden[...]
    both[0] = dot_nn(h, w_query[...]).astype(jnp.bfloat16)
    both[1] = dot_nt(grad_out[...], w_out[...]).astype(jnp.bfloat16)
    both[2] = grad_out[...]
    chips = ht_own.shape[2]
    block = h.shape[1] // chips
    for chip in range(chips):
        rows = h[:, chip * block : (chip + 1) * block].astype(jnp.float32).T
        put_rows(info, rows, chip, ht_own, ht_pair)


def step_terms(lefts, rights, step):
    total = 0.0
    for left, right in zip(lefts, rights):
        rows = left.shape[1] * left.shape[2] * left.shape[3]
        total = total + dot_nn(left[step].reshape(rows, -1), right)
    return total


def direct_terms(info, lefts, rights, out, at):
    wide, steps = rights[0].shape[1], lefts[0].shape[0]
    for step in range(steps):
        place = (info[4] + step) & (steps - 1)
        to = pl.ds(pl.multiple_of(at + place * wide, 128), wide)
        out[:, to] = step_terms(lefts, rights, step).astype(out.dtype)


def terms_kernel(
    info, at_own, at_pair, own, pair, ht_own, ht_pair, dq_mine, dq_other,
    dq, query_terms, base, *parts,
):
    for step, out in enumerate((base, *parts)):
        out[...] = step_terms((at_own, at_pair), (own[2], pair[2]), step).astype(out.dtype)
    rights = [
        (dq_mine[half].astype(jnp.float32) + dq_other[1 - half].astype(jnp.float32)).astype(dq.dtype)
        for half in range(2)
    ]
    dq[...] = rights[0]
    direct_terms(info, (ht_own, ht_pair), rights, query_terms, 0)


def rows_kernel(dk_parts, dv_parts, out):
    for at, parts in ((0, dk_parts), (HS, dv_parts)):
        total = parts[0].astype(jnp.float32)
        for n in range(1, parts.shape[0]):
            total = total + parts[n].astype(jnp.float32)
        out[:, pl.ds(at, HS)] = total.astype(out.dtype)


def collect_kernel(info, base, one, two, three, query_terms, ht_own, ht_pair, dkv, dkv_pair, out):
    total = base[...]
    for arrived in (one, two, three):
        total = total + arrived[...].astype(jnp.float32)
    wide = total.shape[1]
    out[:, pl.ds(0, wide)] = total.astype(out.dtype)
    out[:, pl.ds(wide, query_terms.shape[1])] = query_terms[...]
    rights = (dkv[...], dkv_pair[...])
    direct_terms(info, (ht_own, ht_pair), rights, out, wide + query_terms.shape[1])


def spread_kernel(parts, out):
    total = parts[0].astype(jnp.float32)
    for n in range(1, parts.shape[0]):
        total = total + parts[n].astype(jnp.float32)
    total = total.astype(out.dtype)
    for n in range(out.shape[0]):
        out[n] = total


def weights_kernel(steps, shared, w_query, w_key, w_value, gain, d_query, d_key, d_value, d_out, d_gain):
    size = shared.shape[1]
    wide, heads_wide = d_out.shape[1], d_query.shape[1]
    gains = []
    for place in range(shared.shape[0]):
        outer, x = place // steps, place % steps
        rows = slice(place * size, (place + 1) * size)
        d_out[rows, :] = shared[place, :, pl.ds(0, wide)].astype(jnp.float32)

        def added(at, width):
            total = 0.0
            for source in range(steps):
                total = total + shared[outer * steps + source, :, pl.ds(at, width)].astype(jnp.float32)
            return total

        query = added(wide + x * heads_wide, heads_wide)
        kv = added(wide + steps * heads_wide + x * 2 * HS, 2 * HS)
        d_query[rows, :] = query
        d_key[rows, :] = kv[:, :HS]
        d_value[rows, :] = kv[:, HS:]
        row_sum = (
            jnp.sum(w_query[rows, :].astype(jnp.float32) * query, axis=1, keepdims=True)
            + jnp.sum(w_key[rows, :].astype(jnp.float32) * kv[:, :HS], axis=1, keepdims=True)
            + jnp.sum(w_value[rows, :].astype(jnp.float32) * kv[:, HS:], axis=1, keepdims=True)
        )
        gains.append(jnp.broadcast_to(row_sum, (size, 128)))
    d_gain[...] = jnp.concatenate(gains, axis=0).T[0:1, :] / gain[...]


def finish_kernel(x, grad_out, gain, dq, dkv, w_query, w_key, w_value, d_in):
    dhidden = (
        dot_nt(dq[...], w_query[...])
        + dot_nt(dkv[:, :HS], w_key[...])
        + dot_nt(dkv[:, HS:], w_value[...])
    )
    xf = x[...].astype(jnp.float32)
    inv = lax.rsqrt(jnp.mean(xf * xf, axis=-1, keepdims=True) + EPS)
    normed = xf * inv
    scaled = dhidden * gain[...]
    mean = jnp.mean(scaled * normed, axis=-1, keepdims=True)
    d_in[...] = (grad_out[...].astype(jnp.float32) + inv * (scaled - normed * mean)).astype(d_in.dtype)


SMEM = pl.BlockSpec(memory_space=pltpu.SMEM)
VMEM = pl.BlockSpec(memory_space=pltpu.VMEM)
ANY = pl.BlockSpec(memory_space=pl.ANY)


def shape(*dims, dtype=jnp.bfloat16):
    return jax.ShapeDtypeStruct(dims, dtype)


def call(body, outs, args, flops, smem=0, scratch=(), in_any=(), out_any=()):
    specs = [SMEM if n < smem else ANY if n in in_any else VMEM for n in range(len(args))]
    if isinstance(outs, tuple):
        out_specs = tuple(ANY if n in out_any else VMEM for n in range(len(outs)))
    else:
        out_specs = VMEM
    return pl.pallas_call(
        body,
        out_shape=outs,
        in_specs=specs,
        out_specs=out_specs,
        scratch_shapes=list(scratch),
        compiler_params=pltpu.CompilerParams(vmem_limit_bytes=VMEM_BYTES),
        cost_estimate=pl.CostEstimate(flops=flops, bytes_accessed=1 << 20, transcendentals=0),
    )(*args)


def scratch(*dims, dtype=jnp.bfloat16):
    return pltpu.VMEM(dims, dtype)


def run_stats(info, own, pair, keys):
    tok, wide = own.shape[1:]
    chips, heads = keys.shape[0], wide // HS
    seq = 2 * tok * chips
    rows = scratch(1, 2 * wide, dtype=jnp.float32)
    return call(
        functools.partial(stats_kernel, heads, seq),
        shape(2, 2, wide, dtype=jnp.float32),
        (info, own, pair, keys),
        2 * seq * wide * HS,
        smem=1,
        scratch=(rows, rows),
    )


def run_attend(info, own, pair, mine, other, keys, values):
    tok, wide = own.shape[1:]
    chips, heads = keys.shape[0], wide // HS
    seq = 2 * tok * chips
    return call(
        functools.partial(attend_kernel, heads, seq),
        (shape(2, wide, tok), shape(chips, tok, HS), shape(chips * tok, 2 * wide)),
        (info, own, pair, mine, other, keys, values),
        6 * seq * wide * HS,
        smem=1,
        out_any=(2,),
        scratch=(
            scratch(HS, chips * tok),
            scratch(2 * wide, HS),
            scratch(chips * tok, 2 * wide),
            scratch(1, 2 * wide, dtype=jnp.float32),
            pltpu.SemaphoreType.DMA((chips,)),
        ),
    )


def run_grads(info, own, pair, mine, other, keys, values, probs, filed):
    tok, wide = own.shape[1:]
    chips, heads = keys.shape[0], wide // HS
    seq = 2 * tok * chips
    return call(
        functools.partial(grads_kernel, heads, seq),
        (filed, filed, shape(chips, tok, HS), shape(2, tok, wide)),
        (info, own, pair, mine, other, keys, values, probs),
        6 * seq * wide * HS,
        smem=1,
        in_any=(7,),
        scratch=(
            scratch(HS, chips * tok),
            scratch(2 * wide, HS),
            scratch(chips * tok, 2 * wide),
            scratch(chips * tok, 2 * wide),
            scratch(1, 2 * wide, dtype=jnp.float32),
            pltpu.SemaphoreType.DMA((chips,)),
        ),
    )


CORES = 2
X = 4


def swap_cores(value):
    count = lax.axis_size("blk")
    return lax.ppermute(value, "blk", [(i, i ^ 1) for i in range(count)])


def send_along_x(value, step):
    count = lax.axis_size("dp")
    return lax.ppermute(
        value, "dp", [(i, i // X * X + (i + step) % X) for i in range(count)]
    )


def exchange_chips(value):
    chips = lax.axis_size("blk") // CORES
    groups = [[core + CORES * chip for chip in range(chips)] for core in range(CORES)]
    return lax.all_to_all(value, "blk", 0, 0, tiled=True, axis_index_groups=groups)


def exchange_plane(value):
    blk, dp = lax.axis_size("blk"), lax.axis_size("dp")
    groups = [
        [(outer * X + x) * blk + chip * CORES + core for outer in range(dp // X) for chip in range(blk // CORES)]
        for x in range(X)
        for core in range(CORES)
    ]
    return lax.all_to_all(value, ("dp", "blk"), 0, 0, tiled=True, axis_index_groups=groups)


def per_device(inputs, upstream, gain, w_query, w_key, w_value, w_out, prefix_len, bound):
    return whole(inputs[0], upstream[0], gain, w_query, w_key, w_value, w_out, prefix_len, bound)


def whole(inputs, grad_out, gain, w_query, w_key, w_value, w_out, prefix_len, bound):
    tok, wide = inputs.shape
    heads_wide = w_query.shape[1]
    my, dp = lax.axis_index("blk"), lax.axis_index("dp")
    count, share = lax.axis_size("blk"), lax.axis_size("dp")
    chips, outer = count // CORES, share // X
    size = wide // (count * share)
    core, x = my % CORES, dp % X
    info = jnp.stack([my, prefix_len[0], bound[0] * BLOCK, core, x]).astype(jnp.int32)
    gain_row = gain.reshape(1, wide)
    filed = shape(X, outer, chips, size, tok)
    copies = shape(chips, tok, HS)
    hidden, k_copies, v_copies = call(
        functools.partial(prepare_kernel, chips),
        (shape(tok, wide), copies, copies),
        (inputs, gain_row, w_key, w_value),
        4 * tok * wide * HS,
    )
    keys = exchange_chips(k_copies)
    values = exchange_chips(v_copies)
    own, ht_own, ht_pair = call(
        project_kernel,
        (shape(3, tok, heads_wide), filed, filed),
        (info, hidden, grad_out, w_query, w_out),
        4 * tok * wide * wide,
        smem=1,
    )
    pair = swap_cores(own)
    ht_pair = swap_cores(ht_pair)
    mine = run_stats(info, own, pair, keys)
    other = swap_cores(mine)
    attn, dv, probs = run_attend(info, own, pair, mine, other, keys, values)
    attn_other = swap_cores(attn)
    dv_parts = exchange_chips(dv)
    at_own, at_pair, dk, dq_mine = run_grads(
        info, own, pair, attn, attn_other, keys, values, probs, filed
    )
    dq_other = swap_cores(dq_mine)
    dk_parts = exchange_chips(dk)
    rows = outer * chips * size
    d_query_rows, query_terms, base, *parts = call(
        terms_kernel,
        (
            shape(tok, heads_wide),
            shape(rows, X * heads_wide),
            shape(rows, wide, dtype=jnp.float32),
            *[shape(rows, wide)] * (X - 1),
        ),
        (info, at_own, at_pair, own, pair, ht_own, ht_pair, dq_mine, dq_other),
        8 * X * rows * wide * tok,
        smem=1,
    )
    arrived = []
    for step, terms in enumerate(parts, 1):
        arrived.append(send_along_x(terms, step))
    d_kv_rows = call(rows_kernel, shape(tok, 2 * HS), (dk_parts, dv_parts), 1 << 30)
    d_kv_pair = swap_cores(d_kv_rows)
    total = wide + X * (heads_wide + 2 * HS)
    terms = call(
        collect_kernel,
        shape(rows, total),
        (info, base, *arrived, query_terms, ht_own, ht_pair, d_kv_rows, d_kv_pair),
        1 << 30,
        smem=1,
    )
    parts = exchange_plane(terms.reshape(outer * chips, size, total))
    copies = call(spread_kernel, shape(share, size, total), (parts,), 1 << 30)
    shared = lax.all_to_all(copies, "dp", 0, 0, tiled=True)
    d_in = call(
        finish_kernel,
        shape(tok, wide),
        (inputs, grad_out, gain_row, d_query_rows, d_kv_rows, w_query, w_key, w_value),
        2 * tok * wide * (wide + 2 * HS),
    )
    held = wide // count

    def my_rows(value):
        return lax.dynamic_slice_in_dim(value, my * held, held, 0)

    slices = [my_rows(w) for w in (w_query, w_key, w_value)]
    slices.append(my_rows(gain).reshape(1, held))
    f32 = functools.partial(shape, dtype=jnp.float32)
    d_query, d_key, d_value, d_out, d_gain = call(
        functools.partial(weights_kernel, X),
        (f32(held, heads_wide), f32(held, HS), f32(held, HS), f32(held, wide), f32(1, held)),
        (shared, *slices),
        1 << 30,
    )
    return (d_in[None], d_query, d_key, d_value, d_out, d_gain.reshape(held))


def solution(mesh):
    placed = (P("dp", "blk", None), P("dp", "blk", None), P(), P(), P(), P(), P(), P("dp"), P("dp"))
    return jax.shard_map(
        per_device,
        mesh=mesh,
        in_specs=placed,
        out_specs=(
            P("dp", "blk", None),
            P("blk", None),
            P("blk", None),
            P("blk", None),
            P("blk", None),
            P("blk"),
        ),
        check_vma=False,
    )
```

```python
import functools

import jax
import jax.numpy as jnp
from jax import lax
from jax.experimental import pallas as pl
from jax.experimental.pallas import tpu as pltpu
from jax.sharding import PartitionSpec as P

HS = 256
ACT = 64
BLOCK = 128
NEG = -1e30
EPS = 1e-06
LOG2E = 1.4426950408889634
VMEM_BYTES = 67043328
NT = (((1,), (1,)), ((), ()))


def dot_nt(a, b):
    return lax.dot_general(a, b, NT, preferred_element_type=jnp.float32)


def dot_nn(a, b):
    return jnp.dot(a, b, preferred_element_type=jnp.float32)


def head(h):
    return pl.ds(h * HS, HS)


def part(half, h, heads):
    return pl.ds((half * heads + h) * HS, HS)


def block_state(info, chip, half, tok, seq):
    rows, plen, edge, core = info[0] ^ half, info[1], info[2], info[3]
    low = (chip * 2 + core) * tok
    high = low + tok
    first, last = rows * tok, rows * tok + tok - 1
    seen = ((low < plen) | (high > seq - ACT)) & ((low < edge) | (low <= last))
    full = (high <= plen) & ((high <= edge) | (high - 1 <= first))
    return seen, full


def mask_of(info, chip, half, tok, seq):
    rows, plen, edge, core = info[0] ^ half, info[1], info[2], info[3]
    k_pos = (chip * 2 + core) * tok + lax.broadcasted_iota(jnp.int32, (tok, tok), 0)
    q_pos = rows * tok + lax.broadcasted_iota(jnp.int32, (tok, tok), 1)
    key_ok = (k_pos < plen) | (k_pos >= seq - ACT)
    return key_ok & ((k_pos < edge) | (k_pos <= q_pos))


def when_seen(info, chip, half, tok, seq, work, rest):
    seen, full = block_state(info, chip, half, tok, seq)

    @pl.when(full)
    def _():
        work(None)

    @pl.when(seen & jnp.logical_not(full))
    def _():
        work(mask_of(info, chip, half, tok, seq))

    if rest is not None:
        pl.when(jnp.logical_not(seen))(rest)


def each_chip(chips, step):
    def body(chip, carry):
        step(chip)
        return carry

    lax.fori_loop(0, chips, body, 0)


def scaled_scores(keys, q, h, mask):
    s = dot_nt(keys, q[0, :, head(h)]) * (HS ** (-0.5) * LOG2E)
    return s if mask is None else jnp.where(mask, s, NEG)


def stats_kernel(heads, seq, info, own, pair, keys, out, top, total):
    chips, tok, _ = keys.shape
    top[...] = jnp.full(top.shape, NEG, jnp.float32)
    total[...] = jnp.zeros(total.shape, jnp.float32)

    def step(chip):
        for half, q in enumerate((own, pair)):

            def work(mask, half=half, q=q):
                for h in range(heads):
                    at = part(half, h, heads)
                    s = scaled_scores(keys[chip], q, h, mask)
                    old = top[:, at]
                    new = jnp.maximum(old, jnp.max(s, axis=0, keepdims=True))
                    top[:, at] = new
                    total[:, at] = total[:, at] * jnp.exp2(old - new) + jnp.sum(
                        jnp.exp2(s - new), axis=0, keepdims=True
                    )

            when_seen(info, chip, half, tok, seq, work, None)

    each_chip(chips, step)
    wide = heads * HS
    for half in range(2):
        out[half, 0:1, :] = top[:, pl.ds(half * wide, wide)]
        out[half, 1:2, :] = total[:, pl.ds(half * wide, wide)]


def attend_kernel(
    heads, seq, info, own, pair, mine, other, keys, values,
    attn, dv, probs_out,
    values_t, da_rows, probs, lse, out_sems,
):
    chips, tok, _ = keys.shape
    wide = heads * HS
    for half, qd in enumerate((own, pair)):
        for h in range(heads):
            da_rows[part(half, h, heads), :] = qd[1, :, head(h)]
        top_a, top_b = mine[half, 0:1, :], other[1 - half, 0:1, :]
        top = jnp.maximum(top_a, top_b)
        total = mine[half, 1:2, :] * jnp.exp2(top_a - top)
        total = total + other[1 - half, 1:2, :] * jnp.exp2(top_b - top)
        lse[:, pl.ds(half * wide, wide)] = top + jnp.log(total) * LOG2E
    for chip in range(chips):
        values_t[:, pl.ds(chip * tok, tok)] = values[chip].T

    def rows_of(chip):
        return pl.ds(pl.multiple_of(chip * tok, tok), tok)

    def out_copy(chip):
        rows = rows_of(chip)
        return pltpu.make_async_copy(probs.at[rows, :], probs_out.at[rows, :], out_sems.at[chip])

    def step(chip):
        rows = rows_of(chip)
        for half, q in enumerate((own, pair)):

            def work(mask, half=half, q=q):
                for h in range(heads):
                    at = part(half, h, heads)
                    s = scaled_scores(keys[chip], q, h, mask)
                    probs[rows, at] = jnp.exp2(s - lse[:, at]).astype(jnp.bfloat16)

            def rest(half=half):
                probs[rows, pl.ds(half * wide, wide)] = jnp.zeros((tok, wide), jnp.bfloat16)

            when_seen(info, chip, half, tok, seq, work, rest)
        dv[chip] = dot_nn(probs[rows, :], da_rows[...]).astype(jnp.bfloat16)
        out_copy(chip).start()

    each_chip(chips, step)
    for half in range(2):
        for h in range(heads):
            attn[half, head(h), :] = dot_nn(values_t[...], probs[:, part(half, h, heads)]).astype(
                jnp.bfloat16
            )
    each_chip(chips, lambda chip: out_copy(chip).wait())


def put_rows(info, rows, chip, own, pair):
    core, x = info[3], info[4]
    steps, outer, _, size, _ = own.shape

    def put(same):
        for n in range(rows.shape[0] // size):
            place = n % (outer * steps)
            to = own if (n // (outer * steps)) == same else pair
            if to is None:
                continue
            step = (place % steps - x + steps) & (steps - 1)
            to[step, place // steps, chip] = rows[n * size : (n + 1) * size].astype(to.dtype)

    for same in range(2):
        pl.when(core == same)(functools.partial(put, same))


def grads_kernel(
    heads, seq, info, own, pair, mine, other, keys, values, probs_in,
    at_own, at_pair, dk, dq,
    keys_t, q_rows, probs, dscores, delta, in_sems,
):
    chips, tok, _ = keys.shape

    def rows_of(chip):
        return pl.ds(pl.multiple_of(chip * tok, tok), tok)

    def in_copy(chip):
        rows = rows_of(chip)
        return pltpu.make_async_copy(probs_in.at[rows, :], probs.at[rows, :], in_sems.at[chip])

    each_chip(chips, lambda chip: in_copy(chip).start())
    per_head = chips // heads
    block = HS // per_head
    for half, qd in enumerate((own, pair)):
        for h in range(heads):
            at = part(half, h, heads)
            q_rows[at, :] = qd[0, :, head(h)]
            both = mine[half, head(h), :].astype(jnp.float32) + other[1 - half, head(h), :].astype(
                jnp.float32
            )
            a = both.astype(jnp.bfloat16).astype(jnp.float32)
            delta[:, at] = jnp.sum(
                a * qd[1, :, head(h)].T.astype(jnp.float32), axis=0, keepdims=True
            )
            for n in range(per_head):
                put_rows(info, a[n * block : (n + 1) * block], h * per_head + n, (at_own, at_pair)[half], None)
    for chip in range(chips):
        keys_t[:, pl.ds(chip * tok, tok)] = keys[chip].T

    def step(chip):
        rows = rows_of(chip)
        in_copy(chip).wait()
        for half, qd in enumerate((own, pair)):
            seen, _ = block_state(info, chip, half, tok, seq)

            @pl.when(seen)
            def _(half=half, qd=qd):
                for h in range(heads):
                    at = part(half, h, heads)
                    dp = dot_nt(values[chip], qd[1, :, head(h)])
                    p = probs[rows, at].astype(jnp.float32)
                    dscores[rows, at] = (p * (dp - delta[:, at])).astype(jnp.bfloat16)

            @pl.when(jnp.logical_not(seen))
            def _(half=half):
                wide = heads * HS
                dscores[rows, pl.ds(half * wide, wide)] = jnp.zeros((tok, wide), jnp.bfloat16)

        dk[chip] = (dot_nn(dscores[rows, :], q_rows[...]) * HS ** (-0.5)).astype(jnp.bfloat16)

    each_chip(chips, step)
    for half in range(2):
        for h in range(heads):
            d = dot_nn(keys_t[...], dscores[:, part(half, h, heads)]) * HS ** (-0.5)
            dq[half, :, head(h)] = d.T.astype(jnp.bfloat16)


def prepare_kernel(chips, x, gain, w_key, w_value, hidden, k_copies, v_copies):
    xf = x[...].astype(jnp.float32)
    inv = lax.rsqrt(jnp.mean(xf * xf, axis=-1, keepdims=True) + EPS)
    h = (xf * inv * gain[...]).astype(jnp.bfloat16)
    hidden[...] = h
    for weight, out in ((w_key, k_copies), (w_value, v_copies)):
        rows = dot_nn(h, weight[...]).astype(jnp.bfloat16)
        for chip in range(chips):
            out[chip] = rows


def project_kernel(info, hidden, grad_out, w_query, w_out, both, ht_own, ht_pair):
    h = hidden[...]
    both[0] = dot_nn(h, w_query[...]).astype(jnp.bfloat16)
    both[1] = dot_nt(grad_out[...], w_out[...]).astype(jnp.bfloat16)
    both[2] = grad_out[...]
    chips = ht_own.shape[2]
    block = h.shape[1] // chips
    for chip in range(chips):
        rows = h[:, chip * block : (chip + 1) * block].astype(jnp.float32).T
        put_rows(info, rows, chip, ht_own, ht_pair)


def step_terms(lefts, rights, step):
    total = 0.0
    for left, right in zip(lefts, rights):
        rows = left.shape[1] * left.shape[2] * left.shape[3]
        total = total + dot_nn(left[step].reshape(rows, -1), right)
    return total


def direct_terms(info, lefts, rights, out, at):
    wide, steps = rights[0].shape[1], lefts[0].shape[0]
    for step in range(steps):
        place = (info[4] + step) & (steps - 1)
        to = pl.ds(pl.multiple_of(at + place * wide, 128), wide)
        out[:, to] = step_terms(lefts, rights, step).astype(out.dtype)


def terms_kernel(
    info, at_own, at_pair, own, pair, ht_own, ht_pair, dq_mine, dq_other, dq, base, *parts
):
    rights = [
        (dq_mine[half].astype(jnp.float32) + dq_other[1 - half].astype(jnp.float32)).astype(dq.dtype)
        for half in range(2)
    ]
    dq[...] = rights[0]
    for step, out in enumerate((base, *parts)):
        g_out = step_terms((at_own, at_pair), (own[2], pair[2]), step)
        out[:, pl.ds(0, g_out.shape[1])] = g_out.astype(out.dtype)
        g_query = step_terms((ht_own, ht_pair), rights, step)
        out[:, pl.ds(g_out.shape[1], g_query.shape[1])] = g_query.astype(out.dtype)


def rows_kernel(dk_parts, dv_parts, out):
    for at, parts in ((0, dk_parts), (HS, dv_parts)):
        total = parts[0].astype(jnp.float32)
        for n in range(1, parts.shape[0]):
            total = total + parts[n].astype(jnp.float32)
        out[:, pl.ds(at, HS)] = total.astype(out.dtype)


def kv_kernel(info, ht_own, ht_pair, dkv, dkv_pair, out):
    direct_terms(info, (ht_own, ht_pair), (dkv[...], dkv_pair[...]), out, 0)


def collect_kernel(base, one, two, three, out):
    total = base[...]
    for arrived in (one, two, three):
        total = total + arrived[...].astype(jnp.float32)
    out[...] = total.astype(out.dtype)


def added_parts(parts):
    total = parts[0].astype(jnp.float32)
    for n in range(1, parts.shape[0]):
        total = total + parts[n].astype(jnp.float32)
    return total.astype(jnp.bfloat16)


def total_kernel(parts, out):
    out[...] = added_parts(parts)


def spread_kernel(parts, kv, out):
    total = added_parts(parts)
    wide = total.shape[1]
    for n in range(out.shape[0]):
        out[n, :, pl.ds(0, wide)] = total
        out[n, :, pl.ds(wide, kv.shape[1])] = kv[...]


def weights_kernel(steps, shared, w_query, w_key, w_value, gain, d_query, d_key, d_value, d_out, d_gain):
    size = shared.shape[1]
    wide, heads_wide = d_out.shape[1], d_query.shape[1]
    gains = []
    for place in range(shared.shape[0]):
        outer, x = place // steps, place % steps
        rows = slice(place * size, (place + 1) * size)
        d_out[rows, :] = shared[place, :, pl.ds(0, wide)].astype(jnp.float32)
        query = shared[place, :, pl.ds(wide, heads_wide)].astype(jnp.float32)
        kv = 0.0
        for source in range(steps):
            at = pl.ds(wide + heads_wide + x * 2 * HS, 2 * HS)
            kv = kv + shared[outer * steps + source, :, at].astype(jnp.float32)
        d_query[rows, :] = query
        d_key[rows, :] = kv[:, :HS]
        d_value[rows, :] = kv[:, HS:]
        row_sum = (
            jnp.sum(w_query[rows, :].astype(jnp.float32) * query, axis=1, keepdims=True)
            + jnp.sum(w_key[rows, :].astype(jnp.float32) * kv[:, :HS], axis=1, keepdims=True)
            + jnp.sum(w_value[rows, :].astype(jnp.float32) * kv[:, HS:], axis=1, keepdims=True)
        )
        gains.append(jnp.broadcast_to(row_sum, (size, 128)))
    d_gain[...] = jnp.concatenate(gains, axis=0).T[0:1, :] / gain[...]


def finish_kernel(x, grad_out, gain, dq, dkv, w_query, w_key, w_value, d_in):
    dhidden = (
        dot_nt(dq[...], w_query[...])
        + dot_nt(dkv[:, :HS], w_key[...])
        + dot_nt(dkv[:, HS:], w_value[...])
    )
    xf = x[...].astype(jnp.float32)
    inv = lax.rsqrt(jnp.mean(xf * xf, axis=-1, keepdims=True) + EPS)
    normed = xf * inv
    scaled = dhidden * gain[...]
    mean = jnp.mean(scaled * normed, axis=-1, keepdims=True)
    d_in[...] = (grad_out[...].astype(jnp.float32) + inv * (scaled - normed * mean)).astype(d_in.dtype)


SMEM = pl.BlockSpec(memory_space=pltpu.SMEM)
VMEM = pl.BlockSpec(memory_space=pltpu.VMEM)
ANY = pl.BlockSpec(memory_space=pl.ANY)


def shape(*dims, dtype=jnp.bfloat16):
    return jax.ShapeDtypeStruct(dims, dtype)


def call(body, outs, args, flops, smem=0, scratch=(), in_any=(), out_any=()):
    specs = [SMEM if n < smem else ANY if n in in_any else VMEM for n in range(len(args))]
    if isinstance(outs, tuple):
        out_specs = tuple(ANY if n in out_any else VMEM for n in range(len(outs)))
    else:
        out_specs = VMEM
    return pl.pallas_call(
        body,
        out_shape=outs,
        in_specs=specs,
        out_specs=out_specs,
        scratch_shapes=list(scratch),
        compiler_params=pltpu.CompilerParams(vmem_limit_bytes=VMEM_BYTES),
        cost_estimate=pl.CostEstimate(flops=flops, bytes_accessed=1 << 20, transcendentals=0),
    )(*args)


def scratch(*dims, dtype=jnp.bfloat16):
    return pltpu.VMEM(dims, dtype)


def run_stats(info, own, pair, keys):
    tok, wide = own.shape[1:]
    chips, heads = keys.shape[0], wide // HS
    seq = 2 * tok * chips
    rows = scratch(1, 2 * wide, dtype=jnp.float32)
    return call(
        functools.partial(stats_kernel, heads, seq),
        shape(2, 2, wide, dtype=jnp.float32),
        (info, own, pair, keys),
        2 * seq * wide * HS,
        smem=1,
        scratch=(rows, rows),
    )


def run_attend(info, own, pair, mine, other, keys, values):
    tok, wide = own.shape[1:]
    chips, heads = keys.shape[0], wide // HS
    seq = 2 * tok * chips
    return call(
        functools.partial(attend_kernel, heads, seq),
        (shape(2, wide, tok), shape(chips, tok, HS), shape(chips * tok, 2 * wide)),
        (info, own, pair, mine, other, keys, values),
        6 * seq * wide * HS,
        smem=1,
        out_any=(2,),
        scratch=(
            scratch(HS, chips * tok),
            scratch(2 * wide, HS),
            scratch(chips * tok, 2 * wide),
            scratch(1, 2 * wide, dtype=jnp.float32),
            pltpu.SemaphoreType.DMA((chips,)),
        ),
    )


def run_grads(info, own, pair, mine, other, keys, values, probs, filed):
    tok, wide = own.shape[1:]
    chips, heads = keys.shape[0], wide // HS
    seq = 2 * tok * chips
    return call(
        functools.partial(grads_kernel, heads, seq),
        (filed, filed, shape(chips, tok, HS), shape(2, tok, wide)),
        (info, own, pair, mine, other, keys, values, probs),
        6 * seq * wide * HS,
        smem=1,
        in_any=(7,),
        scratch=(
            scratch(HS, chips * tok),
            scratch(2 * wide, HS),
            scratch(chips * tok, 2 * wide),
            scratch(chips * tok, 2 * wide),
            scratch(1, 2 * wide, dtype=jnp.float32),
            pltpu.SemaphoreType.DMA((chips,)),
        ),
    )


CORES = 2
X = 4


def swap_cores(value):
    count = lax.axis_size("blk")
    return lax.ppermute(value, "blk", [(i, i ^ 1) for i in range(count)])


def send_along_x(value, step):
    count = lax.axis_size("dp")
    return lax.ppermute(
        value, "dp", [(i, i // X * X + (i + step) % X) for i in range(count)]
    )


def exchange_chips(value):
    chips = lax.axis_size("blk") // CORES
    groups = [[core + CORES * chip for chip in range(chips)] for core in range(CORES)]
    return lax.all_to_all(value, "blk", 0, 0, tiled=True, axis_index_groups=groups)


def exchange_plane(value):
    blk, dp = lax.axis_size("blk"), lax.axis_size("dp")
    groups = [
        [(outer * X + x) * blk + chip * CORES + core for outer in range(dp // X) for chip in range(blk // CORES)]
        for x in range(X)
        for core in range(CORES)
    ]
    value = value.reshape(dp // X * (blk // CORES), -1, value.shape[1])
    return lax.all_to_all(value, ("dp", "blk"), 0, 0, tiled=True, axis_index_groups=groups)


def per_device(inputs, upstream, gain, w_query, w_key, w_value, w_out, prefix_len, bound):
    return whole(inputs[0], upstream[0], gain, w_query, w_key, w_value, w_out, prefix_len, bound)


def whole(inputs, grad_out, gain, w_query, w_key, w_value, w_out, prefix_len, bound):
    tok, wide = inputs.shape
    heads_wide = w_query.shape[1]
    my, dp = lax.axis_index("blk"), lax.axis_index("dp")
    count, share = lax.axis_size("blk"), lax.axis_size("dp")
    chips, outer = count // CORES, share // X
    size = wide // (count * share)
    core, x = my % CORES, dp % X
    info = jnp.stack([my, prefix_len[0], bound[0] * BLOCK, core, x]).astype(jnp.int32)
    gain_row = gain.reshape(1, wide)
    filed = shape(X, outer, chips, size, tok)
    copies = shape(chips, tok, HS)
    hidden, k_copies, v_copies = call(
        functools.partial(prepare_kernel, chips),
        (shape(tok, wide), copies, copies),
        (inputs, gain_row, w_key, w_value),
        4 * tok * wide * HS,
    )
    keys = exchange_chips(k_copies)
    values = exchange_chips(v_copies)
    own, ht_own, ht_pair = call(
        project_kernel,
        (shape(3, tok, heads_wide), filed, filed),
        (info, hidden, grad_out, w_query, w_out),
        4 * tok * wide * wide,
        smem=1,
    )
    pair = swap_cores(own)
    ht_pair = swap_cores(ht_pair)
    mine = run_stats(info, own, pair, keys)
    other = swap_cores(mine)
    attn, dv, probs = run_attend(info, own, pair, mine, other, keys, values)
    attn_other = swap_cores(attn)
    dv_parts = exchange_chips(dv)
    at_own, at_pair, dk, dq_mine = run_grads(
        info, own, pair, attn, attn_other, keys, values, probs, filed
    )
    dq_other = swap_cores(dq_mine)
    dk_parts = exchange_chips(dk)
    rows = outer * chips * size
    d_query_rows, base, *parts = call(
        terms_kernel,
        (
            shape(tok, heads_wide),
            shape(rows, wide + heads_wide, dtype=jnp.float32),
            *[shape(rows, wide + heads_wide)] * (X - 1),
        ),
        (info, at_own, at_pair, own, pair, ht_own, ht_pair, dq_mine, dq_other),
        8 * X * rows * wide * tok,
        smem=1,
    )
    arrived = []
    for step, terms in enumerate(parts, 1):
        arrived.append(send_along_x(terms, step))
    d_kv_rows = call(rows_kernel, shape(tok, 2 * HS), (dk_parts, dv_parts), 1 << 30)
    d_kv_pair = swap_cores(d_kv_rows)
    kv_terms = call(
        kv_kernel,
        shape(rows, X * 2 * HS),
        (info, ht_own, ht_pair, d_kv_rows, d_kv_pair),
        1 << 30,
        smem=1,
    )
    kv_parts = exchange_plane(kv_terms)
    terms = call(collect_kernel, shape(rows, wide + heads_wide), (base, *arrived), 1 << 30)
    parts = exchange_plane(terms)
    kv_total = call(total_kernel, shape(size, X * 2 * HS), (kv_parts,), 1 << 30)
    total = wide + heads_wide + X * 2 * HS
    copies = call(spread_kernel, shape(share, size, total), (parts, kv_total), 1 << 30)
    shared = lax.all_to_all(copies, "dp", 0, 0, tiled=True)
    d_in = call(
        finish_kernel,
        shape(tok, wide),
        (inputs, grad_out, gain_row, d_query_rows, d_kv_rows, w_query, w_key, w_value),
        2 * tok * wide * (wide + 2 * HS),
    )
    held = wide // count

    def my_rows(value):
        return lax.dynamic_slice_in_dim(value, my * held, held, 0)

    slices = [my_rows(w) for w in (w_query, w_key, w_value)]
    slices.append(my_rows(gain).reshape(1, held))
    f32 = functools.partial(shape, dtype=jnp.float32)
    d_query, d_key, d_value, d_out, d_gain = call(
        functools.partial(weights_kernel, X),
        (f32(held, heads_wide), f32(held, HS), f32(held, HS), f32(held, wide), f32(1, held)),
        (shared, *slices),
        1 << 30,
    )
    return (d_in[None], d_query, d_key, d_value, d_out, d_gain.reshape(held))


def solution(mesh):
    placed = (P("dp", "blk", None), P("dp", "blk", None), P(), P(), P(), P(), P(), P("dp"), P("dp"))
    return jax.shard_map(
        per_device,
        mesh=mesh,
        in_specs=placed,
        out_specs=(
            P("dp", "blk", None),
            P("blk", None),
            P("blk", None),
            P("blk", None),
            P("blk", None),
            P("blk"),
        ),
        check_vma=False,
    )
```

```python
import functools

import jax
import jax.numpy as jnp
from jax import lax
from jax.experimental import pallas as pl
from jax.experimental.pallas import tpu as pltpu
from jax.sharding import PartitionSpec as P

HS = 256
ACT = 64
BLOCK = 128
NEG = -1e30
EPS = 1e-06
LOG2E = 1.4426950408889634
VMEM_BYTES = 67043328
NT = (((1,), (1,)), ((), ()))


def dot_nt(a, b):
    return lax.dot_general(a, b, NT, preferred_element_type=jnp.float32)


def dot_nn(a, b):
    return jnp.dot(a, b, preferred_element_type=jnp.float32)


def head(h):
    return pl.ds(h * HS, HS)


def part(half, h, heads):
    return pl.ds((half * heads + h) * HS, HS)


def block_state(info, chip, half, tok, seq):
    rows, plen, edge, core = info[0] ^ half, info[1], info[2], info[3]
    low = (chip * 2 + core) * tok
    high = low + tok
    first, last = rows * tok, rows * tok + tok - 1
    seen = ((low < plen) | (high > seq - ACT)) & ((low < edge) | (low <= last))
    full = (high <= plen) & ((high <= edge) | (high - 1 <= first))
    return seen, full


def mask_of(info, chip, half, tok, seq):
    rows, plen, edge, core = info[0] ^ half, info[1], info[2], info[3]
    k_pos = (chip * 2 + core) * tok + lax.broadcasted_iota(jnp.int32, (tok, tok), 0)
    q_pos = rows * tok + lax.broadcasted_iota(jnp.int32, (tok, tok), 1)
    key_ok = (k_pos < plen) | (k_pos >= seq - ACT)
    return key_ok & ((k_pos < edge) | (k_pos <= q_pos))


def when_seen(info, chip, half, tok, seq, work, rest):
    seen, full = block_state(info, chip, half, tok, seq)

    @pl.when(full)
    def _():
        work(None)

    @pl.when(seen & jnp.logical_not(full))
    def _():
        work(mask_of(info, chip, half, tok, seq))

    if rest is not None:
        pl.when(jnp.logical_not(seen))(rest)


def each_chip(chips, step):
    def body(chip, carry):
        step(chip)
        return carry

    lax.fori_loop(0, chips, body, 0)


def scaled_scores(keys, q, h, mask):
    s = dot_nt(keys, q[0, :, head(h)]) * (HS ** (-0.5) * LOG2E)
    return s if mask is None else jnp.where(mask, s, NEG)


def stats_kernel(heads, seq, info, own, pair, keys, out, top, total):
    chips, tok, _ = keys.shape
    top[...] = jnp.full(top.shape, NEG, jnp.float32)
    total[...] = jnp.zeros(total.shape, jnp.float32)

    def step(chip):
        for half, q in enumerate((own, pair)):

            def work(mask, half=half, q=q):
                for h in range(heads):
                    at = part(half, h, heads)
                    s = scaled_scores(keys[chip], q, h, mask)
                    old = top[:, at]
                    new = jnp.maximum(old, jnp.max(s, axis=0, keepdims=True))
                    top[:, at] = new
                    total[:, at] = total[:, at] * jnp.exp2(old - new) + jnp.sum(
                        jnp.exp2(s - new), axis=0, keepdims=True
                    )

            when_seen(info, chip, half, tok, seq, work, None)

    each_chip(chips, step)
    wide = heads * HS
    for half in range(2):
        out[half, 0:1, :] = top[:, pl.ds(half * wide, wide)]
        out[half, 1:2, :] = total[:, pl.ds(half * wide, wide)]


def attend_kernel(
    heads, seq, info, own, pair, mine, other, keys, values_in,
    attn, dv_out, probs_out,
    values, values_t, da_rows, dv, probs, lse, value_sem, dv_sems, out_sems,
):
    chips, tok, _ = keys.shape
    wide = heads * HS
    for half, qd in enumerate((own, pair)):
        for h in range(heads):
            da_rows[part(half, h, heads), :] = qd[1, :, head(h)]
        top_a, top_b = mine[half, 0:1, :], other[1 - half, 0:1, :]
        top = jnp.maximum(top_a, top_b)
        total = mine[half, 1:2, :] * jnp.exp2(top_a - top)
        total = total + other[1 - half, 1:2, :] * jnp.exp2(top_b - top)
        lse[:, pl.ds(half * wide, wide)] = top + jnp.log(total) * LOG2E
    value_copy = pltpu.make_async_copy(values_in, values, value_sem)
    value_copy.start()

    def dv_copy(chip):
        return pltpu.make_async_copy(dv.at[chip], dv_out.at[chip], dv_sems.at[chip])

    def rows_of(chip):
        return pl.ds(pl.multiple_of(chip * tok, tok), tok)

    def out_copy(chip):
        rows = rows_of(chip)
        return pltpu.make_async_copy(probs.at[rows, :], probs_out.at[rows, :], out_sems.at[chip])

    def step(chip):
        rows = rows_of(chip)
        for half, q in enumerate((own, pair)):

            def work(mask, half=half, q=q):
                for h in range(heads):
                    at = part(half, h, heads)
                    s = scaled_scores(keys[chip], q, h, mask)
                    probs[rows, at] = jnp.exp2(s - lse[:, at]).astype(jnp.bfloat16)

            def rest(half=half):
                probs[rows, pl.ds(half * wide, wide)] = jnp.zeros((tok, wide), jnp.bfloat16)

            when_seen(info, chip, half, tok, seq, work, rest)
        dv[chip] = dot_nn(probs[rows, :], da_rows[...]).astype(jnp.bfloat16)
        out_copy(chip).start()
        dv_copy(chip).start()

    each_chip(chips, step)
    value_copy.wait()
    for chip in range(chips):
        values_t[:, pl.ds(chip * tok, tok)] = values[chip].T
    for half in range(2):
        for h in range(heads):
            attn[half, head(h), :] = dot_nn(values_t[...], probs[:, part(half, h, heads)]).astype(
                jnp.bfloat16
            )
    each_chip(chips, lambda chip: dv_copy(chip).wait())
    each_chip(chips, lambda chip: out_copy(chip).wait())


def put_rows(info, rows, chip, own, pair):
    core, x = info[3], info[4]
    steps, outer, _, size, _ = own.shape

    def put(same):
        for n in range(rows.shape[0] // size):
            place = n % (outer * steps)
            to = own if (n // (outer * steps)) == same else pair
            if to is None:
                continue
            step = (place % steps - x + steps) & (steps - 1)
            to[step, place // steps, chip] = rows[n * size : (n + 1) * size].astype(to.dtype)

    for same in range(2):
        pl.when(core == same)(functools.partial(put, same))


def grads_kernel(
    heads, seq, info, own, pair, mine, other, keys_in, values, probs_in,
    at_own, at_pair, dk_out, dq,
    keys, keys_t, q_rows, dk, probs, dscores, delta, key_sem, dk_sems, in_sems,
):
    chips, tok, _ = values.shape
    key_copy = pltpu.make_async_copy(keys_in, keys, key_sem)
    key_copy.start()

    def dk_copy(chip):
        return pltpu.make_async_copy(dk.at[chip], dk_out.at[chip], dk_sems.at[chip])

    def rows_of(chip):
        return pl.ds(pl.multiple_of(chip * tok, tok), tok)

    def in_copy(chip):
        rows = rows_of(chip)
        return pltpu.make_async_copy(probs_in.at[rows, :], probs.at[rows, :], in_sems.at[chip])

    each_chip(chips, lambda chip: in_copy(chip).start())
    per_head = chips // heads
    block = HS // per_head
    for half, qd in enumerate((own, pair)):
        for h in range(heads):
            at = part(half, h, heads)
            q_rows[at, :] = qd[0, :, head(h)]
            both = mine[half, head(h), :].astype(jnp.float32) + other[1 - half, head(h), :].astype(
                jnp.float32
            )
            a = both.astype(jnp.bfloat16).astype(jnp.float32)
            delta[:, at] = jnp.sum(
                a * qd[1, :, head(h)].T.astype(jnp.float32), axis=0, keepdims=True
            )
            for n in range(per_head):
                put_rows(info, a[n * block : (n + 1) * block], h * per_head + n, (at_own, at_pair)[half], None)

    def step(chip):
        rows = rows_of(chip)
        in_copy(chip).wait()
        for half, qd in enumerate((own, pair)):
            seen, _ = block_state(info, chip, half, tok, seq)

            @pl.when(seen)
            def _(half=half, qd=qd):
                for h in range(heads):
                    at = part(half, h, heads)
                    dp = dot_nt(values[chip], qd[1, :, head(h)])
                    p = probs[rows, at].astype(jnp.float32)
                    dscores[rows, at] = (p * (dp - delta[:, at])).astype(jnp.bfloat16)

            @pl.when(jnp.logical_not(seen))
            def _(half=half):
                wide = heads * HS
                dscores[rows, pl.ds(half * wide, wide)] = jnp.zeros((tok, wide), jnp.bfloat16)

        dk[chip] = (dot_nn(dscores[rows, :], q_rows[...]) * HS ** (-0.5)).astype(jnp.bfloat16)
        dk_copy(chip).start()

    each_chip(chips, step)
    key_copy.wait()
    for chip in range(chips):
        keys_t[:, pl.ds(chip * tok, tok)] = keys[chip].T
    for half in range(2):
        for h in range(heads):
            d = dot_nn(keys_t[...], dscores[:, part(half, h, heads)]) * HS ** (-0.5)
            dq[half, :, head(h)] = d.T.astype(jnp.bfloat16)
    each_chip(chips, lambda chip: dk_copy(chip).wait())


def prepare_kernel(chips, x, gain, w_key, hidden, k_copies):
    xf = x[...].astype(jnp.float32)
    inv = lax.rsqrt(jnp.mean(xf * xf, axis=-1, keepdims=True) + EPS)
    h = (xf * inv * gain[...]).astype(jnp.bfloat16)
    hidden[...] = h
    rows = dot_nn(h, w_key[...]).astype(jnp.bfloat16)
    for chip in range(chips):
        k_copies[chip] = rows


def project_kernel(info, hidden, grad_out, w_query, w_out, w_value, both, v_copies, ht_own, ht_pair):
    h = hidden[...]
    values = dot_nn(h, w_value[...]).astype(jnp.bfloat16)
    for chip in range(v_copies.shape[0]):
        v_copies[chip] = values
    both[0] = dot_nn(h, w_query[...]).astype(jnp.bfloat16)
    both[1] = dot_nt(grad_out[...], w_out[...]).astype(jnp.bfloat16)
    chips = ht_own.shape[2]
    block = h.shape[1] // chips
    for chip in range(chips):
        rows = h[:, chip * block : (chip + 1) * block].astype(jnp.float32).T
        put_rows(info, rows, chip, ht_own, ht_pair)


def step_terms(lefts, rights, step):
    total = 0.0
    for left, right in zip(lefts, rights):
        rows = left.shape[1] * left.shape[2] * left.shape[3]
        total = total + dot_nn(left[step].reshape(rows, -1), right)
    return total


def direct_terms(info, lefts, rights, out, at):
    wide, steps = rights[0].shape[1], lefts[0].shape[0]
    for step in range(steps):
        place = (info[4] + step) & (steps - 1)
        to = pl.ds(pl.multiple_of(at + place * wide, 128), wide)
        out[:, to] = step_terms(lefts, rights, step).astype(out.dtype)


def terms_kernel(
    info, at_own, at_pair, go_own, go_pair, ht_own, ht_pair, dq_mine, dq_other, dq, base, *parts
):
    rights = [
        (dq_mine[half].astype(jnp.float32) + dq_other[1 - half].astype(jnp.float32)).astype(dq.dtype)
        for half in range(2)
    ]
    dq[...] = rights[0]
    for step, out in enumerate((base, *parts)):
        g_out = step_terms((at_own, at_pair), (go_own[...], go_pair[...]), step)
        out[:, pl.ds(0, g_out.shape[1])] = g_out.astype(out.dtype)
        g_query = step_terms((ht_own, ht_pair), rights, step)
        out[:, pl.ds(g_out.shape[1], g_query.shape[1])] = g_query.astype(out.dtype)


def rows_kernel(dk_parts, dv_rows, out):
    out[:, pl.ds(0, HS)] = added_parts(dk_parts)
    out[:, pl.ds(HS, HS)] = dv_rows[...]


def kv_kernel(info, ht_own, ht_pair, dkv, dkv_pair, out):
    direct_terms(info, (ht_own, ht_pair), (dkv[...], dkv_pair[...]), out, 0)


def collect_kernel(base, one, two, three, out):
    total = base[...]
    for arrived in (one, two, three):
        total = total + arrived[...].astype(jnp.float32)
    out[...] = total.astype(out.dtype)


def added_parts(parts):
    total = parts[0].astype(jnp.float32)
    for n in range(1, parts.shape[0]):
        total = total + parts[n].astype(jnp.float32)
    return total.astype(jnp.bfloat16)


def total_kernel(parts, out):
    out[...] = added_parts(parts)


def spread_kernel(parts, kv, out):
    total = added_parts(parts)
    wide = total.shape[1]
    for n in range(out.shape[0]):
        out[n, :, pl.ds(0, wide)] = total
        out[n, :, pl.ds(wide, kv.shape[1])] = kv[...]


def weights_kernel(steps, shared, w_query, w_key, w_value, gain, d_query, d_key, d_value, d_out, d_gain):
    size = shared.shape[1]
    wide, heads_wide = d_out.shape[1], d_query.shape[1]
    gains = []
    for place in range(shared.shape[0]):
        outer, x = place // steps, place % steps
        rows = slice(place * size, (place + 1) * size)
        d_out[rows, :] = shared[place, :, pl.ds(0, wide)].astype(jnp.float32)
        query = shared[place, :, pl.ds(wide, heads_wide)].astype(jnp.float32)
        kv = 0.0
        for source in range(steps):
            at = pl.ds(wide + heads_wide + x * 2 * HS, 2 * HS)
            kv = kv + shared[outer * steps + source, :, at].astype(jnp.float32)
        d_query[rows, :] = query
        d_key[rows, :] = kv[:, :HS]
        d_value[rows, :] = kv[:, HS:]
        row_sum = (
            jnp.sum(w_query[rows, :].astype(jnp.float32) * query, axis=1, keepdims=True)
            + jnp.sum(w_key[rows, :].astype(jnp.float32) * kv[:, :HS], axis=1, keepdims=True)
            + jnp.sum(w_value[rows, :].astype(jnp.float32) * kv[:, HS:], axis=1, keepdims=True)
        )
        gains.append(jnp.broadcast_to(row_sum, (size, 128)))
    d_gain[...] = jnp.concatenate(gains, axis=0).T[0:1, :] / gain[...]


def finish_kernel(x, grad_out, gain, dq, dkv, w_query, w_key, w_value, d_in):
    dhidden = (
        dot_nt(dq[...], w_query[...])
        + dot_nt(dkv[:, :HS], w_key[...])
        + dot_nt(dkv[:, HS:], w_value[...])
    )
    xf = x[...].astype(jnp.float32)
    inv = lax.rsqrt(jnp.mean(xf * xf, axis=-1, keepdims=True) + EPS)
    normed = xf * inv
    scaled = dhidden * gain[...]
    mean = jnp.mean(scaled * normed, axis=-1, keepdims=True)
    d_in[...] = (grad_out[...].astype(jnp.float32) + inv * (scaled - normed * mean)).astype(d_in.dtype)


SMEM = pl.BlockSpec(memory_space=pltpu.SMEM)
VMEM = pl.BlockSpec(memory_space=pltpu.VMEM)
ANY = pl.BlockSpec(memory_space=pl.ANY)


def shape(*dims, dtype=jnp.bfloat16):
    return jax.ShapeDtypeStruct(dims, dtype)


def call(body, outs, args, flops, smem=0, scratch=(), in_any=(), out_any=()):
    specs = [SMEM if n < smem else ANY if n in in_any else VMEM for n in range(len(args))]
    if isinstance(outs, tuple):
        out_specs = tuple(ANY if n in out_any else VMEM for n in range(len(outs)))
    else:
        out_specs = VMEM
    return pl.pallas_call(
        body,
        out_shape=outs,
        in_specs=specs,
        out_specs=out_specs,
        scratch_shapes=list(scratch),
        compiler_params=pltpu.CompilerParams(vmem_limit_bytes=VMEM_BYTES),
        cost_estimate=pl.CostEstimate(flops=flops, bytes_accessed=1 << 20, transcendentals=0),
    )(*args)


def scratch(*dims, dtype=jnp.bfloat16):
    return pltpu.VMEM(dims, dtype)


def run_stats(info, own, pair, keys):
    tok, wide = own.shape[1:]
    chips, heads = keys.shape[0], wide // HS
    seq = 2 * tok * chips
    rows = scratch(1, 2 * wide, dtype=jnp.float32)
    return call(
        functools.partial(stats_kernel, heads, seq),
        shape(2, 2, wide, dtype=jnp.float32),
        (info, own, pair, keys),
        2 * seq * wide * HS,
        smem=1,
        scratch=(rows, rows),
    )


def run_attend(info, own, pair, mine, other, keys, values):
    tok, wide = own.shape[1:]
    chips, heads = keys.shape[0], wide // HS
    seq = 2 * tok * chips
    return call(
        functools.partial(attend_kernel, heads, seq),
        (shape(2, wide, tok), shape(chips, tok, HS), shape(chips * tok, 2 * wide)),
        (info, own, pair, mine, other, keys, values),
        6 * seq * wide * HS,
        smem=1,
        in_any=(6,),
        out_any=(1, 2),
        scratch=(
            scratch(chips, tok, HS),
            scratch(HS, chips * tok),
            scratch(2 * wide, HS),
            scratch(chips, tok, HS),
            scratch(chips * tok, 2 * wide),
            scratch(1, 2 * wide, dtype=jnp.float32),
            pltpu.SemaphoreType.DMA,
            pltpu.SemaphoreType.DMA((chips,)),
            pltpu.SemaphoreType.DMA((chips,)),
        ),
    )


def run_grads(info, own, pair, mine, other, keys, values, probs, filed):
    tok, wide = own.shape[1:]
    chips, heads = keys.shape[0], wide // HS
    seq = 2 * tok * chips
    return call(
        functools.partial(grads_kernel, heads, seq),
        (filed, filed, shape(chips, tok, HS), shape(2, tok, wide)),
        (info, own, pair, mine, other, keys, values, probs),
        6 * seq * wide * HS,
        smem=1,
        in_any=(5, 7),
        out_any=(2,),
        scratch=(
            scratch(chips, tok, HS),
            scratch(HS, chips * tok),
            scratch(2 * wide, HS),
            scratch(chips, tok, HS),
            scratch(chips * tok, 2 * wide),
            scratch(chips * tok, 2 * wide),
            scratch(1, 2 * wide, dtype=jnp.float32),
            pltpu.SemaphoreType.DMA,
            pltpu.SemaphoreType.DMA((chips,)),
            pltpu.SemaphoreType.DMA((chips,)),
        ),
    )


CORES = 2
X = 4


def swap_cores(value):
    count = lax.axis_size("blk")
    return lax.ppermute(value, "blk", [(i, i ^ 1) for i in range(count)])


def send_along_x(value, step):
    count = lax.axis_size("dp")
    return lax.ppermute(
        value, "dp", [(i, i // X * X + (i + step) % X) for i in range(count)]
    )


def exchange_chips(value):
    chips = lax.axis_size("blk") // CORES
    groups = [[core + CORES * chip for chip in range(chips)] for core in range(CORES)]
    return lax.all_to_all(value, "blk", 0, 0, tiled=True, axis_index_groups=groups)


def exchange_plane(value):
    blk, dp = lax.axis_size("blk"), lax.axis_size("dp")
    groups = [
        [(outer * X + x) * blk + chip * CORES + core for outer in range(dp // X) for chip in range(blk // CORES)]
        for x in range(X)
        for core in range(CORES)
    ]
    value = value.reshape(dp // X * (blk // CORES), -1, value.shape[1])
    return lax.all_to_all(value, ("dp", "blk"), 0, 0, tiled=True, axis_index_groups=groups)


def per_device(inputs, upstream, gain, w_query, w_key, w_value, w_out, prefix_len, bound):
    return whole(inputs[0], upstream[0], gain, w_query, w_key, w_value, w_out, prefix_len, bound)


def whole(inputs, grad_out, gain, w_query, w_key, w_value, w_out, prefix_len, bound):
    tok, wide = inputs.shape
    heads_wide = w_query.shape[1]
    my, dp = lax.axis_index("blk"), lax.axis_index("dp")
    count, share = lax.axis_size("blk"), lax.axis_size("dp")
    chips, outer = count // CORES, share // X
    size = wide // (count * share)
    core, x = my % CORES, dp % X
    info = jnp.stack([my, prefix_len[0], bound[0] * BLOCK, core, x]).astype(jnp.int32)
    gain_row = gain.reshape(1, wide)
    filed = shape(X, outer, chips, size, tok)
    copies = shape(chips, tok, HS)
    hidden, k_copies = call(
        functools.partial(prepare_kernel, chips),
        (shape(tok, wide), copies),
        (inputs, gain_row, w_key),
        4 * tok * wide * HS,
    )
    keys = exchange_chips(k_copies)
    own, v_copies, ht_own, ht_pair = call(
        project_kernel,
        (shape(2, tok, heads_wide), copies, filed, filed),
        (info, hidden, grad_out, w_query, w_out, w_value),
        4 * tok * wide * wide,
        smem=1,
    )
    values = exchange_chips(v_copies)
    pair = swap_cores(own)
    grad_pair = swap_cores(grad_out)
    ht_pair = swap_cores(ht_pair)
    mine = run_stats(info, own, pair, keys)
    other = swap_cores(mine)
    attn, dv, probs = run_attend(info, own, pair, mine, other, keys, values)
    attn_other = swap_cores(attn)
    dv_parts = exchange_chips(dv)
    at_own, at_pair, dk, dq_mine = run_grads(
        info, own, pair, attn, attn_other, keys, values, probs, filed
    )
    dq_other = swap_cores(dq_mine)
    dk_parts = exchange_chips(dk)
    rows = outer * chips * size
    d_query_rows, base, *parts = call(
        terms_kernel,
        (
            shape(tok, heads_wide),
            shape(rows, wide + heads_wide, dtype=jnp.float32),
            *[shape(rows, wide + heads_wide)] * (X - 1),
        ),
        (info, at_own, at_pair, grad_out, grad_pair, ht_own, ht_pair, dq_mine, dq_other),
        8 * X * rows * wide * tok,
        smem=1,
    )
    arrived = []
    for step, terms in enumerate(parts, 1):
        arrived.append(send_along_x(terms, step))
    d_value_rows = call(total_kernel, shape(tok, HS), (dv_parts,), 1 << 30)
    d_kv_rows = call(rows_kernel, shape(tok, 2 * HS), (dk_parts, d_value_rows), 1 << 30)
    d_kv_pair = swap_cores(d_kv_rows)
    kv_terms = call(
        kv_kernel,
        shape(rows, X * 2 * HS),
        (info, ht_own, ht_pair, d_kv_rows, d_kv_pair),
        1 << 30,
        smem=1,
    )
    kv_parts = exchange_plane(kv_terms)
    terms = call(collect_kernel, shape(rows, wide + heads_wide), (base, *arrived), 1 << 30)
    parts = exchange_plane(terms)
    kv_total = call(total_kernel, shape(size, X * 2 * HS), (kv_parts,), 1 << 30)
    total = wide + heads_wide + X * 2 * HS
    copies = call(spread_kernel, shape(share, size, total), (parts, kv_total), 1 << 30)
    shared = lax.all_to_all(copies, "dp", 0, 0, tiled=True)
    d_in = call(
        finish_kernel,
        shape(tok, wide),
        (inputs, grad_out, gain_row, d_query_rows, d_kv_rows, w_query, w_key, w_value),
        2 * tok * wide * (wide + 2 * HS),
    )
    held = wide // count

    def my_rows(value):
        return lax.dynamic_slice_in_dim(value, my * held, held, 0)

    slices = [my_rows(w) for w in (w_query, w_key, w_value)]
    slices.append(my_rows(gain).reshape(1, held))
    f32 = functools.partial(shape, dtype=jnp.float32)
    d_query, d_key, d_value, d_out, d_gain = call(
        functools.partial(weights_kernel, X),
        (f32(held, heads_wide), f32(held, HS), f32(held, HS), f32(held, wide), f32(1, held)),
        (shared, *slices),
        1 << 30,
    )
    return (d_in[None], d_query, d_key, d_value, d_out, d_gain.reshape(held))


def solution(mesh):
    placed = (P("dp", "blk", None), P("dp", "blk", None), P(), P(), P(), P(), P(), P("dp"), P("dp"))
    return jax.shard_map(
        per_device,
        mesh=mesh,
        in_specs=placed,
        out_specs=(
            P("dp", "blk", None),
            P("blk", None),
            P("blk", None),
            P("blk", None),
            P("blk", None),
            P("blk"),
        ),
        check_vma=False,
    )
```

```python
import functools

import jax
import jax.numpy as jnp
from jax import lax
from jax.experimental import pallas as pl
from jax.experimental.pallas import tpu as pltpu
from jax.sharding import PartitionSpec as P

HS = 256
ACT = 64
BLOCK = 128
NEG = -1e30
EPS = 1e-06
LOG2E = 1.4426950408889634
VMEM_BYTES = 67043328
NT = (((1,), (1,)), ((), ()))


def dot_nt(a, b):
    return lax.dot_general(a, b, NT, preferred_element_type=jnp.float32)


def dot_nn(a, b):
    return jnp.dot(a, b, preferred_element_type=jnp.float32)


def head(h):
    return pl.ds(h * HS, HS)


def part(half, h, heads):
    return pl.ds((half * heads + h) * HS, HS)


def block_state(info, chip, half, tok, seq):
    rows, plen, edge, core = info[0] ^ half, info[1], info[2], info[3]
    low = (chip * 2 + core) * tok
    high = low + tok
    first, last = rows * tok, rows * tok + tok - 1
    seen = ((low < plen) | (high > seq - ACT)) & ((low < edge) | (low <= last))
    full = (high <= plen) & ((high <= edge) | (high - 1 <= first))
    return seen, full


def mask_of(info, chip, half, tok, seq):
    rows, plen, edge, core = info[0] ^ half, info[1], info[2], info[3]
    k_pos = (chip * 2 + core) * tok + lax.broadcasted_iota(jnp.int32, (tok, tok), 0)
    q_pos = rows * tok + lax.broadcasted_iota(jnp.int32, (tok, tok), 1)
    key_ok = (k_pos < plen) | (k_pos >= seq - ACT)
    return key_ok & ((k_pos < edge) | (k_pos <= q_pos))


def when_seen(info, chip, half, tok, seq, work, rest):
    seen, full = block_state(info, chip, half, tok, seq)

    @pl.when(full)
    def _():
        work(None)

    @pl.when(seen & jnp.logical_not(full))
    def _():
        work(mask_of(info, chip, half, tok, seq))

    if rest is not None:
        pl.when(jnp.logical_not(seen))(rest)


def each_chip(chips, step):
    def body(chip, carry):
        step(chip)
        return carry

    lax.fori_loop(0, chips, body, 0)


def scaled_scores(keys, q, h, mask):
    s = dot_nt(keys, q[0, :, head(h)]) * (HS ** (-0.5) * LOG2E)
    return s if mask is None else jnp.where(mask, s, NEG)


def stats_kernel(heads, seq, info, own, pair, keys, out, top, total):
    chips, tok, _ = keys.shape
    top[...] = jnp.full(top.shape, NEG, jnp.float32)
    total[...] = jnp.zeros(total.shape, jnp.float32)

    def step(chip):
        for half, q in enumerate((own, pair)):

            def work(mask, half=half, q=q):
                for h in range(heads):
                    at = part(half, h, heads)
                    s = scaled_scores(keys[chip], q, h, mask)
                    old = top[:, at]
                    new = jnp.maximum(old, jnp.max(s, axis=0, keepdims=True))
                    top[:, at] = new
                    total[:, at] = total[:, at] * jnp.exp2(old - new) + jnp.sum(
                        jnp.exp2(s - new), axis=0, keepdims=True
                    )

            when_seen(info, chip, half, tok, seq, work, None)

    each_chip(chips, step)
    wide = heads * HS
    for half in range(2):
        out[half, 0:1, :] = top[:, pl.ds(half * wide, wide)]
        out[half, 1:2, :] = total[:, pl.ds(half * wide, wide)]


def attend_kernel(
    heads, seq, info, own, pair, mine, other, keys, values_in,
    attn, dv_out, probs_out,
    values, values_t, da_rows, dv, probs, lse, value_sem, dv_sems, out_sems,
):
    chips, tok, _ = keys.shape
    wide = heads * HS
    for half, qd in enumerate((own, pair)):
        for h in range(heads):
            da_rows[part(half, h, heads), :] = qd[1, :, head(h)]
        top_a, top_b = mine[half, 0:1, :], other[1 - half, 0:1, :]
        top = jnp.maximum(top_a, top_b)
        total = mine[half, 1:2, :] * jnp.exp2(top_a - top)
        total = total + other[1 - half, 1:2, :] * jnp.exp2(top_b - top)
        lse[:, pl.ds(half * wide, wide)] = top + jnp.log(total) * LOG2E
    value_copy = pltpu.make_async_copy(values_in, values, value_sem)
    value_copy.start()

    def dv_copy(chip):
        return pltpu.make_async_copy(dv.at[chip], dv_out.at[chip], dv_sems.at[chip])

    def rows_of(chip):
        return pl.ds(pl.multiple_of(chip * tok, tok), tok)

    def out_copy(chip):
        rows = rows_of(chip)
        return pltpu.make_async_copy(probs.at[rows, :], probs_out.at[rows, :], out_sems.at[chip])

    def step(chip):
        rows = rows_of(chip)
        for half, q in enumerate((own, pair)):

            def work(mask, half=half, q=q):
                for h in range(heads):
                    at = part(half, h, heads)
                    s = scaled_scores(keys[chip], q, h, mask)
                    probs[rows, at] = jnp.exp2(s - lse[:, at]).astype(jnp.bfloat16)

            def rest(half=half):
                probs[rows, pl.ds(half * wide, wide)] = jnp.zeros((tok, wide), jnp.bfloat16)

            when_seen(info, chip, half, tok, seq, work, rest)
        dv[chip] = dot_nn(probs[rows, :], da_rows[...]).astype(jnp.bfloat16)
        out_copy(chip).start()
        dv_copy(chip).start()

    each_chip(chips, step)
    value_copy.wait()
    for chip in range(chips):
        values_t[:, pl.ds(chip * tok, tok)] = values[chip].T
    for half in range(2):
        for h in range(heads):
            attn[half, head(h), :] = dot_nn(values_t[...], probs[:, part(half, h, heads)]).astype(
                jnp.bfloat16
            )
    each_chip(chips, lambda chip: dv_copy(chip).wait())
    each_chip(chips, lambda chip: out_copy(chip).wait())


def put_rows(info, rows, chip, own, pair):
    core, x = info[3], info[4]
    steps, outer, _, size, _ = own.shape

    def put(same):
        for n in range(rows.shape[0] // size):
            place = n % (outer * steps)
            to = own if (n // (outer * steps)) == same else pair
            if to is None:
                continue
            step = (place % steps - x + steps) & (steps - 1)
            to[step, place // steps, chip] = rows[n * size : (n + 1) * size].astype(to.dtype)

    for same in range(2):
        pl.when(core == same)(functools.partial(put, same))


def grads_kernel(
    heads, seq, info, own, pair, mine, other, keys_in, values, probs_in,
    dk_out, dq,
    keys, keys_t, q_rows, dk, probs, dscores, delta, key_sem, dk_sems, in_sems,
):
    chips, tok, _ = values.shape
    key_copy = pltpu.make_async_copy(keys_in, keys, key_sem)
    key_copy.start()

    def dk_copy(chip):
        return pltpu.make_async_copy(dk.at[chip], dk_out.at[chip], dk_sems.at[chip])

    def rows_of(chip):
        return pl.ds(pl.multiple_of(chip * tok, tok), tok)

    def in_copy(chip):
        rows = rows_of(chip)
        return pltpu.make_async_copy(probs_in.at[rows, :], probs.at[rows, :], in_sems.at[chip])

    each_chip(chips, lambda chip: in_copy(chip).start())
    for half, qd in enumerate((own, pair)):
        for h in range(heads):
            at = part(half, h, heads)
            q_rows[at, :] = qd[0, :, head(h)]
            both = mine[half, head(h), :].astype(jnp.float32) + other[1 - half, head(h), :].astype(
                jnp.float32
            )
            a = both.astype(jnp.bfloat16).astype(jnp.float32)
            delta[:, at] = jnp.sum(
                a * qd[1, :, head(h)].T.astype(jnp.float32), axis=0, keepdims=True
            )

    def step(chip):
        rows = rows_of(chip)
        in_copy(chip).wait()
        for half, qd in enumerate((own, pair)):
            seen, _ = block_state(info, chip, half, tok, seq)

            @pl.when(seen)
            def _(half=half, qd=qd):
                for h in range(heads):
                    at = part(half, h, heads)
                    dp = dot_nt(values[chip], qd[1, :, head(h)])
                    p = probs[rows, at].astype(jnp.float32)
                    dscores[rows, at] = (p * (dp - delta[:, at])).astype(jnp.bfloat16)

            @pl.when(jnp.logical_not(seen))
            def _(half=half):
                wide = heads * HS
                dscores[rows, pl.ds(half * wide, wide)] = jnp.zeros((tok, wide), jnp.bfloat16)

        dk[chip] = (dot_nn(dscores[rows, :], q_rows[...]) * HS ** (-0.5)).astype(jnp.bfloat16)
        dk_copy(chip).start()

    each_chip(chips, step)
    key_copy.wait()
    for chip in range(chips):
        keys_t[:, pl.ds(chip * tok, tok)] = keys[chip].T
    for half in range(2):
        for h in range(heads):
            d = dot_nn(keys_t[...], dscores[:, part(half, h, heads)]) * HS ** (-0.5)
            dq[half, :, head(h)] = d.T.astype(jnp.bfloat16)
    each_chip(chips, lambda chip: dk_copy(chip).wait())


def prepare_kernel(chips, x, gain, w_key, hidden, k_copies):
    xf = x[...].astype(jnp.float32)
    inv = lax.rsqrt(jnp.mean(xf * xf, axis=-1, keepdims=True) + EPS)
    h = (xf * inv * gain[...]).astype(jnp.bfloat16)
    hidden[...] = h
    rows = dot_nn(h, w_key[...]).astype(jnp.bfloat16)
    for chip in range(chips):
        k_copies[chip] = rows


def project_kernel(info, hidden, grad_out, w_query, w_out, w_value, both, v_copies, ht_own, ht_pair):
    h = hidden[...]
    values = dot_nn(h, w_value[...]).astype(jnp.bfloat16)
    for chip in range(v_copies.shape[0]):
        v_copies[chip] = values
    both[0] = dot_nn(h, w_query[...]).astype(jnp.bfloat16)
    both[1] = dot_nt(grad_out[...], w_out[...]).astype(jnp.bfloat16)
    chips = ht_own.shape[2]
    block = h.shape[1] // chips
    for chip in range(chips):
        rows = h[:, chip * block : (chip + 1) * block].astype(jnp.float32).T
        put_rows(info, rows, chip, ht_own, ht_pair)


def step_terms(lefts, rights, step):
    total = 0.0
    for left, right in zip(lefts, rights):
        rows = left.shape[1] * left.shape[2] * left.shape[3]
        total = total + dot_nn(left[step].reshape(rows, -1), right)
    return total


def direct_terms(info, lefts, rights, out, at):
    wide, steps = rights[0].shape[1], lefts[0].shape[0]
    for step in range(steps):
        place = (info[4] + step) & (steps - 1)
        to = pl.ds(pl.multiple_of(at + place * wide, 128), wide)
        out[:, to] = step_terms(lefts, rights, step).astype(out.dtype)


def terms_kernel(
    info, attn, attn_other, go_own, go_pair, ht_own, ht_pair, dq_mine, dq_other, dq, *refs
):
    outs, filed = refs[:-2], refs[-2:]
    block = attn.shape[1] // ht_own.shape[2]
    for half in range(2):
        for chip in range(ht_own.shape[2]):
            rows = pl.ds(chip * block, block)
            both = attn[half, rows, :].astype(jnp.float32) + attn_other[1 - half, rows, :].astype(
                jnp.float32
            )
            put_rows(info, both, chip, filed[half], None)
    rights = [
        (dq_mine[half].astype(jnp.float32) + dq_other[1 - half].astype(jnp.float32)).astype(dq.dtype)
        for half in range(2)
    ]
    dq[...] = rights[0]
    for step, out in enumerate(outs):
        g_out = step_terms(filed, (go_own[...], go_pair[...]), step)
        out[:, pl.ds(0, g_out.shape[1])] = g_out.astype(out.dtype)
        g_query = step_terms((ht_own, ht_pair), rights, step)
        out[:, pl.ds(g_out.shape[1], g_query.shape[1])] = g_query.astype(out.dtype)


def rows_kernel(dk_parts, dv_rows, out):
    out[:, pl.ds(0, HS)] = added_parts(dk_parts)
    out[:, pl.ds(HS, HS)] = dv_rows[...]


def kv_kernel(info, ht_own, ht_pair, dkv, dkv_pair, out):
    direct_terms(info, (ht_own, ht_pair), (dkv[...], dkv_pair[...]), out, 0)


def collect_kernel(base, one, two, three, out):
    total = base[...]
    for arrived in (one, two, three):
        total = total + arrived[...].astype(jnp.float32)
    out[...] = total.astype(out.dtype)


def added_parts(parts):
    total = parts[0].astype(jnp.float32)
    for n in range(1, parts.shape[0]):
        total = total + parts[n].astype(jnp.float32)
    return total.astype(jnp.bfloat16)


def total_kernel(parts, out):
    out[...] = added_parts(parts)


def spread_kernel(parts, kv, out):
    total = added_parts(parts)
    wide = total.shape[1]
    for n in range(out.shape[0]):
        out[n, :, pl.ds(0, wide)] = total
        out[n, :, pl.ds(wide, kv.shape[1])] = kv[...]


def weights_kernel(
    steps, info, shared, gain, wq_in, wk_in, wv_in,
    d_query, d_key, d_value, d_out, d_gain,
    w_query, w_key, w_value, sems,
):
    size = shared.shape[1]
    held = d_out.shape[0]
    mine = pl.ds(pl.multiple_of(info[0] * held, held), held)
    copies = [
        pltpu.make_async_copy(w.at[mine, :], into, sems.at[n])
        for n, (w, into) in enumerate(((wq_in, w_query), (wk_in, w_key), (wv_in, w_value)))
    ]
    for c in copies:
        c.start()
    for c in copies:
        c.wait()
    wide, heads_wide = d_out.shape[1], d_query.shape[1]
    gains = []
    for place in range(shared.shape[0]):
        outer, x = place // steps, place % steps
        rows = slice(place * size, (place + 1) * size)
        d_out[rows, :] = shared[place, :, pl.ds(0, wide)].astype(jnp.float32)
        query = shared[place, :, pl.ds(wide, heads_wide)].astype(jnp.float32)
        kv = 0.0
        for source in range(steps):
            at = pl.ds(wide + heads_wide + x * 2 * HS, 2 * HS)
            kv = kv + shared[outer * steps + source, :, at].astype(jnp.float32)
        d_query[rows, :] = query
        d_key[rows, :] = kv[:, :HS]
        d_value[rows, :] = kv[:, HS:]
        row_sum = (
            jnp.sum(w_query[rows, :].astype(jnp.float32) * query, axis=1, keepdims=True)
            + jnp.sum(w_key[rows, :].astype(jnp.float32) * kv[:, :HS], axis=1, keepdims=True)
            + jnp.sum(w_value[rows, :].astype(jnp.float32) * kv[:, HS:], axis=1, keepdims=True)
        )
        gains.append(jnp.broadcast_to(row_sum, (size, 128)))
    d_gain[...] = jnp.concatenate(gains, axis=0).T[0:1, :] / gain[pl.ds(info[0], 1), :]


def finish_kernel(x, grad_out, gain, dq, dkv, w_query, w_key, w_value, d_in):
    dhidden = (
        dot_nt(dq[...], w_query[...])
        + dot_nt(dkv[:, :HS], w_key[...])
        + dot_nt(dkv[:, HS:], w_value[...])
    )
    xf = x[...].astype(jnp.float32)
    inv = lax.rsqrt(jnp.mean(xf * xf, axis=-1, keepdims=True) + EPS)
    normed = xf * inv
    scaled = dhidden * gain[...]
    mean = jnp.mean(scaled * normed, axis=-1, keepdims=True)
    d_in[...] = (grad_out[...].astype(jnp.float32) + inv * (scaled - normed * mean)).astype(d_in.dtype)


SMEM = pl.BlockSpec(memory_space=pltpu.SMEM)
VMEM = pl.BlockSpec(memory_space=pltpu.VMEM)
ANY = pl.BlockSpec(memory_space=pl.ANY)


def shape(*dims, dtype=jnp.bfloat16):
    return jax.ShapeDtypeStruct(dims, dtype)


def call(body, outs, args, flops, smem=0, scratch=(), in_any=(), out_any=()):
    specs = [SMEM if n < smem else ANY if n in in_any else VMEM for n in range(len(args))]
    if isinstance(outs, tuple):
        out_specs = tuple(ANY if n in out_any else VMEM for n in range(len(outs)))
    else:
        out_specs = VMEM
    return pl.pallas_call(
        body,
        out_shape=outs,
        in_specs=specs,
        out_specs=out_specs,
        scratch_shapes=list(scratch),
        compiler_params=pltpu.CompilerParams(vmem_limit_bytes=VMEM_BYTES),
        cost_estimate=pl.CostEstimate(flops=flops, bytes_accessed=1 << 20, transcendentals=0),
    )(*args)


def scratch(*dims, dtype=jnp.bfloat16):
    return pltpu.VMEM(dims, dtype)


def run_stats(info, own, pair, keys):
    tok, wide = own.shape[1:]
    chips, heads = keys.shape[0], wide // HS
    seq = 2 * tok * chips
    rows = scratch(1, 2 * wide, dtype=jnp.float32)
    return call(
        functools.partial(stats_kernel, heads, seq),
        shape(2, 2, wide, dtype=jnp.float32),
        (info, own, pair, keys),
        2 * seq * wide * HS,
        smem=1,
        scratch=(rows, rows),
    )


def run_attend(info, own, pair, mine, other, keys, values):
    tok, wide = own.shape[1:]
    chips, heads = keys.shape[0], wide // HS
    seq = 2 * tok * chips
    return call(
        functools.partial(attend_kernel, heads, seq),
        (shape(2, wide, tok), shape(chips, tok, HS), shape(chips * tok, 2 * wide)),
        (info, own, pair, mine, other, keys, values),
        6 * seq * wide * HS,
        smem=1,
        in_any=(6,),
        out_any=(1, 2),
        scratch=(
            scratch(chips, tok, HS),
            scratch(HS, chips * tok),
            scratch(2 * wide, HS),
            scratch(chips, tok, HS),
            scratch(chips * tok, 2 * wide),
            scratch(1, 2 * wide, dtype=jnp.float32),
            pltpu.SemaphoreType.DMA,
            pltpu.SemaphoreType.DMA((chips,)),
            pltpu.SemaphoreType.DMA((chips,)),
        ),
    )


def run_grads(info, own, pair, mine, other, keys, values, probs):
    tok, wide = own.shape[1:]
    chips, heads = keys.shape[0], wide // HS
    seq = 2 * tok * chips
    return call(
        functools.partial(grads_kernel, heads, seq),
        (shape(chips, tok, HS), shape(2, tok, wide)),
        (info, own, pair, mine, other, keys, values, probs),
        6 * seq * wide * HS,
        smem=1,
        in_any=(5, 7),
        out_any=(0,),
        scratch=(
            scratch(chips, tok, HS),
            scratch(HS, chips * tok),
            scratch(2 * wide, HS),
            scratch(chips, tok, HS),
            scratch(chips * tok, 2 * wide),
            scratch(chips * tok, 2 * wide),
            scratch(1, 2 * wide, dtype=jnp.float32),
            pltpu.SemaphoreType.DMA,
            pltpu.SemaphoreType.DMA((chips,)),
            pltpu.SemaphoreType.DMA((chips,)),
        ),
    )


CORES = 2
X = 4


def swap_cores(value):
    count = lax.axis_size("blk")
    return lax.ppermute(value, "blk", [(i, i ^ 1) for i in range(count)])


def send_along_x(value, step):
    count = lax.axis_size("dp")
    return lax.ppermute(
        value, "dp", [(i, i // X * X + (i + step) % X) for i in range(count)]
    )


def exchange_chips(value):
    chips = lax.axis_size("blk") // CORES
    groups = [[core + CORES * chip for chip in range(chips)] for core in range(CORES)]
    return lax.all_to_all(value, "blk", 0, 0, tiled=True, axis_index_groups=groups)


def exchange_plane(value):
    blk, dp = lax.axis_size("blk"), lax.axis_size("dp")
    groups = [
        [(outer * X + x) * blk + chip * CORES + core for outer in range(dp // X) for chip in range(blk // CORES)]
        for x in range(X)
        for core in range(CORES)
    ]
    value = value.reshape(dp // X * (blk // CORES), -1, value.shape[1])
    return lax.all_to_all(value, ("dp", "blk"), 0, 0, tiled=True, axis_index_groups=groups)


def per_device(inputs, upstream, gain, w_query, w_key, w_value, w_out, prefix_len, bound):
    return whole(inputs[0], upstream[0], gain, w_query, w_key, w_value, w_out, prefix_len, bound)


def whole(inputs, grad_out, gain, w_query, w_key, w_value, w_out, prefix_len, bound):
    tok, wide = inputs.shape
    heads_wide = w_query.shape[1]
    my, dp = lax.axis_index("blk"), lax.axis_index("dp")
    count, share = lax.axis_size("blk"), lax.axis_size("dp")
    chips, outer = count // CORES, share // X
    size = wide // (count * share)
    core, x = my % CORES, dp % X
    info = jnp.stack([my, prefix_len[0], bound[0] * BLOCK, core, x]).astype(jnp.int32)
    gain_row = gain.reshape(1, wide)
    filed = shape(X, outer, chips, size, tok)
    copies = shape(chips, tok, HS)
    hidden, k_copies = call(
        functools.partial(prepare_kernel, chips),
        (shape(tok, wide), copies),
        (inputs, gain_row, w_key),
        4 * tok * wide * HS,
    )
    keys = exchange_chips(k_copies)
    own, v_copies, ht_own, ht_pair = call(
        project_kernel,
        (shape(2, tok, heads_wide), copies, filed, filed),
        (info, hidden, grad_out, w_query, w_out, w_value),
        4 * tok * wide * wide,
        smem=1,
    )
    values = exchange_chips(v_copies)
    pair = swap_cores(own)
    grad_pair = swap_cores(grad_out)
    ht_pair = swap_cores(ht_pair)
    mine = run_stats(info, own, pair, keys)
    other = swap_cores(mine)
    attn, dv, probs = run_attend(info, own, pair, mine, other, keys, values)
    attn_other = swap_cores(attn)
    dv_parts = exchange_chips(dv)
    dk, dq_mine = run_grads(info, own, pair, attn, attn_other, keys, values, probs)
    dq_other = swap_cores(dq_mine)
    dk_parts = exchange_chips(dk)
    rows = outer * chips * size
    d_query_rows, base, *parts = call(
        terms_kernel,
        (
            shape(tok, heads_wide),
            shape(rows, wide + heads_wide, dtype=jnp.float32),
            *[shape(rows, wide + heads_wide)] * (X - 1),
        ),
        (info, attn, attn_other, grad_out, grad_pair, ht_own, ht_pair, dq_mine, dq_other),
        8 * X * rows * wide * tok,
        smem=1,
        scratch=[scratch(*filed.shape)] * 2,
    )
    arrived = []
    for step, terms in enumerate(parts, 1):
        arrived.append(send_along_x(terms, step))
    d_value_rows = call(total_kernel, shape(tok, HS), (dv_parts,), 1 << 30)
    d_kv_rows = call(rows_kernel, shape(tok, 2 * HS), (dk_parts, d_value_rows), 1 << 30)
    d_kv_pair = swap_cores(d_kv_rows)
    kv_terms = call(
        kv_kernel,
        shape(rows, X * 2 * HS),
        (info, ht_own, ht_pair, d_kv_rows, d_kv_pair),
        1 << 30,
        smem=1,
    )
    kv_parts = exchange_plane(kv_terms)
    terms = call(collect_kernel, shape(rows, wide + heads_wide), (base, *arrived), 1 << 30)
    parts = exchange_plane(terms)
    kv_total = call(total_kernel, shape(size, X * 2 * HS), (kv_parts,), 1 << 30)
    total = wide + heads_wide + X * 2 * HS
    copies = call(spread_kernel, shape(share, size, total), (parts, kv_total), 1 << 30)
    shared = lax.all_to_all(copies, "dp", 0, 0, tiled=True)
    d_in = call(
        finish_kernel,
        shape(tok, wide),
        (inputs, grad_out, gain_row, d_query_rows, d_kv_rows, w_query, w_key, w_value),
        2 * tok * wide * (wide + 2 * HS),
    )
    held = wide // count
    f32 = functools.partial(shape, dtype=jnp.float32)
    d_query, d_key, d_value, d_out, d_gain = call(
        functools.partial(weights_kernel, X),
        (f32(held, heads_wide), f32(held, HS), f32(held, HS), f32(held, wide), f32(1, held)),
        (info, shared, gain.reshape(count, held), w_query, w_key, w_value),
        1 << 30,
        smem=1,
        in_any=(3, 4, 5),
        scratch=(
            scratch(held, heads_wide),
            scratch(held, HS),
            scratch(held, HS),
            pltpu.SemaphoreType.DMA((3,)),
        ),
    )
    return (d_in[None], d_query, d_key, d_value, d_out, d_gain.reshape(held))


def solution(mesh):
    placed = (P("dp", "blk", None), P("dp", "blk", None), P(), P(), P(), P(), P(), P("dp"), P("dp"))
    return jax.shard_map(
        per_device,
        mesh=mesh,
        in_specs=placed,
        out_specs=(
            P("dp", "blk", None),
            P("blk", None),
            P("blk", None),
            P("blk", None),
            P("blk", None),
            P("blk"),
        ),
        check_vma=False,
    )
```

```python
import functools

import jax
import jax.numpy as jnp
from jax import lax
from jax.experimental import pallas as pl
from jax.experimental.pallas import tpu as pltpu
from jax.sharding import PartitionSpec as P

HS = 256
ACT = 64
BLOCK = 128
NEG = -1e30
EPS = 1e-06
LOG2E = 1.4426950408889634
VMEM_BYTES = 67043328
NT = (((1,), (1,)), ((), ()))


def dot_nt(a, b):
    return lax.dot_general(a, b, NT, preferred_element_type=jnp.float32)


def dot_nn(a, b):
    return jnp.dot(a, b, preferred_element_type=jnp.float32)


def head(h):
    return pl.ds(h * HS, HS)


def part(half, h, heads):
    return pl.ds((half * heads + h) * HS, HS)


def block_state(info, chip, half, tok, seq):
    rows, plen, edge, core = info[0] ^ half, info[1], info[2], info[3]
    low = (chip * 2 + core) * tok
    high = low + tok
    first, last = rows * tok, rows * tok + tok - 1
    seen = ((low < plen) | (high > seq - ACT)) & ((low < edge) | (low <= last))
    full = (high <= plen) & ((high <= edge) | (high - 1 <= first))
    return seen, full


def mask_of(info, chip, half, tok, seq):
    rows, plen, edge, core = info[0] ^ half, info[1], info[2], info[3]
    k_pos = (chip * 2 + core) * tok + lax.broadcasted_iota(jnp.int32, (tok, tok), 0)
    q_pos = rows * tok + lax.broadcasted_iota(jnp.int32, (tok, tok), 1)
    key_ok = (k_pos < plen) | (k_pos >= seq - ACT)
    return key_ok & ((k_pos < edge) | (k_pos <= q_pos))


def when_seen(info, chip, half, tok, seq, work, rest):
    seen, full = block_state(info, chip, half, tok, seq)

    @pl.when(full)
    def _():
        work(None)

    @pl.when(seen & jnp.logical_not(full))
    def _():
        work(mask_of(info, chip, half, tok, seq))

    if rest is not None:
        pl.when(jnp.logical_not(seen))(rest)


def each_chip(chips, step):
    def body(chip, carry):
        step(chip)
        return carry

    lax.fori_loop(0, chips, body, 0)


def scaled_scores(keys, q, h, mask):
    s = dot_nt(keys, q[0, :, head(h)]) * (HS ** (-0.5) * LOG2E)
    return s if mask is None else jnp.where(mask, s, NEG)


def stats_kernel(heads, seq, info, own, pair, keys, out, top, total):
    chips, tok, _ = keys.shape
    top[...] = jnp.full(top.shape, NEG, jnp.float32)
    total[...] = jnp.zeros(total.shape, jnp.float32)

    def step(chip):
        for half, q in enumerate((own, pair)):

            def work(mask, half=half, q=q):
                for h in range(heads):
                    at = part(half, h, heads)
                    s = scaled_scores(keys[chip], q, h, mask)
                    old = top[:, at]
                    new = jnp.maximum(old, jnp.max(s, axis=0, keepdims=True))
                    top[:, at] = new
                    total[:, at] = total[:, at] * jnp.exp2(old - new) + jnp.sum(
                        jnp.exp2(s - new), axis=0, keepdims=True
                    )

            when_seen(info, chip, half, tok, seq, work, None)

    each_chip(chips, step)
    wide = heads * HS
    for half in range(2):
        out[half, 0:1, :] = top[:, pl.ds(half * wide, wide)]
        out[half, 1:2, :] = total[:, pl.ds(half * wide, wide)]


def attend_kernel(
    heads, seq, info, own, pair, mine, other, keys, values_in,
    attn, dv_out, probs_out,
    values, values_t, da_rows, dv, probs, lse, value_sem, dv_sems, out_sems,
):
    chips, tok, _ = keys.shape
    wide = heads * HS
    for half, qd in enumerate((own, pair)):
        for h in range(heads):
            da_rows[part(half, h, heads), :] = qd[1, :, head(h)]
        top_a, top_b = mine[half, 0:1, :], other[1 - half, 0:1, :]
        top = jnp.maximum(top_a, top_b)
        total = mine[half, 1:2, :] * jnp.exp2(top_a - top)
        total = total + other[1 - half, 1:2, :] * jnp.exp2(top_b - top)
        lse[:, pl.ds(half * wide, wide)] = top + jnp.log(total) * LOG2E
    value_copy = pltpu.make_async_copy(values_in, values, value_sem)
    value_copy.start()

    def dv_copy(chip):
        return pltpu.make_async_copy(dv.at[chip], dv_out.at[chip], dv_sems.at[chip])

    def rows_of(chip):
        return pl.ds(pl.multiple_of(chip * tok, tok), tok)

    def out_copy(chip):
        rows = rows_of(chip)
        return pltpu.make_async_copy(probs.at[rows, :], probs_out.at[rows, :], out_sems.at[chip])

    def step(chip):
        rows = rows_of(chip)
        for half, q in enumerate((own, pair)):

            def work(mask, half=half, q=q):
                for h in range(heads):
                    at = part(half, h, heads)
                    s = scaled_scores(keys[chip], q, h, mask)
                    probs[rows, at] = jnp.exp2(s - lse[:, at]).astype(jnp.bfloat16)

            def rest(half=half):
                probs[rows, pl.ds(half * wide, wide)] = jnp.zeros((tok, wide), jnp.bfloat16)

            when_seen(info, chip, half, tok, seq, work, rest)
        dv[chip] = dot_nn(probs[rows, :], da_rows[...]).astype(jnp.bfloat16)
        out_copy(chip).start()
        dv_copy(chip).start()

    each_chip(chips, step)
    value_copy.wait()
    for chip in range(chips):
        values_t[:, pl.ds(chip * tok, tok)] = values[chip].T
    for half in range(2):
        for h in range(heads):
            attn[half, head(h), :] = dot_nn(values_t[...], probs[:, part(half, h, heads)]).astype(
                jnp.bfloat16
            )
    each_chip(chips, lambda chip: dv_copy(chip).wait())
    each_chip(chips, lambda chip: out_copy(chip).wait())


def put_rows(info, rows, chip, own, pair):
    core, x = info[3], info[4]
    steps, outer, _, size, _ = own.shape

    def put(same):
        for n in range(rows.shape[0] // size):
            place = n % (outer * steps)
            to = own if (n // (outer * steps)) == same else pair
            if to is None:
                continue
            step = (place % steps - x + steps) & (steps - 1)
            to[step, place // steps, chip] = rows[n * size : (n + 1) * size].astype(to.dtype)

    for same in range(2):
        pl.when(core == same)(functools.partial(put, same))


def grads_kernel(
    heads, seq, info, own, pair, mine, other, keys_in, values, probs_in,
    dk_out, dq,
    keys, keys_t, q_rows, dk, probs, dscores, delta, key_sem, dk_sems, in_sems,
):
    chips, tok, _ = values.shape
    key_copy = pltpu.make_async_copy(keys_in, keys, key_sem)
    key_copy.start()

    def dk_copy(chip):
        return pltpu.make_async_copy(dk.at[chip], dk_out.at[chip], dk_sems.at[chip])

    def rows_of(chip):
        return pl.ds(pl.multiple_of(chip * tok, tok), tok)

    def in_copy(chip):
        rows = rows_of(chip)
        return pltpu.make_async_copy(probs_in.at[rows, :], probs.at[rows, :], in_sems.at[chip])

    each_chip(chips, lambda chip: in_copy(chip).start())
    for half, qd in enumerate((own, pair)):
        for h in range(heads):
            at = part(half, h, heads)
            q_rows[at, :] = qd[0, :, head(h)]
            both = mine[half, head(h), :].astype(jnp.float32) + other[1 - half, head(h), :].astype(
                jnp.float32
            )
            a = both.astype(jnp.bfloat16).astype(jnp.float32)
            delta[:, at] = jnp.sum(
                a * qd[1, :, head(h)].T.astype(jnp.float32), axis=0, keepdims=True
            )

    def step(chip):
        rows = rows_of(chip)
        in_copy(chip).wait()
        for half, qd in enumerate((own, pair)):
            seen, _ = block_state(info, chip, half, tok, seq)

            @pl.when(seen)
            def _(half=half, qd=qd):
                for h in range(heads):
                    at = part(half, h, heads)
                    dp = dot_nt(values[chip], qd[1, :, head(h)])
                    p = probs[rows, at].astype(jnp.float32)
                    dscores[rows, at] = (p * (dp - delta[:, at])).astype(jnp.bfloat16)

            @pl.when(jnp.logical_not(seen))
            def _(half=half):
                wide = heads * HS
                dscores[rows, pl.ds(half * wide, wide)] = jnp.zeros((tok, wide), jnp.bfloat16)

        dk[chip] = (dot_nn(dscores[rows, :], q_rows[...]) * HS ** (-0.5)).astype(jnp.bfloat16)
        dk_copy(chip).start()

    each_chip(chips, step)
    key_copy.wait()
    for chip in range(chips):
        keys_t[:, pl.ds(chip * tok, tok)] = keys[chip].T
    for half in range(2):
        for h in range(heads):
            d = dot_nn(keys_t[...], dscores[:, part(half, h, heads)]) * HS ** (-0.5)
            dq[half, :, head(h)] = d.T.astype(jnp.bfloat16)
    each_chip(chips, lambda chip: dk_copy(chip).wait())


def prepare_kernel(chips, x, gain, w_key, hidden, k_copies):
    xf = x[...].astype(jnp.float32)
    inv = lax.rsqrt(jnp.mean(xf * xf, axis=-1, keepdims=True) + EPS)
    h = (xf * inv * gain[...]).astype(jnp.bfloat16)
    hidden[...] = h
    rows = dot_nn(h, w_key[...]).astype(jnp.bfloat16)
    for chip in range(chips):
        k_copies[chip] = rows


def project_kernel(info, hidden, grad_out, w_query, w_out, w_value, both, v_copies, ht_own, ht_pair):
    h = hidden[...]
    values = dot_nn(h, w_value[...]).astype(jnp.bfloat16)
    for chip in range(v_copies.shape[0]):
        v_copies[chip] = values
    both[0] = dot_nn(h, w_query[...]).astype(jnp.bfloat16)
    both[1] = dot_nt(grad_out[...], w_out[...]).astype(jnp.bfloat16)
    chips = ht_own.shape[2]
    block = h.shape[1] // chips
    for chip in range(chips):
        rows = h[:, chip * block : (chip + 1) * block].astype(jnp.float32).T
        put_rows(info, rows, chip, ht_own, ht_pair)


def step_terms(lefts, rights, step):
    total = 0.0
    for left, right in zip(lefts, rights):
        rows = left.shape[1] * left.shape[2] * left.shape[3]
        total = total + dot_nn(left[step].reshape(rows, -1), right)
    return total


def direct_terms(info, lefts, rights, out, at):
    wide, steps = rights[0].shape[1], lefts[0].shape[0]
    for step in range(steps):
        place = (info[4] + step) & (steps - 1)
        to = pl.ds(pl.multiple_of(at + place * wide, 128), wide)
        out[:, to] = step_terms(lefts, rights, step).astype(out.dtype)


def terms_kernel(
    info, attn, attn_other, go_own, go_pair, ht_own, ht_pair, dq_mine, dq_other, dq, *refs
):
    outs, filed = refs[:-2], refs[-2:]
    block = attn.shape[1] // ht_own.shape[2]
    for half in range(2):
        for chip in range(ht_own.shape[2]):
            rows = pl.ds(chip * block, block)
            both = attn[half, rows, :].astype(jnp.float32) + attn_other[1 - half, rows, :].astype(
                jnp.float32
            )
            put_rows(info, both, chip, filed[half], None)
    rights = [
        (dq_mine[half].astype(jnp.float32) + dq_other[1 - half].astype(jnp.float32)).astype(dq.dtype)
        for half in range(2)
    ]
    dq[...] = rights[0]
    for step, out in enumerate(outs):
        g_out = step_terms(filed, (go_own[...], go_pair[...]), step)
        out[:, pl.ds(0, g_out.shape[1])] = g_out.astype(out.dtype)
        g_query = step_terms((ht_own, ht_pair), rights, step)
        out[:, pl.ds(g_out.shape[1], g_query.shape[1])] = g_query.astype(out.dtype)


def rows_kernel(dk_parts, dv_rows, out):
    out[:, pl.ds(0, HS)] = added_parts(dk_parts)
    out[:, pl.ds(HS, HS)] = dv_rows[...]


def kv_kernel(info, ht_own, ht_pair, dkv, dkv_pair, out):
    direct_terms(info, (ht_own, ht_pair), (dkv[...], dkv_pair[...]), out, 0)


def collect_kernel(base, one, two, three, out):
    total = base[...]
    for arrived in (one, two, three):
        total = total + arrived[...].astype(jnp.float32)
    out[...] = total.astype(out.dtype)


def added_parts(parts):
    total = parts[0].astype(jnp.float32)
    for n in range(1, parts.shape[0]):
        total = total + parts[n].astype(jnp.float32)
    return total.astype(jnp.bfloat16)


def total_kernel(parts, out):
    out[...] = added_parts(parts)


def split_kernel(info, parts, *outs):
    steps = len(outs)
    for step, out in enumerate(outs):
        wide = out.shape[1]
        place = (info[4] + step) & (steps - 1)
        at = pl.ds(pl.multiple_of(place * wide, 128), wide)
        total = parts[0, :, at].astype(jnp.float32)
        for n in range(1, parts.shape[0]):
            total = total + parts[n, :, at].astype(jnp.float32)
        out[...] = total.astype(out.dtype)


def spread_kernel(parts, kv, out):
    total = added_parts(parts)
    wide = total.shape[1]
    for n in range(out.shape[0]):
        out[n, :, pl.ds(0, wide)] = total
        out[n, :, pl.ds(wide, kv.shape[1])] = kv[...]


def weights_kernel(
    info, shared, gain, wq_in, wk_in, wv_in,
    d_query, d_key, d_value, d_out, d_gain,
    w_query, w_key, w_value, sems,
):
    size = shared.shape[1]
    held = d_out.shape[0]
    mine = pl.ds(pl.multiple_of(info[0] * held, held), held)
    copies = [
        pltpu.make_async_copy(w.at[mine, :], into, sems.at[n])
        for n, (w, into) in enumerate(((wq_in, w_query), (wk_in, w_key), (wv_in, w_value)))
    ]
    for c in copies:
        c.start()
    for c in copies:
        c.wait()
    wide, heads_wide = d_out.shape[1], d_query.shape[1]
    gains = []
    for place in range(shared.shape[0]):
        rows = slice(place * size, (place + 1) * size)
        d_out[rows, :] = shared[place, :, pl.ds(0, wide)].astype(jnp.float32)
        query = shared[place, :, pl.ds(wide, heads_wide)].astype(jnp.float32)
        kv = shared[place, :, pl.ds(wide + heads_wide, 2 * HS)].astype(jnp.float32)
        d_query[rows, :] = query
        d_key[rows, :] = kv[:, :HS]
        d_value[rows, :] = kv[:, HS:]
        row_sum = (
            jnp.sum(w_query[rows, :].astype(jnp.float32) * query, axis=1, keepdims=True)
            + jnp.sum(w_key[rows, :].astype(jnp.float32) * kv[:, :HS], axis=1, keepdims=True)
            + jnp.sum(w_value[rows, :].astype(jnp.float32) * kv[:, HS:], axis=1, keepdims=True)
        )
        gains.append(jnp.broadcast_to(row_sum, (size, 128)))
    d_gain[...] = jnp.concatenate(gains, axis=0).T[0:1, :] / gain[pl.ds(info[0], 1), :]


def finish_kernel(x, grad_out, gain, dq, dkv, w_query, w_key, w_value, d_in):
    dhidden = (
        dot_nt(dq[...], w_query[...])
        + dot_nt(dkv[:, :HS], w_key[...])
        + dot_nt(dkv[:, HS:], w_value[...])
    )
    xf = x[...].astype(jnp.float32)
    inv = lax.rsqrt(jnp.mean(xf * xf, axis=-1, keepdims=True) + EPS)
    normed = xf * inv
    scaled = dhidden * gain[...]
    mean = jnp.mean(scaled * normed, axis=-1, keepdims=True)
    d_in[...] = (grad_out[...].astype(jnp.float32) + inv * (scaled - normed * mean)).astype(d_in.dtype)


SMEM = pl.BlockSpec(memory_space=pltpu.SMEM)
VMEM = pl.BlockSpec(memory_space=pltpu.VMEM)
ANY = pl.BlockSpec(memory_space=pl.ANY)


def shape(*dims, dtype=jnp.bfloat16):
    return jax.ShapeDtypeStruct(dims, dtype)


def call(body, outs, args, flops, smem=0, scratch=(), in_any=(), out_any=()):
    specs = [SMEM if n < smem else ANY if n in in_any else VMEM for n in range(len(args))]
    if isinstance(outs, tuple):
        out_specs = tuple(ANY if n in out_any else VMEM for n in range(len(outs)))
    else:
        out_specs = VMEM
    return pl.pallas_call(
        body,
        out_shape=outs,
        in_specs=specs,
        out_specs=out_specs,
        scratch_shapes=list(scratch),
        compiler_params=pltpu.CompilerParams(vmem_limit_bytes=VMEM_BYTES),
        cost_estimate=pl.CostEstimate(flops=flops, bytes_accessed=1 << 20, transcendentals=0),
    )(*args)


def scratch(*dims, dtype=jnp.bfloat16):
    return pltpu.VMEM(dims, dtype)


def run_stats(info, own, pair, keys):
    tok, wide = own.shape[1:]
    chips, heads = keys.shape[0], wide // HS
    seq = 2 * tok * chips
    rows = scratch(1, 2 * wide, dtype=jnp.float32)
    return call(
        functools.partial(stats_kernel, heads, seq),
        shape(2, 2, wide, dtype=jnp.float32),
        (info, own, pair, keys),
        2 * seq * wide * HS,
        smem=1,
        scratch=(rows, rows),
    )


def run_attend(info, own, pair, mine, other, keys, values):
    tok, wide = own.shape[1:]
    chips, heads = keys.shape[0], wide // HS
    seq = 2 * tok * chips
    return call(
        functools.partial(attend_kernel, heads, seq),
        (shape(2, wide, tok), shape(chips, tok, HS), shape(chips * tok, 2 * wide)),
        (info, own, pair, mine, other, keys, values),
        6 * seq * wide * HS,
        smem=1,
        in_any=(6,),
        out_any=(1, 2),
        scratch=(
            scratch(chips, tok, HS),
            scratch(HS, chips * tok),
            scratch(2 * wide, HS),
            scratch(chips, tok, HS),
            scratch(chips * tok, 2 * wide),
            scratch(1, 2 * wide, dtype=jnp.float32),
            pltpu.SemaphoreType.DMA,
            pltpu.SemaphoreType.DMA((chips,)),
            pltpu.SemaphoreType.DMA((chips,)),
        ),
    )


def run_grads(info, own, pair, mine, other, keys, values, probs):
    tok, wide = own.shape[1:]
    chips, heads = keys.shape[0], wide // HS
    seq = 2 * tok * chips
    return call(
        functools.partial(grads_kernel, heads, seq),
        (shape(chips, tok, HS), shape(2, tok, wide)),
        (info, own, pair, mine, other, keys, values, probs),
        6 * seq * wide * HS,
        smem=1,
        in_any=(5, 7),
        out_any=(0,),
        scratch=(
            scratch(chips, tok, HS),
            scratch(HS, chips * tok),
            scratch(2 * wide, HS),
            scratch(chips, tok, HS),
            scratch(chips * tok, 2 * wide),
            scratch(chips * tok, 2 * wide),
            scratch(1, 2 * wide, dtype=jnp.float32),
            pltpu.SemaphoreType.DMA,
            pltpu.SemaphoreType.DMA((chips,)),
            pltpu.SemaphoreType.DMA((chips,)),
        ),
    )


CORES = 2
X = 4


def swap_cores(value):
    count = lax.axis_size("blk")
    return lax.ppermute(value, "blk", [(i, i ^ 1) for i in range(count)])


def send_along_x(value, step):
    count = lax.axis_size("dp")
    return lax.ppermute(
        value, "dp", [(i, i // X * X + (i + step) % X) for i in range(count)]
    )


def exchange_chips(value):
    chips = lax.axis_size("blk") // CORES
    groups = [[core + CORES * chip for chip in range(chips)] for core in range(CORES)]
    return lax.all_to_all(value, "blk", 0, 0, tiled=True, axis_index_groups=groups)


def exchange_plane(value):
    blk, dp = lax.axis_size("blk"), lax.axis_size("dp")
    groups = [
        [(outer * X + x) * blk + chip * CORES + core for outer in range(dp // X) for chip in range(blk // CORES)]
        for x in range(X)
        for core in range(CORES)
    ]
    value = value.reshape(dp // X * (blk // CORES), -1, value.shape[1])
    return lax.all_to_all(value, ("dp", "blk"), 0, 0, tiled=True, axis_index_groups=groups)


def per_device(inputs, upstream, gain, w_query, w_key, w_value, w_out, prefix_len, bound):
    return whole(inputs[0], upstream[0], gain, w_query, w_key, w_value, w_out, prefix_len, bound)


def whole(inputs, grad_out, gain, w_query, w_key, w_value, w_out, prefix_len, bound):
    tok, wide = inputs.shape
    heads_wide = w_query.shape[1]
    my, dp = lax.axis_index("blk"), lax.axis_index("dp")
    count, share = lax.axis_size("blk"), lax.axis_size("dp")
    chips, outer = count // CORES, share // X
    size = wide // (count * share)
    core, x = my % CORES, dp % X
    info = jnp.stack([my, prefix_len[0], bound[0] * BLOCK, core, x]).astype(jnp.int32)
    gain_row = gain.reshape(1, wide)
    filed = shape(X, outer, chips, size, tok)
    copies = shape(chips, tok, HS)
    hidden, k_copies = call(
        functools.partial(prepare_kernel, chips),
        (shape(tok, wide), copies),
        (inputs, gain_row, w_key),
        4 * tok * wide * HS,
    )
    keys = exchange_chips(k_copies)
    own, v_copies, ht_own, ht_pair = call(
        project_kernel,
        (shape(2, tok, heads_wide), copies, filed, filed),
        (info, hidden, grad_out, w_query, w_out, w_value),
        4 * tok * wide * wide,
        smem=1,
    )
    values = exchange_chips(v_copies)
    pair = swap_cores(own)
    grad_pair = swap_cores(grad_out)
    ht_pair = swap_cores(ht_pair)
    mine = run_stats(info, own, pair, keys)
    other = swap_cores(mine)
    attn, dv, probs = run_attend(info, own, pair, mine, other, keys, values)
    attn_other = swap_cores(attn)
    dv_parts = exchange_chips(dv)
    dk, dq_mine = run_grads(info, own, pair, attn, attn_other, keys, values, probs)
    dq_other = swap_cores(dq_mine)
    dk_parts = exchange_chips(dk)
    rows = outer * chips * size
    d_query_rows, base, *parts = call(
        terms_kernel,
        (
            shape(tok, heads_wide),
            shape(rows, wide + heads_wide, dtype=jnp.float32),
            *[shape(rows, wide + heads_wide)] * (X - 1),
        ),
        (info, attn, attn_other, grad_out, grad_pair, ht_own, ht_pair, dq_mine, dq_other),
        8 * X * rows * wide * tok,
        smem=1,
        scratch=[scratch(*filed.shape)] * 2,
    )
    arrived = []
    for step, terms in enumerate(parts, 1):
        arrived.append(send_along_x(terms, step))
    d_value_rows = call(total_kernel, shape(tok, HS), (dv_parts,), 1 << 30)
    d_kv_rows = call(rows_kernel, shape(tok, 2 * HS), (dk_parts, d_value_rows), 1 << 30)
    d_kv_pair = swap_cores(d_kv_rows)
    kv_terms = call(
        kv_kernel,
        shape(rows, X * 2 * HS),
        (info, ht_own, ht_pair, d_kv_rows, d_kv_pair),
        1 << 30,
        smem=1,
    )
    kv_parts = exchange_plane(kv_terms)
    terms = call(collect_kernel, shape(rows, wide + heads_wide), (base, *arrived), 1 << 30)
    parts = exchange_plane(terms)
    kv_base, *kv_pieces = call(
        split_kernel,
        (shape(size, 2 * HS, dtype=jnp.float32), *[shape(size, 2 * HS)] * (X - 1)),
        (info, kv_parts),
        1 << 30,
        smem=1,
    )
    kv_arrived = []
    for step, piece in enumerate(kv_pieces, 1):
        kv_arrived.append(send_along_x(piece, step))
    kv_total = call(collect_kernel, shape(size, 2 * HS), (kv_base, *kv_arrived), 1 << 20)
    total = wide + heads_wide + 2 * HS
    copies = call(spread_kernel, shape(share, size, total), (parts, kv_total), 1 << 30)
    shared = lax.all_to_all(copies, "dp", 0, 0, tiled=True)
    d_in = call(
        finish_kernel,
        shape(tok, wide),
        (inputs, grad_out, gain_row, d_query_rows, d_kv_rows, w_query, w_key, w_value),
        2 * tok * wide * (wide + 2 * HS),
    )
    held = wide // count
    f32 = functools.partial(shape, dtype=jnp.float32)
    d_query, d_key, d_value, d_out, d_gain = call(
        weights_kernel,
        (f32(held, heads_wide), f32(held, HS), f32(held, HS), f32(held, wide), f32(1, held)),
        (info, shared, gain.reshape(count, held), w_query, w_key, w_value),
        1 << 30,
        smem=1,
        in_any=(3, 4, 5),
        scratch=(
            scratch(held, heads_wide),
            scratch(held, HS),
            scratch(held, HS),
            pltpu.SemaphoreType.DMA((3,)),
        ),
    )
    return (d_in[None], d_query, d_key, d_value, d_out, d_gain.reshape(held))


def solution(mesh):
    placed = (P("dp", "blk", None), P("dp", "blk", None), P(), P(), P(), P(), P(), P("dp"), P("dp"))
    return jax.shard_map(
        per_device,
        mesh=mesh,
        in_specs=placed,
        out_specs=(
            P("dp", "blk", None),
            P("blk", None),
            P("blk", None),
            P("blk", None),
            P("blk", None),
            P("blk"),
        ),
        check_vma=False,
    )
```

```python
import functools

import jax
import jax.numpy as jnp
from jax import lax
from jax.experimental import pallas as pl
from jax.experimental.pallas import tpu as pltpu
from jax.sharding import PartitionSpec as P

HS = 256
ACT = 64
BLOCK = 128
NEG = -1e30
EPS = 1e-06
LOG2E = 1.4426950408889634
VMEM_BYTES = 67043328
NT = (((1,), (1,)), ((), ()))


def dot_nt(a, b):
    return lax.dot_general(a, b, NT, preferred_element_type=jnp.float32)


def dot_nn(a, b):
    return jnp.dot(a, b, preferred_element_type=jnp.float32)


def head(h):
    return pl.ds(h * HS, HS)


def part(half, h, heads):
    return pl.ds((half * heads + h) * HS, HS)


def block_state(info, chip, half, tok, seq):
    rows, plen, edge, core = info[0] ^ half, info[1], info[2], info[3]
    low = (chip * 2 + core) * tok
    high = low + tok
    first, last = rows * tok, rows * tok + tok - 1
    seen = ((low < plen) | (high > seq - ACT)) & ((low < edge) | (low <= last))
    full = (high <= plen) & ((high <= edge) | (high - 1 <= first))
    return seen, full


def mask_of(info, chip, half, tok, seq):
    rows, plen, edge, core = info[0] ^ half, info[1], info[2], info[3]
    k_pos = (chip * 2 + core) * tok + lax.broadcasted_iota(jnp.int32, (tok, tok), 0)
    q_pos = rows * tok + lax.broadcasted_iota(jnp.int32, (tok, tok), 1)
    key_ok = (k_pos < plen) | (k_pos >= seq - ACT)
    return key_ok & ((k_pos < edge) | (k_pos <= q_pos))


def when_seen(info, chip, half, tok, seq, work, rest):
    seen, full = block_state(info, chip, half, tok, seq)

    @pl.when(full)
    def _():
        work(None)

    @pl.when(seen & jnp.logical_not(full))
    def _():
        work(mask_of(info, chip, half, tok, seq))

    if rest is not None:
        pl.when(jnp.logical_not(seen))(rest)


def each_chip(chips, step):
    def body(chip, carry):
        step(chip)
        return carry

    lax.fori_loop(0, chips, body, 0)


def scaled_scores(keys, q, h, mask):
    s = dot_nt(keys, q[0, :, head(h)]) * (HS ** (-0.5) * LOG2E)
    return s if mask is None else jnp.where(mask, s, NEG)


def stats_kernel(heads, seq, info, own, pair, keys, out, top, total):
    chips, tok, _ = keys.shape
    top[...] = jnp.full(top.shape, NEG, jnp.float32)
    total[...] = jnp.zeros(total.shape, jnp.float32)

    def step(chip):
        for half, q in enumerate((own, pair)):

            def work(mask, half=half, q=q):
                for h in range(heads):
                    at = part(half, h, heads)
                    s = scaled_scores(keys[chip], q, h, mask)
                    old = top[:, at]
                    new = jnp.maximum(old, jnp.max(s, axis=0, keepdims=True))
                    top[:, at] = new
                    total[:, at] = total[:, at] * jnp.exp2(old - new) + jnp.sum(
                        jnp.exp2(s - new), axis=0, keepdims=True
                    )

            when_seen(info, chip, half, tok, seq, work, None)

    each_chip(chips, step)
    wide = heads * HS
    for half in range(2):
        out[half, 0:1, :] = top[:, pl.ds(half * wide, wide)]
        out[half, 1:2, :] = total[:, pl.ds(half * wide, wide)]


def attend_kernel(
    heads, seq, info, own, pair, mine, other, keys, values_in,
    attn, dv_out, probs_out,
    values, values_t, da_rows, dv, probs, lse, value_sem, dv_sems, out_sems,
):
    chips, tok, _ = keys.shape
    wide = heads * HS
    for half, qd in enumerate((own, pair)):
        for h in range(heads):
            da_rows[part(half, h, heads), :] = qd[1, :, head(h)]
        top_a, top_b = mine[half, 0:1, :], other[1 - half, 0:1, :]
        top = jnp.maximum(top_a, top_b)
        total = mine[half, 1:2, :] * jnp.exp2(top_a - top)
        total = total + other[1 - half, 1:2, :] * jnp.exp2(top_b - top)
        lse[:, pl.ds(half * wide, wide)] = top + jnp.log(total) * LOG2E
    value_copy = pltpu.make_async_copy(values_in, values, value_sem)
    value_copy.start()

    def dv_copy(chip):
        return pltpu.make_async_copy(dv.at[chip], dv_out.at[chip], dv_sems.at[chip])

    def rows_of(chip):
        return pl.ds(pl.multiple_of(chip * tok, tok), tok)

    def out_copy(chip):
        rows = rows_of(chip)
        return pltpu.make_async_copy(probs.at[rows, :], probs_out.at[rows, :], out_sems.at[chip])

    def step(chip):
        rows = rows_of(chip)
        for half, q in enumerate((own, pair)):

            def work(mask, half=half, q=q):
                for h in range(heads):
                    at = part(half, h, heads)
                    s = scaled_scores(keys[chip], q, h, mask)
                    probs[rows, at] = jnp.exp2(s - lse[:, at]).astype(jnp.bfloat16)

            def rest(half=half):
                probs[rows, pl.ds(half * wide, wide)] = jnp.zeros((tok, wide), jnp.bfloat16)

            when_seen(info, chip, half, tok, seq, work, rest)
        dv[chip] = dot_nn(probs[rows, :], da_rows[...]).astype(jnp.bfloat16)
        out_copy(chip).start()
        dv_copy(chip).start()

    each_chip(chips, step)
    value_copy.wait()
    for chip in range(chips):
        values_t[:, pl.ds(chip * tok, tok)] = values[chip].T
    for half in range(2):
        for h in range(heads):
            attn[half, head(h), :] = dot_nn(values_t[...], probs[:, part(half, h, heads)]).astype(
                jnp.bfloat16
            )
    each_chip(chips, lambda chip: dv_copy(chip).wait())
    each_chip(chips, lambda chip: out_copy(chip).wait())


def put_rows(info, rows, chip, own, pair):
    core, x = info[3], info[4]
    steps, outer, _, size, _ = own.shape

    def put(same):
        for n in range(rows.shape[0] // size):
            place = n % (outer * steps)
            to = own if (n // (outer * steps)) == same else pair
            if to is None:
                continue
            step = (place % steps - x + steps) & (steps - 1)
            to[step, place // steps, chip] = rows[n * size : (n + 1) * size].astype(to.dtype)

    for same in range(2):
        pl.when(core == same)(functools.partial(put, same))


def grads_kernel(
    heads, seq, info, own, pair, mine, other, keys_in, values, probs_in,
    dk_out, dq,
    keys, keys_t, q_rows, dk, probs, dscores, delta, key_sem, dk_sems, in_sems,
):
    chips, tok, _ = values.shape
    key_copy = pltpu.make_async_copy(keys_in, keys, key_sem)
    key_copy.start()

    def dk_copy(chip):
        return pltpu.make_async_copy(dk.at[chip], dk_out.at[chip], dk_sems.at[chip])

    def rows_of(chip):
        return pl.ds(pl.multiple_of(chip * tok, tok), tok)

    def in_copy(chip):
        rows = rows_of(chip)
        return pltpu.make_async_copy(probs_in.at[rows, :], probs.at[rows, :], in_sems.at[chip])

    each_chip(chips, lambda chip: in_copy(chip).start())
    for half, qd in enumerate((own, pair)):
        for h in range(heads):
            at = part(half, h, heads)
            q_rows[at, :] = qd[0, :, head(h)]
            both = mine[half, head(h), :].astype(jnp.float32) + other[1 - half, head(h), :].astype(
                jnp.float32
            )
            a = both.astype(jnp.bfloat16).astype(jnp.float32)
            delta[:, at] = jnp.sum(
                a * qd[1, :, head(h)].T.astype(jnp.float32), axis=0, keepdims=True
            )

    def step(chip):
        rows = rows_of(chip)
        in_copy(chip).wait()
        for half, qd in enumerate((own, pair)):
            seen, _ = block_state(info, chip, half, tok, seq)

            @pl.when(seen)
            def _(half=half, qd=qd):
                for h in range(heads):
                    at = part(half, h, heads)
                    dp = dot_nt(values[chip], qd[1, :, head(h)])
                    p = probs[rows, at].astype(jnp.float32)
                    dscores[rows, at] = (p * (dp - delta[:, at])).astype(jnp.bfloat16)

            @pl.when(jnp.logical_not(seen))
            def _(half=half):
                wide = heads * HS
                dscores[rows, pl.ds(half * wide, wide)] = jnp.zeros((tok, wide), jnp.bfloat16)

        dk[chip] = (dot_nn(dscores[rows, :], q_rows[...]) * HS ** (-0.5)).astype(jnp.bfloat16)
        dk_copy(chip).start()

    each_chip(chips, step)
    key_copy.wait()
    for chip in range(chips):
        keys_t[:, pl.ds(chip * tok, tok)] = keys[chip].T
    for half in range(2):
        for h in range(heads):
            d = dot_nn(keys_t[...], dscores[:, part(half, h, heads)]) * HS ** (-0.5)
            dq[half, :, head(h)] = d.T.astype(jnp.bfloat16)
    each_chip(chips, lambda chip: dk_copy(chip).wait())


def prepare_kernel(chips, x, gain, w_key, hidden, k_copies):
    xf = x[...].astype(jnp.float32)
    inv = lax.rsqrt(jnp.mean(xf * xf, axis=-1, keepdims=True) + EPS)
    h = (xf * inv * gain[...]).astype(jnp.bfloat16)
    hidden[...] = h
    rows = dot_nn(h, w_key[...]).astype(jnp.bfloat16)
    for chip in range(chips):
        k_copies[chip] = rows


def project_kernel(info, hidden, grad_out, w_query, w_out, w_value, both, v_copies, ht_own, ht_pair):
    h = hidden[...]
    values = dot_nn(h, w_value[...]).astype(jnp.bfloat16)
    for chip in range(v_copies.shape[0]):
        v_copies[chip] = values
    both[0] = dot_nn(h, w_query[...]).astype(jnp.bfloat16)
    both[1] = dot_nt(grad_out[...], w_out[...]).astype(jnp.bfloat16)
    chips = ht_own.shape[2]
    block = h.shape[1] // chips
    for chip in range(chips):
        rows = h[:, chip * block : (chip + 1) * block].astype(jnp.float32).T
        put_rows(info, rows, chip, ht_own, ht_pair)


def step_terms(lefts, rights, step):
    total = 0.0
    for left, right in zip(lefts, rights):
        rows = left.shape[1] * left.shape[2] * left.shape[3]
        total = total + dot_nn(left[step].reshape(rows, -1), right)
    return total


def direct_terms(info, lefts, rights, out, at):
    wide, steps = rights[0].shape[1], lefts[0].shape[0]
    for step in range(steps):
        place = (info[4] + step) & (steps - 1)
        to = pl.ds(pl.multiple_of(at + place * wide, 128), wide)
        out[:, to] = step_terms(lefts, rights, step).astype(out.dtype)


def terms_kernel(
    info, attn, attn_other, go_own, go_pair, ht_own, ht_pair, dq_mine, dq_other, dq, *refs
):
    outs, filed = refs[:-2], refs[-2:]
    block = attn.shape[1] // ht_own.shape[2]
    for half in range(2):
        for chip in range(ht_own.shape[2]):
            rows = pl.ds(chip * block, block)
            both = attn[half, rows, :].astype(jnp.float32) + attn_other[1 - half, rows, :].astype(
                jnp.float32
            )
            put_rows(info, both, chip, filed[half], None)
    rights = [
        (dq_mine[half].astype(jnp.float32) + dq_other[1 - half].astype(jnp.float32)).astype(dq.dtype)
        for half in range(2)
    ]
    dq[...] = rights[0]
    for step, out in enumerate(outs):
        g_out = step_terms(filed, (go_own[...], go_pair[...]), step)
        out[:, pl.ds(0, g_out.shape[1])] = g_out.astype(out.dtype)
        g_query = step_terms((ht_own, ht_pair), rights, step)
        out[:, pl.ds(g_out.shape[1], g_query.shape[1])] = g_query.astype(out.dtype)


def rows_kernel(dk_parts, dv_rows, out):
    out[:, pl.ds(0, HS)] = added_parts(dk_parts)
    out[:, pl.ds(HS, HS)] = dv_rows[...]


def kv_kernel(info, ht_own, ht_pair, dkv, dkv_pair, out):
    direct_terms(info, (ht_own, ht_pair), (dkv[...], dkv_pair[...]), out, 0)


def collect_kernel(base, one, two, three, out):
    total = base[...]
    for arrived in (one, two, three):
        total = total + arrived[...].astype(jnp.float32)
    out[...] = total.astype(out.dtype)


def added_parts(parts):
    total = parts[0].astype(jnp.float32)
    for n in range(1, parts.shape[0]):
        total = total + parts[n].astype(jnp.float32)
    return total.astype(jnp.bfloat16)


def total_kernel(parts, out):
    out[...] = added_parts(parts)


def split_kernel(info, parts, *outs):
    steps = len(outs)
    for step, out in enumerate(outs):
        wide = out.shape[1]
        place = (info[4] + step) & (steps - 1)
        at = pl.ds(pl.multiple_of(place * wide, 128), wide)
        total = parts[0, :, at].astype(jnp.float32)
        for n in range(1, parts.shape[0]):
            total = total + parts[n, :, at].astype(jnp.float32)
        out[...] = total.astype(out.dtype)


def spread_kernel(parts, kv, out):
    total = added_parts(parts)
    wide = total.shape[1]
    for n in range(out.shape[0]):
        out[n, :, pl.ds(0, wide)] = total
        out[n, :, pl.ds(wide, kv.shape[1])] = kv[...]


def weights_kernel(
    info, shared, gain, wq_in, wk_in, wv_in,
    d_query, d_key, d_value, d_out, d_gain,
    w_query, w_key, w_value, sems,
):
    size = shared.shape[1]
    held = d_out.shape[0]
    mine = pl.ds(pl.multiple_of(info[0] * held, held), held)
    copies = [
        pltpu.make_async_copy(w.at[mine, :], into, sems.at[n])
        for n, (w, into) in enumerate(((wq_in, w_query), (wk_in, w_key), (wv_in, w_value)))
    ]
    for c in copies:
        c.start()
    wide, heads_wide = d_out.shape[1], d_query.shape[1]
    gains = []
    for place in range(shared.shape[0]):
        rows = slice(place * size, (place + 1) * size)
        d_out[rows, :] = shared[place, :, pl.ds(0, wide)].astype(jnp.float32)
        query = shared[place, :, pl.ds(wide, heads_wide)].astype(jnp.float32)
        kv = shared[place, :, pl.ds(wide + heads_wide, 2 * HS)].astype(jnp.float32)
        d_query[rows, :] = query
        d_key[rows, :] = kv[:, :HS]
        d_value[rows, :] = kv[:, HS:]
    for c in copies:
        c.wait()
    for place in range(shared.shape[0]):
        rows = slice(place * size, (place + 1) * size)
        row_sum = 0.0
        for weight, grad in ((w_query, d_query), (w_key, d_key), (w_value, d_value)):
            terms = weight[rows, :].astype(jnp.float32) * grad[rows, :]
            row_sum = row_sum + jnp.sum(terms, axis=1, keepdims=True)
        gains.append(jnp.broadcast_to(row_sum, (size, 128)))
    d_gain[...] = jnp.concatenate(gains, axis=0).T[0:1, :] / gain[pl.ds(info[0], 1), :]


def finish_kernel(x, grad_out, gain, dq, dkv, w_query, w_key, w_value, d_in):
    dhidden = (
        dot_nt(dq[...], w_query[...])
        + dot_nt(dkv[:, :HS], w_key[...])
        + dot_nt(dkv[:, HS:], w_value[...])
    )
    xf = x[...].astype(jnp.float32)
    inv = lax.rsqrt(jnp.mean(xf * xf, axis=-1, keepdims=True) + EPS)
    normed = xf * inv
    scaled = dhidden * gain[...]
    mean = jnp.mean(scaled * normed, axis=-1, keepdims=True)
    d_in[...] = (grad_out[...].astype(jnp.float32) + inv * (scaled - normed * mean)).astype(d_in.dtype)


SMEM = pl.BlockSpec(memory_space=pltpu.SMEM)
VMEM = pl.BlockSpec(memory_space=pltpu.VMEM)
ANY = pl.BlockSpec(memory_space=pl.ANY)


def shape(*dims, dtype=jnp.bfloat16):
    return jax.ShapeDtypeStruct(dims, dtype)


def call(body, outs, args, flops, smem=0, scratch=(), in_any=(), out_any=()):
    specs = [SMEM if n < smem else ANY if n in in_any else VMEM for n in range(len(args))]
    if isinstance(outs, tuple):
        out_specs = tuple(ANY if n in out_any else VMEM for n in range(len(outs)))
    else:
        out_specs = VMEM
    return pl.pallas_call(
        body,
        out_shape=outs,
        in_specs=specs,
        out_specs=out_specs,
        scratch_shapes=list(scratch),
        compiler_params=pltpu.CompilerParams(vmem_limit_bytes=VMEM_BYTES),
        cost_estimate=pl.CostEstimate(flops=flops, bytes_accessed=1 << 20, transcendentals=0),
    )(*args)


def scratch(*dims, dtype=jnp.bfloat16):
    return pltpu.VMEM(dims, dtype)


def run_stats(info, own, pair, keys):
    tok, wide = own.shape[1:]
    chips, heads = keys.shape[0], wide // HS
    seq = 2 * tok * chips
    rows = scratch(1, 2 * wide, dtype=jnp.float32)
    return call(
        functools.partial(stats_kernel, heads, seq),
        shape(2, 2, wide, dtype=jnp.float32),
        (info, own, pair, keys),
        2 * seq * wide * HS,
        smem=1,
        scratch=(rows, rows),
    )


def run_attend(info, own, pair, mine, other, keys, values):
    tok, wide = own.shape[1:]
    chips, heads = keys.shape[0], wide // HS
    seq = 2 * tok * chips
    return call(
        functools.partial(attend_kernel, heads, seq),
        (shape(2, wide, tok), shape(chips, tok, HS), shape(chips * tok, 2 * wide)),
        (info, own, pair, mine, other, keys, values),
        6 * seq * wide * HS,
        smem=1,
        in_any=(6,),
        out_any=(1, 2),
        scratch=(
            scratch(chips, tok, HS),
            scratch(HS, chips * tok),
            scratch(2 * wide, HS),
            scratch(chips, tok, HS),
            scratch(chips * tok, 2 * wide),
            scratch(1, 2 * wide, dtype=jnp.float32),
            pltpu.SemaphoreType.DMA,
            pltpu.SemaphoreType.DMA((chips,)),
            pltpu.SemaphoreType.DMA((chips,)),
        ),
    )


def run_grads(info, own, pair, mine, other, keys, values, probs):
    tok, wide = own.shape[1:]
    chips, heads = keys.shape[0], wide // HS
    seq = 2 * tok * chips
    return call(
        functools.partial(grads_kernel, heads, seq),
        (shape(chips, tok, HS), shape(2, tok, wide)),
        (info, own, pair, mine, other, keys, values, probs),
        6 * seq * wide * HS,
        smem=1,
        in_any=(5, 7),
        out_any=(0,),
        scratch=(
            scratch(chips, tok, HS),
            scratch(HS, chips * tok),
            scratch(2 * wide, HS),
            scratch(chips, tok, HS),
            scratch(chips * tok, 2 * wide),
            scratch(chips * tok, 2 * wide),
            scratch(1, 2 * wide, dtype=jnp.float32),
            pltpu.SemaphoreType.DMA,
            pltpu.SemaphoreType.DMA((chips,)),
            pltpu.SemaphoreType.DMA((chips,)),
        ),
    )


CORES = 2
X = 4


def swap_cores(value):
    count = lax.axis_size("blk")
    return lax.ppermute(value, "blk", [(i, i ^ 1) for i in range(count)])


def send_along_x(value, step):
    count = lax.axis_size("dp")
    return lax.ppermute(
        value, "dp", [(i, i // X * X + (i + step) % X) for i in range(count)]
    )


def exchange_chips(value):
    chips = lax.axis_size("blk") // CORES
    groups = [[core + CORES * chip for chip in range(chips)] for core in range(CORES)]
    return lax.all_to_all(value, "blk", 0, 0, tiled=True, axis_index_groups=groups)


def exchange_plane(value):
    blk, dp = lax.axis_size("blk"), lax.axis_size("dp")
    groups = [
        [(outer * X + x) * blk + chip * CORES + core for outer in range(dp // X) for chip in range(blk // CORES)]
        for x in range(X)
        for core in range(CORES)
    ]
    value = value.reshape(dp // X * (blk // CORES), -1, value.shape[1])
    return lax.all_to_all(value, ("dp", "blk"), 0, 0, tiled=True, axis_index_groups=groups)


def per_device(inputs, upstream, gain, w_query, w_key, w_value, w_out, prefix_len, bound):
    return whole(inputs[0], upstream[0], gain, w_query, w_key, w_value, w_out, prefix_len, bound)


def whole(inputs, grad_out, gain, w_query, w_key, w_value, w_out, prefix_len, bound):
    tok, wide = inputs.shape
    heads_wide = w_query.shape[1]
    my, dp = lax.axis_index("blk"), lax.axis_index("dp")
    count, share = lax.axis_size("blk"), lax.axis_size("dp")
    chips, outer = count // CORES, share // X
    size = wide // (count * share)
    core, x = my % CORES, dp % X
    info = jnp.stack([my, prefix_len[0], bound[0] * BLOCK, core, x]).astype(jnp.int32)
    gain_row = gain.reshape(1, wide)
    filed = shape(X, outer, chips, size, tok)
    copies = shape(chips, tok, HS)
    hidden, k_copies = call(
        functools.partial(prepare_kernel, chips),
        (shape(tok, wide), copies),
        (inputs, gain_row, w_key),
        4 * tok * wide * HS,
    )
    keys = exchange_chips(k_copies)
    own, v_copies, ht_own, ht_pair = call(
        project_kernel,
        (shape(2, tok, heads_wide), copies, filed, filed),
        (info, hidden, grad_out, w_query, w_out, w_value),
        4 * tok * wide * wide,
        smem=1,
    )
    values = exchange_chips(v_copies)
    pair = swap_cores(own)
    grad_pair = swap_cores(grad_out)
    ht_pair = swap_cores(ht_pair)
    mine = run_stats(info, own, pair, keys)
    other = swap_cores(mine)
    attn, dv, probs = run_attend(info, own, pair, mine, other, keys, values)
    attn_other = swap_cores(attn)
    dv_parts = exchange_chips(dv)
    dk, dq_mine = run_grads(info, own, pair, attn, attn_other, keys, values, probs)
    dq_other = swap_cores(dq_mine)
    dk_parts = exchange_chips(dk)
    rows = outer * chips * size
    d_query_rows, base, *parts = call(
        terms_kernel,
        (
            shape(tok, heads_wide),
            shape(rows, wide + heads_wide, dtype=jnp.float32),
            *[shape(rows, wide + heads_wide)] * (X - 1),
        ),
        (info, attn, attn_other, grad_out, grad_pair, ht_own, ht_pair, dq_mine, dq_other),
        8 * X * rows * wide * tok,
        smem=1,
        scratch=[scratch(*filed.shape)] * 2,
    )
    arrived = []
    for step, terms in enumerate(parts, 1):
        arrived.append(send_along_x(terms, step))
    d_value_rows = call(total_kernel, shape(tok, HS), (dv_parts,), 1 << 30)
    d_kv_rows = call(rows_kernel, shape(tok, 2 * HS), (dk_parts, d_value_rows), 1 << 30)
    d_kv_pair = swap_cores(d_kv_rows)
    kv_terms = call(
        kv_kernel,
        shape(rows, X * 2 * HS),
        (info, ht_own, ht_pair, d_kv_rows, d_kv_pair),
        1 << 30,
        smem=1,
    )
    kv_parts = exchange_plane(kv_terms)
    terms = call(collect_kernel, shape(rows, wide + heads_wide), (base, *arrived), 1 << 30)
    parts = exchange_plane(terms)
    kv_base, *kv_pieces = call(
        split_kernel,
        (shape(size, 2 * HS, dtype=jnp.float32), *[shape(size, 2 * HS)] * (X - 1)),
        (info, kv_parts),
        1 << 30,
        smem=1,
    )
    kv_arrived = []
    for step, piece in enumerate(kv_pieces, 1):
        kv_arrived.append(send_along_x(piece, step))
    kv_total = call(collect_kernel, shape(size, 2 * HS), (kv_base, *kv_arrived), 1 << 20)
    total = wide + heads_wide + 2 * HS
    copies = call(spread_kernel, shape(share, size, total), (parts, kv_total), 1 << 30)
    shared = lax.all_to_all(copies, "dp", 0, 0, tiled=True)
    d_in = call(
        finish_kernel,
        shape(tok, wide),
        (inputs, grad_out, gain_row, d_query_rows, d_kv_rows, w_query, w_key, w_value),
        2 * tok * wide * (wide + 2 * HS),
    )
    held = wide // count
    f32 = functools.partial(shape, dtype=jnp.float32)
    d_query, d_key, d_value, d_out, d_gain = call(
        weights_kernel,
        (f32(held, heads_wide), f32(held, HS), f32(held, HS), f32(held, wide), f32(1, held)),
        (info, shared, gain.reshape(count, held), w_query, w_key, w_value),
        1 << 30,
        smem=1,
        in_any=(3, 4, 5),
        scratch=(
            scratch(held, heads_wide),
            scratch(held, HS),
            scratch(held, HS),
            pltpu.SemaphoreType.DMA((3,)),
        ),
    )
    return (d_in[None], d_query, d_key, d_value, d_out, d_gain.reshape(held))


def solution(mesh):
    placed = (P("dp", "blk", None), P("dp", "blk", None), P(), P(), P(), P(), P(), P("dp"), P("dp"))
    return jax.shard_map(
        per_device,
        mesh=mesh,
        in_specs=placed,
        out_specs=(
            P("dp", "blk", None),
            P("blk", None),
            P("blk", None),
            P("blk", None),
            P("blk", None),
            P("blk"),
        ),
        check_vma=False,
    )
```
